256 devices in a mesh: gx: 16 (over x, z_lo, core), gy: 16 (over z_hi, y).
Axes of the slice: x: 4, y: 4, z: 8 (z_hi: 4, z_lo: 2; z = z_hi * 2 + z_lo), core: 2. Of those that a mesh axis runs over, the one named last changes fastest.
Arguments:
- fine_source: bfloat16 [16, 16, 4, 8000], P('gx', 'gy'), may hold values from -6 to 6
- fine_blocks: bfloat16 [3, 12, 20, 20], replicated, may hold values from -0.5 to 0.5
- coarse_blocks: bfloat16 [3, 12, 20, 20], replicated, may hold values from -0.5 to 0.5
- child_filter_matrices: bfloat16 [2, 20, 20], replicated, may hold values from -1 to 1
Outputs:
- fine_result: float32 [16, 16, 4, 8000], P('gx', 'gy')
The draws below stay inside these ranges and needn't reach their ends.
All inputs are finite; a program needn't handle non-finite values.
Results may differ from the reference program's by a relative error of at most 0.013.
Values may be sent and summed in bfloat16 or wider, within the bound.
No kernel may reach another device: no remote copies, remote signals or barrier semaphores. Data moves between devices by JAX's collectives and lax.ppermute only.
A program may use at most 64 MiB of HBM per device.

```python
import jax
import jax.numpy as jnp
from jax import lax

K2 = 20
TERMS = 12
FZ = 4
NXF = 16
NYF = 16


def block_levels(key, extent, split, smallest, top_value):
    factor_of = 1.0
    for position, parts in split:
        draws = jax.random.uniform(jax.random.fold_in(jax.random.fold_in(key, 6), position), (parts,), jnp.float32, smallest / len(split), top_value / len(split))
        factor_of = factor_of * jnp.repeat(jnp.exp(draws), extent[position] // parts).reshape((-1,) + (1,) * (len(extent) - 1 - position))
    return factor_of


def bell_draw(rng, extent, spread, most, cuts=(), kind=jnp.bfloat16):
    array = jax.random.normal(rng, extent, jnp.float32) * spread
    if len(cuts) > 0:
        array = block_levels(rng, extent, cuts, -0.22, 0.18) * array
    return jnp.clip(array, min=-most, max=most).astype(kind)


def setup_inputs(seed: int = 0) -> dict:
    keys = jax.random.split(jax.random.key(seed), 5)
    return {
        "fine_source": bell_draw(keys[0], (NXF, NYF, FZ, K2 * K2 * K2), 1.0, 6.0, ((0, 16), (1, 16))),
        "fine_blocks": bell_draw(keys[1], (3, TERMS, K2, K2), (6 * K2) ** -0.5, 0.5),
        "coarse_blocks": bell_draw(keys[2], (3, TERMS, K2, K2), (6 * K2) ** -0.5, 0.5),
        "child_filter_matrices": bell_draw(keys[3], (2, K2, K2), (2 * K2) ** -0.5, 1.0),
    }


def run_pass(values, matrix, coef_axis):
    matrix = matrix.astype(jnp.float32)
    values = values.astype(jnp.float32)
    if coef_axis == 0:
        return jnp.einsum('ca,...ajk->...cjk', matrix, values)
    if coef_axis == 1:
        return jnp.einsum('ca,...iak->...ick', matrix, values)
    return jnp.einsum('ca,...ija->...ijc', matrix, values)


def rounded(values):
    return lax.optimization_barrier(values.astype(jnp.bfloat16))


def shifted(values, grid_axis, offset):
    widths = [(0, 0)] * values.ndim
    widths[grid_axis] = (1, 1)
    padded = jnp.pad(values, widths)
    length = values.shape[grid_axis]
    return lax.slice_in_dim(padded, 1 + offset, 1 + offset + length, axis=grid_axis)


def apply_level(source, blocks):
    def one_term(summed, term_index):
        current = lax.dynamic_index_in_dim(blocks, term_index, 1, keepdims=False)
        lower_block, middle, upper_block = current[0], current[1], current[2]
        base_x = rounded(run_pass(source, middle, 0))
        upper_x = rounded(run_pass(shifted(source, 0, 1), upper_block, 0))
        lower_x = rounded(run_pass(shifted(source, 0, -1), lower_block, 0))
        base_y = rounded(run_pass(base_x, middle, 1))
        upper_y = rounded(run_pass(shifted(base_x, 1, 1), upper_block, 1))
        lower_child_y = rounded(run_pass(shifted(base_x, 1, -1), lower_block, 1))
        upper_xy = rounded(run_pass(upper_x, middle, 1))
        lower_xy = rounded(run_pass(lower_x, middle, 1))
        summed = summed + run_pass(base_y, middle, 2)
        summed = summed + run_pass(shifted(base_y, 2, 1), upper_block, 2)
        summed = summed + run_pass(shifted(base_y, 2, -1), lower_block, 2)
        summed = summed + run_pass(upper_y, middle, 2) + run_pass(lower_child_y, middle, 2)
        summed = summed + run_pass(upper_xy, middle, 2) + run_pass(lower_xy, middle, 2)
        return summed, None

    summed = jnp.zeros(source.shape, jnp.float32)
    summed, _ = lax.scan(one_term, summed, jnp.arange(TERMS, dtype=jnp.int32))
    return summed


def reference(fine_source, fine_blocks, coarse_blocks, child_filter_matrices):
    source = fine_source.reshape(NXF, NYF, FZ, K2, K2, K2)
    fine_term = apply_level(source, fine_blocks)
    scale_factors = child_filter_matrices.astype(jnp.float32)
    children = source.reshape(NXF // 2, 2, NYF // 2, 2, FZ // 2, 2, K2, K2, K2).astype(jnp.float32)
    after_x = rounded(jnp.einsum('ali,xaybzcijk->xaybzcljk', scale_factors, children)).astype(jnp.float32)
    after_y_pass = rounded(jnp.einsum('blj,xaybzcijk->xaybzcilk', scale_factors, after_x)).astype(jnp.float32)
    filtered_coefficients = jnp.einsum('fet,huwgofnmt->huwgofnme', scale_factors, after_y_pass)
    coarse_source = rounded(jnp.sum(filtered_coefficients, axis=(1, 3, 5)))
    coarse_result = rounded(apply_level(coarse_source, coarse_blocks)).astype(jnp.float32)
    grown_x = rounded(jnp.einsum('ail,xyzijk->xayzljk', scale_factors, coarse_result)).astype(jnp.float32)
    grown_y = rounded(jnp.einsum('bjm,xayzljk->xaybzlmk', scale_factors, grown_x)).astype(jnp.float32)
    expanded = jnp.einsum('ckn,xaybzlmk->xaybzclmn', scale_factors, grown_y)
    expanded = expanded.reshape(NXF, NYF, FZ, K2, K2, K2)
    return (fine_term + expanded).reshape(NXF, NYF, FZ, K2 * K2 * K2)
```

```python
import functools

import jax
import jax.numpy as jnp
from jax import lax
from jax.experimental import pallas as pl
from jax.experimental.pallas import tpu as pltpu
from jax.sharding import PartitionSpec as P

K2 = 20
TERMS = 12
BF = jnp.bfloat16
F32 = jnp.float32
ORDER = (1, 2, 0)
FINE_ROWS = 80
COARSE_ROWS = 48


def iota(shape, dim):
    return lax.broadcasted_iota(jnp.int32, shape, dim)


def dot(a, b):
    return jnp.dot(a, b, preferred_element_type=F32)


def place(n):
    block, t = n >> 7, n & 127
    first = (t * 205) >> 11
    return block, first, t - 10 * first, t < 100


def lane_constants(which):
    b, f, s, ok = place(iota((256, K2), 0))
    index = b * 10 + (f if which == 0 else s)
    spread_rows = jnp.where(ok & (index == iota((256, K2), 1)), 1.0, 0.0).astype(BF)
    b, f, s, ok = place(iota((K2, 256), 1))
    index = b * 10 + (f if which == 0 else s)
    spread_lanes = jnp.where(ok & (index == iota((K2, 256), 0)), 1.0, 0.0).astype(BF)
    _, f0, s0, ok0 = place(iota((256, 256), 0))
    _, f1, s1, ok1 = place(iota((256, 256), 1))
    same = (s0 == s1) if which == 0 else (f0 == f1)
    mask = jnp.where(same & ok0 & ok1, 1.0, 0.0)
    return spread_rows, spread_lanes, mask


def lane_matrix(transposed, constants):
    spread_rows, spread_lanes, mask = constants
    wide = dot(transposed, spread_lanes).astype(BF)
    return (dot(spread_rows, wide) * mask).astype(BF)


def row_constants(rows, nz, copies):
    shift = nz.bit_length() - 1
    r = iota((rows, K2), 0)
    spread_rows = jnp.where((r >> shift) == iota((rows, K2), 1), 1.0, 0.0).astype(BF)
    spreads = []
    for c in range(copies):
        col = iota((K2, copies * rows), 1) - c * rows
        here = (col >= 0) & (col < rows) & ((col >> shift) == iota((K2, copies * rows), 0))
        spreads.append(jnp.where(here, 1.0, 0.0).astype(BF))
    shape = (rows, copies * rows)
    col = iota(shape, 1)
    for c in range(1, copies):
        col = jnp.where(iota(shape, 1) >= c * rows, iota(shape, 1) - c * rows, col)
    mask = jnp.where((iota(shape, 0) & (nz - 1)) == (col & (nz - 1)), 1.0, 0.0)
    return spread_rows, spreads, mask


def flipped(matrix):
    return matrix.astype(F32).T.astype(BF)


def build_kernel(fine_ref, coarse_ref, child_ref, *outs):
    (fine_rows, fine_y, fine_z, coarse_rows, coarse_y, coarse_z,
     down_rows, down_y, down_z, up_rows, up_y, up_z) = outs
    on_first, on_second = lane_constants(0), lane_constants(1)
    levels = (
        (fine_ref, fine_rows, fine_y, fine_z, FINE_ROWS, 4),
        (coarse_ref, coarse_rows, coarse_y, coarse_z, COARSE_ROWS, 2),
    )
    for blocks, rows_out, y_out, z_out, rows, nz in levels:
        spread_rows, spreads, mask = row_constants(rows, nz, 3)

        def term(m, carry, blocks=blocks, rows_out=rows_out, y_out=y_out, z_out=z_out, rows=rows,
                 spread_rows=spread_rows, spreads=spreads, mask=mask):
            wide = jnp.zeros((K2, 3 * rows), F32)
            for n, d in enumerate(ORDER):
                matrix = blocks[d, m]
                wide = wide + dot(matrix, spreads[n])
                transposed = flipped(matrix)
                y_out[m, pl.ds(n * 256, 256), :] = lane_matrix(transposed, on_first)
                z_out[n, m] = lane_matrix(transposed, on_second)
            rows_out[m] = (dot(spread_rows, wide.astype(BF)) * mask).astype(BF)
            return carry

        lax.fori_loop(0, TERMS, term, 0, unroll=2)

    px, py = lax.axis_index("gx") & 1, lax.axis_index("gy") & 1
    own_x, other_x, own_y, other_y = child_ref[px], child_ref[1 - px], child_ref[py], child_ref[1 - py]
    down_y[0] = lane_matrix(flipped(own_y), on_first)
    down_y[1] = lane_matrix(flipped(other_y), on_first)
    up_y[...] = lane_matrix(own_y, on_first)
    for c in range(2):
        down_z[c] = lane_matrix(flipped(child_ref[c]), on_second)
        up_z[c] = lane_matrix(child_ref[c], on_second)
    _, spreads, _ = row_constants(FINE_ROWS, 4, 2)
    wide = (dot(own_x, spreads[0]) + dot(other_x, spreads[1])).astype(BF)
    r = iota((2 * COARSE_ROWS, K2), 0)
    r = jnp.where(r >= COARSE_ROWS, r - COARSE_ROWS, r)
    spread_rows = jnp.where((r >> 1) == iota((2 * COARSE_ROWS, K2), 1), 1.0, 0.0).astype(BF)
    shape = (2 * COARSE_ROWS, 2 * FINE_ROWS)
    r = iota(shape, 0)
    cz = jnp.where(r >= COARSE_ROWS, 1, 0)
    keep = (2 * (r & 1) + cz) == (iota(shape, 1) & 3)
    down_rows[...] = (dot(spread_rows, wide) * jnp.where(keep, 1.0, 0.0)).astype(BF)
    shape = (K2, COARSE_ROWS)
    spread = jnp.where((iota(shape, 1) >> 1) == iota(shape, 0), 1.0, 0.0).astype(BF)
    wide = dot(flipped(own_x), spread).astype(BF)
    shape = (FINE_ROWS, K2)
    spread_rows = jnp.where((iota(shape, 0) >> 2) == iota(shape, 1), 1.0, 0.0).astype(BF)
    shape = (FINE_ROWS, COARSE_ROWS)
    keep = ((iota(shape, 0) & 3) >> 1) == (iota(shape, 1) & 1)
    up_rows[...] = (dot(spread_rows, wide) * jnp.where(keep, 1.0, 0.0)).astype(BF)


def build(fine_blocks, coarse_blocks, child):
    def s(*shape):
        return jax.ShapeDtypeStruct(shape, BF)

    out_shape = (
        s(TERMS, FINE_ROWS, 3 * FINE_ROWS), s(TERMS, 768, 256), s(3, TERMS, 256, 256),
        s(TERMS, COARSE_ROWS, 3 * COARSE_ROWS), s(TERMS, 768, 256), s(3, TERMS, 256, 256),
        s(2 * COARSE_ROWS, 2 * FINE_ROWS), s(2, 256, 256), s(2, 256, 256),
        s(FINE_ROWS, COARSE_ROWS), s(256, 256), s(2, 256, 256),
    )
    return pl.pallas_call(
        build_kernel, out_shape=out_shape, name="build",
        compiler_params=pltpu.CompilerParams(vmem_limit_bytes=32 << 20),
        cost_estimate=pl.CostEstimate(flops=8 * 10**9, bytes_accessed=20 * 10**6, transcendentals=0),
    )(fine_blocks, coarse_blocks, child)


def source_kernel(own, xup, xlow, yup, ylow, corner, down_rows, down_y, down_z,
                  along_x, along_y, parent, natural, pair_low, pair_high, mixed, turned):
    shape = (400, 512)
    n, lane = iota(shape, 0), iota(shape, 1)
    j = (n * 205) >> 12
    k = n - 20 * j
    g, rest = lane >> 8, lane & 255
    h, jj, kk, ok = place(rest)
    select = jnp.where(ok & (j == 10 * h + jj) & (k == 10 * g + kk), 1.0, 0.0).astype(BF)

    def converted(ref, slot):
        values = ref[0, 0].astype(F32)
        for i in range(K2):
            natural[slot, 4 * i:4 * i + 4, :] = values[:, 400 * i:400 * i + 400]
        return dot(natural[slot].astype(BF), select)

    centre = converted(own, 0).astype(BF)
    x_up, x_low = converted(xup, 1), converted(xlow, 2)
    y_up, y_low = converted(yup, 3), converted(ylow, 4)
    diagonal = converted(corner, 5).astype(BF)
    along_x[0:80, :] = centre
    along_x[80:160, :] = x_up.astype(BF)
    along_x[160:240, :] = x_low.astype(BF)
    along_y[:, 0:512] = centre
    along_y[:, 512:1024] = y_up.astype(BF)
    along_y[:, 1024:1536] = y_low.astype(BF)
    px, py = lax.axis_index("gx") & 1, lax.axis_index("gy") & 1
    pair_low[0:80, :] = centre
    pair_low[80:160, :] = jnp.where(px == 0, x_up, x_low).astype(BF)
    pair_high[0:80, :] = jnp.where(py == 0, y_up, y_low).astype(BF)
    pair_high[80:160, :] = diagonal
    for c, pair in enumerate((pair_low, pair_high)):
        rows = dot(down_rows[...], pair[...]).astype(BF)
        for g in range(2):
            mixed[c, 96 * g:96 * g + 96, :] = rows[:, 256 * g:256 * g + 256]
    summed = dot(mixed[0], down_y[0]) + dot(mixed[1], down_y[1])
    summed = summed.astype(BF)
    for c in range(2):
        for g in range(2):
            for h in range(2):
                turned[c, 48 * h:48 * h + 48, 128 * g:128 * g + 128] = (
                    summed[96 * g + 48 * c:96 * g + 48 * c + 48, 128 * h:128 * h + 128]
                )
    total = (dot(turned[0], down_z[0]) + dot(turned[1], down_z[1])).astype(BF)
    for g in range(2):
        for h in range(2):
            parent[:, 256 * g + 128 * h:256 * g + 128 * h + 128] = (
                total[48 * h:48 * h + 48, 128 * g:128 * g + 128]
            )


def source(columns, down_rows, down_y, down_z):
    out_shape = (
        jax.ShapeDtypeStruct((3 * FINE_ROWS, 512), BF),
        jax.ShapeDtypeStruct((FINE_ROWS, 1536), BF),
        jax.ShapeDtypeStruct((COARSE_ROWS, 512), BF),
    )
    scratch = [
        pltpu.VMEM((6, FINE_ROWS, 400), F32),
        pltpu.VMEM((2 * FINE_ROWS, 512), BF),
        pltpu.VMEM((2 * FINE_ROWS, 512), BF),
        pltpu.VMEM((2, 4 * COARSE_ROWS, 256), BF),
        pltpu.VMEM((2, 2 * COARSE_ROWS, 256), BF),
    ]
    return pl.pallas_call(
        source_kernel, out_shape=out_shape, scratch_shapes=scratch, name="source",
        compiler_params=pltpu.CompilerParams(vmem_limit_bytes=16 << 20),
        cost_estimate=pl.CostEstimate(flops=10**9, bytes_accessed=10**6, transcendentals=0),
    )(*columns, down_rows, down_y, down_z)


def level(rows, nz, along_x, along_y, row_mats, y_mats, z_mats, first, plain, sums, centres):
    for m in range(TERMS):
        both = dot(row_mats[m], along_x)
        sides = dot(row_mats[m][:, 0:rows], along_y)
        for g in range(2):
            here = pl.ds(g * rows, rows)
            first[m, here, 0:256] = both[:, 256 * g:256 * g + 256].astype(BF)
            first[m, here, 256:512] = sides[:, 512 + 256 * g:768 + 256 * g].astype(BF)
            first[m, here, 512:768] = sides[:, 1024 + 256 * g:1280 + 256 * g].astype(BF)
            plain[m, here, :] = sides[:, 256 * g:256 * g + 256].astype(BF)
    for m in range(TERMS):
        summed = dot(first[m], y_mats[m]).astype(BF)
        centre = dot(plain[m], y_mats[m, 0:256, :]).astype(BF)
        for g in range(2):
            for h in range(2):
                here = pl.ds(h * rows, rows)
                lanes = pl.ds(m * 256 + g * 128, 128)
                sums[here, lanes] = summed[g * rows:(g + 1) * rows, 128 * h:128 * h + 128]
                centres[here, lanes] = centre[g * rows:(g + 1) * rows, 128 * h:128 * h + 128]
    total = dot(sums[...], z_mats[0].reshape(TERMS * 256, 256))
    upper = dot(centres[...], z_mats[1].reshape(TERMS * 256, 256))
    lower = dot(centres[...], z_mats[2].reshape(TERMS * 256, 256))
    z = iota((2 * rows, 256), 0) & (nz - 1)
    total = total + jnp.where(z == nz - 1, 0.0, pltpu.roll(upper, 2 * rows - 1, 0))
    return total + jnp.where(z == 0, 0.0, pltpu.roll(lower, 1, 0))


def level_scratch(rows):
    return [
        pltpu.VMEM((TERMS, 2 * rows, 768), BF),
        pltpu.VMEM((TERMS, 2 * rows, 256), BF),
        pltpu.VMEM((2 * rows, TERMS * 256), BF),
        pltpu.VMEM((2 * rows, TERMS * 256), BF),
    ]


def fine_kernel(along_x, along_y, row_mats, y_mats, z_mats, out, *scratch):
    out[...] = level(FINE_ROWS, 4, along_x[...], along_y[...], row_mats, y_mats, z_mats, *scratch)


def fine(along_x, along_y, row_mats, y_mats, z_mats):
    return pl.pallas_call(
        fine_kernel, out_shape=jax.ShapeDtypeStruct((2 * FINE_ROWS, 256), F32),
        scratch_shapes=level_scratch(FINE_ROWS), name="fine",
        compiler_params=pltpu.CompilerParams(vmem_limit_bytes=32 << 20),
        cost_estimate=pl.CostEstimate(flops=6 * 10**9, bytes_accessed=10 * 10**6, transcendentals=0),
    )(along_x, along_y, row_mats, y_mats, z_mats)


def coarse_kernel(own, xup, xlow, yup, ylow, row_mats, y_mats, z_mats, up_rows, up_y, up_z, fine_term,
                  out, along_x, along_y, grown, turned, *scratch):
    along_x[0:48, :] = own[...]
    along_x[48:96, :] = xup[...]
    along_x[96:144, :] = xlow[...]
    along_y[:, 0:512] = own[...]
    along_y[:, 512:1024] = yup[...]
    along_y[:, 1024:1536] = ylow[...]
    result = level(COARSE_ROWS, 2, along_x[...], along_y[...], row_mats, y_mats, z_mats, *scratch).astype(BF)
    for h in range(2):
        part = dot(up_rows[...], result[48 * h:48 * h + 48, :]).astype(BF)
        for g in range(2):
            grown[80 * g:80 * g + 80, 128 * h:128 * h + 128] = part[:, 128 * g:128 * g + 128]
    part = dot(grown[...], up_y[...]).astype(BF)
    for h in range(2):
        for g in range(2):
            turned[80 * h:80 * h + 80, 128 * g:128 * g + 128] = part[80 * g:80 * g + 80, 128 * h:128 * h + 128]
    even = dot(turned[...], up_z[0])
    odd = dot(turned[...], up_z[1])
    expanded = jnp.where((iota((160, 256), 0) & 1) == 0, even, odd)
    total = fine_term[...] + expanded
    high = total.astype(BF)
    low = (total - high.astype(F32)).astype(BF)
    natural = jnp.zeros((80, 400), F32)
    for h in range(2):
        shape = (256, 400)
        g, jj, kk, ok = place(iota(shape, 0))
        n = iota(shape, 1)
        select = jnp.where(ok & (n == (10 * h + jj) * 20 + 10 * g + kk), 1.0, 0.0).astype(BF)
        natural = natural + dot(high[80 * h:80 * h + 80, :], select) + dot(low[80 * h:80 * h + 80, :], select)
    for i in range(K2):
        out[0, 0, :, 400 * i:400 * i + 400] = natural[4 * i:4 * i + 4, :]


def coarse(parents, row_mats, y_mats, z_mats, up_rows, up_y, up_z, fine_term):
    scratch = [
        pltpu.VMEM((3 * COARSE_ROWS, 512), BF),
        pltpu.VMEM((COARSE_ROWS, 1536), BF),
        pltpu.VMEM((160, 256), BF),
        pltpu.VMEM((160, 256), BF),
    ] + level_scratch(COARSE_ROWS)
    return pl.pallas_call(
        coarse_kernel, out_shape=jax.ShapeDtypeStruct((1, 1, 4, 8000), F32),
        scratch_shapes=scratch, name="coarse",
        compiler_params=pltpu.CompilerParams(vmem_limit_bytes=32 << 20),
        cost_estimate=pl.CostEstimate(flops=4 * 10**9, bytes_accessed=10 * 10**6, transcendentals=0),
    )(*parents, row_mats, y_mats, z_mats, up_rows, up_y, up_z, fine_term)


def moved(block, axis, distance):
    count = lax.axis_size(axis)
    route = [(i + distance, i) for i in range(count) if 0 <= i + distance < count]
    return lax.ppermute(block, axis, route)


def corner(block):
    nx, ny = lax.axis_size("gx"), lax.axis_size("gy")
    route = [(x * ny + y, (x ^ 1) * ny + (y ^ 1)) for x in range(nx) for y in range(ny)]
    return lax.ppermute(block, ("gx", "gy"), route)


def shards(fine_source, fine_blocks, coarse_blocks, child_filter_matrices):
    columns = [fine_source, moved(fine_source, "gx", 1), moved(fine_source, "gx", -1),
               moved(fine_source, "gy", 1), moved(fine_source, "gy", -1), corner(fine_source)]
    built = build(fine_blocks, coarse_blocks, child_filter_matrices)
    along_x, along_y, parent = source(columns, *built[6:9])
    parents = [parent, moved(parent, "gx", 2), moved(parent, "gx", -2),
               moved(parent, "gy", 2), moved(parent, "gy", -2)]
    fine_term = fine(along_x, along_y, *built[0:3])
    return coarse(parents, *built[3:6], *built[9:12], fine_term)


def solution(mesh):
    in_specs = (P("gx", "gy", None, None), P(), P(), P())
    out_specs = P("gx", "gy", None, None)
    return jax.shard_map(shards, mesh=mesh, in_specs=in_specs, out_specs=out_specs, check_vma=False)
```

```python
import jax
import jax.numpy as jnp
from jax import lax
from jax.experimental import pallas as pl
from jax.experimental.pallas import tpu as pltpu
from jax.sharding import PartitionSpec as P

K2 = 20
TERMS = 12
BF = jnp.bfloat16
F32 = jnp.float32
FINE_ROWS = 80
COARSE_ROWS = 48


def iota(shape, dim):
    return lax.broadcasted_iota(jnp.int32, shape, dim)


def dot(a, b):
    return jnp.dot(a, b, preferred_element_type=F32)


def place(n):
    piece, t = n >> 5, n & 31
    jj = (t * 13) >> 6
    return piece, jj, t - 5 * jj, t < 25


def natural_place(n, y_order):
    block = n >> 7
    piece, jj, kk, ok = place(n & 127)
    j, k = (piece, block) if y_order else (block, piece)
    return jnp.where(ok, (5 * j + jj) * 20 + 5 * k + kk, -1)


def onehot(condition, dtype=BF):
    return jnp.where(condition, 1.0, 0.0).astype(dtype)


def lane_constants(on_j):
    def index(n):
        piece, jj, kk, ok = place(n)
        return jnp.where(ok, piece * 5 + (jj if on_j else kk), -1)

    def fixed(n, none):
        _, jj, kk, ok = place(n)
        return jnp.where(ok, kk if on_j else jj, none)

    spread_rows = onehot(index(iota((128, 1), 0)) == iota((128, K2), 1))
    spread_lanes = onehot(index(iota((1, 128), 1)) == iota((K2, 128), 0))
    mask = onehot(fixed(iota((128, 1), 0), -1) == fixed(iota((1, 128), 1), -2), F32)
    return spread_rows, spread_lanes, mask


def row_constants(rows, nz):
    shift = nz.bit_length() - 1
    spread_rows = onehot((iota((rows, 1), 0) >> shift) == iota((rows, K2), 1))
    lane = iota((1, 3 * rows), 1)
    which = jnp.where(lane >= rows, 1, 0) + jnp.where(lane >= 2 * rows, 1, 0)
    lane = lane - which * rows
    spreads = [
        onehot(jnp.where(which == c, lane >> shift, -1) == iota((K2, 3 * rows), 0)) for c in range(3)
    ]
    mask = onehot((iota((rows, 1), 0) & (nz - 1)) == (lane & (nz - 1)), F32)
    return spread_rows, spreads, mask


def flipped(matrix):
    return matrix.astype(F32).T.astype(BF)


def exchange(tiles):
    lane = iota((1, 128), 1)
    low = (lane & 64) == 0
    a, b, c, d = tiles
    a, c = jnp.where(low, a, pltpu.roll(c, 64, 1)), jnp.where(low, pltpu.roll(a, 64, 1), c)
    b, d = jnp.where(low, b, pltpu.roll(d, 64, 1)), jnp.where(low, pltpu.roll(b, 64, 1), d)
    low = (lane & 32) == 0
    a, b = jnp.where(low, a, pltpu.roll(b, 32, 1)), jnp.where(low, pltpu.roll(a, 96, 1), b)
    c, d = jnp.where(low, c, pltpu.roll(d, 32, 1)), jnp.where(low, pltpu.roll(c, 96, 1), d)
    return a, b, c, d


def build_kernel(fine_hbm, coarse_hbm, child_hbm, *refs):
    (fine_rows, fine_y, fine_z, fine_sides, coarse_rows, coarse_y, coarse_z, coarse_sides,
     down_rows, down_y, down_z, up_rows, up_y, up_z, fine_ref, coarse_ref, child_ref, sems) = refs
    copies = [
        pltpu.make_async_copy(src, dst, sems.at[n])
        for n, (src, dst) in enumerate(((fine_hbm, fine_ref), (coarse_hbm, coarse_ref), (child_hbm, child_ref)))
    ]
    for copy in copies:
        copy.start()
    px, py = lax.axis_index("gx") & 1, lax.axis_index("gy") & 1
    rows_y, lanes_y, mask_y = lane_constants(True)
    rows_z, lanes_z, mask_z = lane_constants(False)
    mask3_y = jnp.concatenate([mask_y] * 3, axis=1)
    mask3_z = jnp.concatenate([mask_z] * 3, axis=1)
    near_x, near_y = 2 - 2 * px, 2 - 2 * py
    levels = (
        (fine_ref, fine_rows, fine_y, fine_z, fine_sides, FINE_ROWS, 4, (1, near_x, 2 - near_x), (1, near_y, 2 - near_y)),
        (coarse_ref, coarse_rows, coarse_y, coarse_z, coarse_sides, COARSE_ROWS, 2, (1, 2 - near_x, near_x), (1, 2 - near_y, near_y)),
    )
    for copy in copies:
        copy.wait()
    for blocks, rows_out, y_out, z_out, sides_out, rows, nz, order_x, order_y in levels:
        spread_rows, spreads, mask = row_constants(rows, nz)

        def term(m, carry, blocks=blocks, rows_out=rows_out, y_out=y_out, z_out=z_out, sides_out=sides_out,
                 order_x=order_x, order_y=order_y, rows=rows,
                 spread_rows=spread_rows, spreads=spreads, mask=mask):
            wide = sum(dot(blocks[d, m], spreads[n]) for n, d in enumerate(order_x))
            rows_out[m] = (dot(spread_rows, wide.astype(BF)) * mask).astype(BF)
            wide_y = [dot(flipped(blocks[d, m]), lanes_y).astype(BF) for d in order_y]
            wide_z = [dot(flipped(blocks[d, m]), lanes_z).astype(BF) for d in (1, 2, 0)]
            mats = (dot(rows_y, jnp.concatenate(wide_y, axis=1)) * mask3_y).astype(BF)
            zero = jnp.zeros((128, 128), BF)
            for n in range(3):
                y_out[m, 128 * n:128 * n + 128, 0:128] = mats[:, 128 * n:128 * n + 128]
                y_out[m, 128 * n:128 * n + 128, 128:256] = zero
            y_out[m, 384:512, 0:128] = zero
            y_out[m, 384:512, 128:256] = mats[:, 0:128]
            mats = (dot(rows_z, jnp.concatenate(wide_z, axis=1)) * mask3_z).astype(BF)
            z_out[m] = mats[:, 0:128]
            sides_out[m] = mats[:, 128:384]
            return carry

        lax.fori_loop(0, TERMS, term, 0, unroll=6)

    first_child, second_child = child_ref[:, 0, :], child_ref[:, 1, :]

    def chosen(condition, a, b):
        return jnp.where(condition, a.astype(F32), b.astype(F32)).astype(BF)

    own_x, other_x = chosen(px == 0, first_child, second_child), chosen(px == 0, second_child, first_child)
    own_y, other_y = chosen(py == 0, first_child, second_child), chosen(py == 0, second_child, first_child)

    def lane_matrix(transposed, spread_rows, spread_lanes, mask):
        return (dot(spread_rows, dot(transposed, spread_lanes).astype(BF)) * mask).astype(BF)

    down_y[0:128, :] = lane_matrix(flipped(own_y), rows_y, lanes_y, mask_y)
    down_y[128:256, :] = lane_matrix(flipped(other_y), rows_y, lanes_y, mask_y)
    up_y[...] = lane_matrix(own_y, rows_y, lanes_y, mask_y)
    for c, child in enumerate((first_child, second_child)):
        down_z[128 * c:128 * c + 128, :] = lane_matrix(flipped(child), rows_z, lanes_z, mask_z)
        up_z[:, 128 * c:128 * c + 128] = lane_matrix(child, rows_z, lanes_z, mask_z)
    lane = iota((1, 160), 1)
    far = lane >= 80
    lane = jnp.where(far, lane - 80, lane)
    wide = dot(own_x, onehot(jnp.where(far, -1, lane >> 2) == iota((K2, 160), 0)))
    wide = wide + dot(other_x, onehot(jnp.where(far, lane >> 2, -1) == iota((K2, 160), 0)))
    r = iota((96, 1), 0)
    cz = jnp.where(r >= 48, 1, 0)
    r = r - 48 * cz
    mixed = dot(onehot((r >> 1) == iota((96, K2), 1)), wide.astype(BF))
    down_rows[...] = (mixed * onehot((2 * (r & 1) + cz) == (lane & 3), F32)).astype(BF)
    wide = dot(flipped(own_x), onehot((iota((1, 48), 1) >> 1) == iota((K2, 48), 0)))
    mixed = dot(onehot((iota((80, 1), 0) >> 2) == iota((80, K2), 1)), wide.astype(BF))
    keep = ((iota((80, 1), 0) & 3) >> 1) == (iota((1, 48), 1) & 1)
    up_rows[...] = (mixed * onehot(keep, F32)).astype(BF)


def build(fine_blocks, coarse_blocks, child):
    def s(*shape):
        return jax.ShapeDtypeStruct(shape, BF)

    out_shape = ()
    for rows in (FINE_ROWS, COARSE_ROWS):
        out_shape += (s(TERMS, rows, 3 * rows), s(TERMS, 512, 256), s(TERMS, 128, 128), s(TERMS, 128, 256))
    out_shape += (s(96, 160), s(256, 128), s(256, 128), s(80, 48), s(128, 128), s(128, 256))
    return pl.pallas_call(
        build_kernel, out_shape=out_shape, name="build",
        in_specs=[pl.BlockSpec(memory_space=pltpu.HBM)] * 3,
        scratch_shapes=[
            pltpu.VMEM((3, TERMS, K2, K2), BF), pltpu.VMEM((3, TERMS, K2, K2), BF),
            pltpu.VMEM((K2, 2, K2), BF), pltpu.SemaphoreType.DMA((3,)),
        ],
        compiler_params=pltpu.CompilerParams(vmem_limit_bytes=32 << 20),
        cost_estimate=pl.CostEstimate(flops=4 * 10**9, bytes_accessed=10 * 10**6, transcendentals=0),
    )(*(
        pltpu.with_memory_space_constraint(x, pltpu.HBM)
        for x in (fine_blocks, coarse_blocks, jnp.transpose(child, (1, 0, 2)))
    ))


def source_kernel(own, xnear, xfar, ynear, yfar, corner, down_rows, down_y, down_z,
                  along_x, along_y, parent, natural, pair, mixed, turned):
    select = onehot(iota((400, 512), 0) == natural_place(iota((1, 512), 1), True))

    def converted(ref, slot):
        values = ref[0, 0].astype(F32)
        for i in range(K2):
            natural[slot, 4 * i:4 * i + 4, :] = values[:, 400 * i:400 * i + 400]
        return dot(natural[slot].astype(BF), select).astype(BF)

    centre = converted(own, 0)
    x_near, y_near = converted(xnear, 1), converted(ynear, 2)
    diagonal = converted(corner, 3)
    along_x[0:80, :] = centre
    along_x[80:160, :] = x_near
    along_x[160:240, :] = converted(xfar, 4)
    along_y[:, 0:512] = centre
    along_y[:, 512:1024] = y_near
    along_y[:, 1024:1536] = converted(yfar, 5)
    pair[0:80, 0:512] = centre
    pair[80:160, 0:512] = x_near
    pair[0:80, 512:1024] = y_near
    pair[80:160, 512:1024] = diagonal
    rows = dot(down_rows[...], pair[...]).astype(BF)
    for b in range(4):
        for c in range(2):
            mixed[96 * b:96 * b + 96, 128 * c:128 * c + 128] = rows[:, 512 * c + 128 * b:512 * c + 128 * b + 128]
    summed = dot(mixed[...], down_y[...])
    blocks = exchange([summed[96 * b:96 * b + 96, :] for b in range(4)])
    for b in range(4):
        for c in range(2):
            turned[48 * b:48 * b + 48, 128 * c:128 * c + 128] = blocks[b][48 * c:48 * c + 48, :].astype(BF)
    total = dot(turned[...], down_z[...])
    blocks = exchange([total[48 * b:48 * b + 48, :] for b in range(4)])
    for b in range(4):
        parent[:, 128 * b:128 * b + 128] = blocks[b].astype(BF)


def source(columns, down_rows, down_y, down_z):
    out_shape = (
        jax.ShapeDtypeStruct((3 * FINE_ROWS, 512), BF),
        jax.ShapeDtypeStruct((FINE_ROWS, 1536), BF),
        jax.ShapeDtypeStruct((COARSE_ROWS, 512), BF),
    )
    scratch = [
        pltpu.VMEM((6, FINE_ROWS, 400), F32),
        pltpu.VMEM((2 * FINE_ROWS, 1024), BF),
        pltpu.VMEM((8 * COARSE_ROWS, 256), BF),
        pltpu.VMEM((4 * COARSE_ROWS, 256), BF),
    ]
    return pl.pallas_call(
        source_kernel, out_shape=out_shape, scratch_shapes=scratch, name="source",
        compiler_params=pltpu.CompilerParams(vmem_limit_bytes=16 << 20),
        cost_estimate=pl.CostEstimate(flops=10**9, bytes_accessed=10**6, transcendentals=0),
    )(*columns, down_rows, down_y, down_z)


def level_first(rows, along_x, along_y, row_mats, first):
    for m in range(TERMS):
        both = dot(row_mats[m], along_x)
        sides = dot(row_mats[m][:, 0:rows], along_y)
        for b in range(4):
            here = pl.ds(b * rows, rows)
            first[m, here, 0:128] = both[:, 128 * b:128 * b + 128].astype(BF)
            first[m, here, 128:256] = sides[:, 512 + 128 * b:640 + 128 * b].astype(BF)
            first[m, here, 256:384] = sides[:, 1024 + 128 * b:1152 + 128 * b].astype(BF)
            first[m, here, 384:512] = sides[:, 128 * b:128 * b + 128].astype(BF)


def level_rest(rows, nz, first, y_mats, z_mats, side_mats, sums, centres):
    for m in range(TERMS):
        result = dot(first[m], y_mats[m])
        for n, target in enumerate((sums, centres)):
            blocks = exchange([result[b * rows:(b + 1) * rows, 128 * n:128 * n + 128] for b in range(4)])
            for b in range(4):
                target[b * rows:(b + 1) * rows, 128 * m:128 * m + 128] = blocks[b].astype(BF)
    total = dot(sums[...], z_mats[...].reshape(TERMS * 128, 128))
    sides = dot(centres[...], side_mats[...].reshape(TERMS * 128, 256))
    z = iota((4 * rows, 128), 0) & (nz - 1)
    total = total + jnp.where(z == nz - 1, 0.0, pltpu.roll(sides[:, 0:128], 4 * rows - 1, 0))
    return total + jnp.where(z == 0, 0.0, pltpu.roll(sides[:, 128:256], 1, 0))


def level_scratch(rows):
    return [
        pltpu.VMEM((4 * rows, TERMS * 128), BF),
        pltpu.VMEM((4 * rows, TERMS * 128), BF),
    ]


def fine_first_kernel(along_x, along_y, row_mats, first):
    level_first(FINE_ROWS, along_x[...], along_y[...], row_mats, first)


def fine_first(along_x, along_y, row_mats):
    return pl.pallas_call(
        fine_first_kernel, out_shape=jax.ShapeDtypeStruct((TERMS, 4 * FINE_ROWS, 512), BF), name="fine_first",
        compiler_params=pltpu.CompilerParams(vmem_limit_bytes=16 << 20),
        cost_estimate=pl.CostEstimate(flops=2 * 10**9, bytes_accessed=10 * 10**6, transcendentals=0),
    )(along_x, along_y, row_mats)


def fine_rest_kernel(first, y_mats, z_mats, side_mats, out, sums, centres):
    out[...] = level_rest(FINE_ROWS, 4, first, y_mats, z_mats, side_mats, sums, centres)


def fine_rest(first, mats):
    return pl.pallas_call(
        fine_rest_kernel, out_shape=jax.ShapeDtypeStruct((4 * FINE_ROWS, 128), F32),
        scratch_shapes=level_scratch(FINE_ROWS), name="fine_rest",
        compiler_params=pltpu.CompilerParams(vmem_limit_bytes=16 << 20),
        cost_estimate=pl.CostEstimate(flops=4 * 10**9, bytes_accessed=10 * 10**6, transcendentals=0),
    )(first, *mats)


def coarse_kernel(own, xfar, xother, yfar, yother, row_mats, y_mats, z_mats, side_mats,
                  up_rows, up_y, up_z, fine_term, out, along_x, along_y, wide, grown, turned, split, first, *scratch):
    along_x[0:48, :] = own[...]
    along_x[48:96, :] = xfar[...]
    along_x[96:144, :] = xother[...]
    along_y[:, 0:512] = own[...]
    along_y[:, 512:1024] = yfar[...]
    along_y[:, 1024:1536] = yother[...]
    level_first(COARSE_ROWS, along_x[...], along_y[...], row_mats, first)
    result = level_rest(COARSE_ROWS, 2, first, y_mats, z_mats, side_mats, *scratch)
    blocks = exchange([result[48 * b:48 * b + 48, :] for b in range(4)])
    for b in range(4):
        wide[:, 128 * b:128 * b + 128] = blocks[b].astype(BF)
    part = dot(up_rows[...], wide[...]).astype(BF)
    for b in range(4):
        grown[80 * b:80 * b + 80, :] = part[:, 128 * b:128 * b + 128]
    part = dot(grown[...], up_y[...])
    blocks = exchange([part[80 * b:80 * b + 80, :] for b in range(4)])
    for b in range(4):
        turned[80 * b:80 * b + 80, :] = blocks[b].astype(BF)
    both = dot(turned[...], up_z[...])
    expanded = jnp.where((iota((320, 128), 0) & 1) == 0, both[:, 0:128], both[:, 128:256])
    total = fine_term[...] + expanded
    high = total.astype(BF)
    low = (total - high.astype(F32)).astype(BF)
    for b in range(4):
        split[0:80, 128 * b:128 * b + 128] = high[80 * b:80 * b + 80, :]
        split[80:160, 128 * b:128 * b + 128] = low[80 * b:80 * b + 80, :]
    select = onehot(natural_place(iota((512, 1), 0), False) == iota((512, 400), 1))
    natural = dot(split[...], select)
    natural = natural[0:80, :] + natural[80:160, :]
    for i in range(K2):
        out[0, 0, :, 400 * i:400 * i + 400] = natural[4 * i:4 * i + 4, :]


def coarse(parents, mats, up_rows, up_y, up_z, fine_term):
    scratch = [
        pltpu.VMEM((3 * COARSE_ROWS, 512), BF),
        pltpu.VMEM((COARSE_ROWS, 1536), BF),
        pltpu.VMEM((COARSE_ROWS, 512), BF),
        pltpu.VMEM((320, 128), BF),
        pltpu.VMEM((320, 128), BF),
        pltpu.VMEM((160, 512), BF),
        pltpu.VMEM((TERMS, 4 * COARSE_ROWS, 512), BF),
    ] + level_scratch(COARSE_ROWS)
    return pl.pallas_call(
        coarse_kernel, out_shape=jax.ShapeDtypeStruct((1, 1, 4, 8000), F32),
        scratch_shapes=scratch, name="coarse",
        compiler_params=pltpu.CompilerParams(vmem_limit_bytes=32 << 20),
        cost_estimate=pl.CostEstimate(flops=4 * 10**9, bytes_accessed=10 * 10**6, transcendentals=0),
    )(*parents, *mats, up_rows, up_y, up_z, fine_term)


def near(block, axis):
    return lax.ppermute(block, axis, [(i, i ^ 1) for i in range(lax.axis_size(axis))])


def far(block, axis):
    count = lax.axis_size(axis)
    return lax.ppermute(block, axis, [(i, ((i + 1) ^ 1) - 1) for i in range(1, count - 1)])


def corner(block):
    nx, ny = lax.axis_size("gx"), lax.axis_size("gy")
    route = [(x * ny + y, (x ^ 1) * ny + (y ^ 1)) for x in range(nx) for y in range(ny)]
    return lax.ppermute(block, ("gx", "gy"), route)


def shards(fine_source, fine_blocks, coarse_blocks, child_filter_matrices):
    columns = [fine_source, near(fine_source, "gx"), far(fine_source, "gx"),
               near(fine_source, "gy"), far(fine_source, "gy"), corner(fine_source)]
    built = build(fine_blocks, coarse_blocks, child_filter_matrices)
    along_x, along_y, parent = source(columns, *built[8:11])
    x_far, y_far = far(parent, "gx"), far(parent, "gy")
    first = fine_first(along_x, along_y, built[0])
    x_far, y_far, first = lax.optimization_barrier((x_far, y_far, first))
    fine_term = fine_rest(first, built[1:4])
    parents = [parent, x_far, near(x_far, "gx"), y_far, near(y_far, "gy")]
    return coarse(parents, built[4:8], *built[11:14], fine_term)


def solution(mesh):
    in_specs = (P("gx", "gy", None, None), P(), P(), P())
    out_specs = P("gx", "gy", None, None)
    return jax.shard_map(shards, mesh=mesh, in_specs=in_specs, out_specs=out_specs, check_vma=False)
```

```python
import jax
import jax.numpy as jnp
from jax import lax
from jax.experimental import pallas as pl
from jax.experimental.pallas import tpu as pltpu
from jax.sharding import PartitionSpec as P

K2 = 20
TERMS = 12
BF = jnp.bfloat16
F32 = jnp.float32
FINE_ROWS = 80
COARSE_ROWS = 48


def iota(shape, dim):
    return lax.broadcasted_iota(jnp.int32, shape, dim)


def dot(a, b):
    return jnp.dot(a, b, preferred_element_type=F32)


def place(n):
    piece, t = n >> 5, n & 31
    jj = (t * 13) >> 6
    return piece, jj, t - 5 * jj, t < 25


def natural_place(n, y_order):
    block = n >> 7
    piece, jj, kk, ok = place(n & 127)
    j, k = (piece, block) if y_order else (block, piece)
    return jnp.where(ok, (5 * j + jj) * 20 + 5 * k + kk, -1)


def onehot(condition, dtype=BF):
    return jnp.where(condition, 1.0, 0.0).astype(dtype)


def lane_constants(on_j):
    def index(n):
        piece, jj, kk, ok = place(n)
        return jnp.where(ok, piece * 5 + (jj if on_j else kk), -1)

    def fixed(n, none):
        _, jj, kk, ok = place(n)
        return jnp.where(ok, kk if on_j else jj, none)

    spread_rows = onehot(index(iota((128, 1), 0)) == iota((128, 32), 1))
    spread_lanes = onehot(index(iota((1, 128), 1)) == iota((K2, 128), 0))
    mask = onehot(fixed(iota((128, 1), 0), -1) == fixed(iota((1, 128), 1), -2), F32)
    return spread_rows, spread_lanes, mask


def row_constants(rows, nz):
    shift = nz.bit_length() - 1
    spread_rows = onehot((iota((rows, 1), 0) >> shift) == iota((rows, 32), 1))
    wide = 256
    lane = iota((1, wide), 1)
    which = sum(jnp.where(lane >= c * rows, 1, 0) for c in range(1, 4))
    lane = lane - which * rows
    spreads = [
        onehot(jnp.where(which == c, lane >> shift, -1) == iota((K2, wide), 0)) for c in range(3)
    ]
    mask = onehot((iota((rows, 1), 0) & (nz - 1)) == (lane & (nz - 1)), F32)
    return spread_rows, spreads, mask


def flipped(matrix):
    return matrix.astype(F32).T.astype(BF)


def exchange(tiles):
    lane = iota((1, 128), 1)
    low = (lane & 64) == 0
    a, b, c, d = tiles
    a, c = jnp.where(low, a, pltpu.roll(c, 64, 1)), jnp.where(low, pltpu.roll(a, 64, 1), c)
    b, d = jnp.where(low, b, pltpu.roll(d, 64, 1)), jnp.where(low, pltpu.roll(b, 64, 1), d)
    low = (lane & 32) == 0
    a, b = jnp.where(low, a, pltpu.roll(b, 32, 1)), jnp.where(low, pltpu.roll(a, 96, 1), b)
    c, d = jnp.where(low, c, pltpu.roll(d, 32, 1)), jnp.where(low, pltpu.roll(c, 96, 1), d)
    return a, b, c, d


def build_kernel(fine_hbm, coarse_hbm, child_hbm, *refs):
    (fine_rows, fine_y, fine_z, coarse_rows, coarse_y, coarse_z,
     down_rows, down_y, down_z, up_rows, up_y, up_z,
     fine_ref, coarse_ref, child_ref, plain, turned, wide_y, wide_z, wide_rows, sems) = refs
    copies = [
        pltpu.make_async_copy(src, dst, sems.at[n])
        for n, (src, dst) in enumerate(((fine_hbm, fine_ref), (coarse_hbm, coarse_ref), (child_hbm, child_ref)))
    ]
    for copy in copies:
        copy.start()
    plain[...] = jnp.zeros(plain.shape, F32)
    turned[...] = jnp.zeros(turned.shape, F32)
    px, py = lax.axis_index("gx") & 1, lax.axis_index("gy") & 1
    rows_y, lanes_y, mask_y = lane_constants(True)
    rows_z, lanes_z, mask_z = lane_constants(False)
    both = jnp.concatenate([lanes_y, lanes_z], axis=1)
    near_x, near_y = 2 - 2 * px, 2 - 2 * py
    levels = (
        (fine_ref, fine_rows, fine_y, fine_z, FINE_ROWS, 4, (1, near_x, 2 - near_x), (1, near_y, 2 - near_y)),
        (coarse_ref, coarse_rows, coarse_y, coarse_z, COARSE_ROWS, 2, (1, 2 - near_x, near_x), (1, 2 - near_y, near_y)),
    )
    for copy in copies:
        copy.wait()
    for n, blocks in enumerate((fine_ref, coarse_ref)):
        for d in range(3):
            for m in range(TERMS):
                matrix = blocks[d, m].astype(F32)
                plain[n, d, m, 0:K2, :] = matrix
                turned[n, d, m, 0:K2, :] = matrix.T
    for n, (blocks, rows_out, y_out, z_out, rows, nz, order_x, order_y) in enumerate(levels):
        spread_rows, spreads, mask = row_constants(rows, nz)
        count = 3 * TERMS * 32
        wide = dot(turned[n].reshape(count, K2).astype(BF), both).astype(BF)
        wide_y[n] = wide[:, 0:128].reshape(3, TERMS, 32, 128)
        wide_z[n] = wide[:, 128:256].reshape(3, TERMS, 32, 128)
        wide = sum(dot(plain[n, d].reshape(TERMS * 32, K2).astype(BF), spreads[c]) for c, d in enumerate(order_x))
        wide_rows[...] = wide.astype(BF).reshape(TERMS, 32, 256)
        for m in range(TERMS):
            mats = (dot(spread_rows, wide_rows[m]) * mask).astype(BF)
            for c in range(2):
                rows_out[m, c] = mats[:, 128 * c:128 * c + 128]
        for spread, mask, source_ref, order, out in (
            (rows_y, mask_y, wide_y, order_y, y_out), (rows_z, mask_z, wide_z, (1, 2, 0), z_out),
        ):
            for m in range(0, TERMS, 2):
                tiles = [source_ref[n, d, m + c] for c in range(2) for d in order]
                mats = dot(spread, jnp.concatenate(tiles, axis=1))
                for c in range(2):
                    for e in range(3):
                        lane = 384 * c + 128 * e
                        tile = (mats[:, lane:lane + 128] * mask).astype(BF)
                        if out is y_out:
                            out[m + c, e] = tile
                        else:
                            out[e, m + c] = tile

    first_child, second_child = child_ref[:, 0, :], child_ref[:, 1, :]

    def chosen(condition, a, b):
        return jnp.where(condition, a.astype(F32), b.astype(F32)).astype(BF)

    own_x, other_x = chosen(px == 0, first_child, second_child), chosen(px == 0, second_child, first_child)
    own_y, other_y = chosen(py == 0, first_child, second_child), chosen(py == 0, second_child, first_child)

    def lane_matrix(transposed, spread_rows, spread_lanes, mask):
        return (dot(spread_rows[:, 0:K2], dot(transposed, spread_lanes).astype(BF)) * mask).astype(BF)

    down_y[0:128, :] = lane_matrix(flipped(own_y), rows_y, lanes_y, mask_y)
    down_y[128:256, :] = lane_matrix(flipped(other_y), rows_y, lanes_y, mask_y)
    up_y[...] = lane_matrix(own_y, rows_y, lanes_y, mask_y)
    for c, child in enumerate((first_child, second_child)):
        down_z[128 * c:128 * c + 128, :] = lane_matrix(flipped(child), rows_z, lanes_z, mask_z)
        up_z[c] = lane_matrix(child, rows_z, lanes_z, mask_z)
    lane = iota((1, 160), 1)
    far = lane >= 80
    lane = jnp.where(far, lane - 80, lane)
    wide = dot(own_x, onehot(jnp.where(far, -1, lane >> 2) == iota((K2, 160), 0)))
    wide = wide + dot(other_x, onehot(jnp.where(far, lane >> 2, -1) == iota((K2, 160), 0)))
    r = iota((96, 1), 0)
    cz = jnp.where(r >= 48, 1, 0)
    r = r - 48 * cz
    mixed = dot(onehot((r >> 1) == iota((96, K2), 1)), wide.astype(BF))
    down_rows[...] = (mixed * onehot((2 * (r & 1) + cz) == (lane & 3), F32)).astype(BF)
    wide = dot(flipped(own_x), onehot((iota((1, 48), 1) >> 1) == iota((K2, 48), 0)))
    mixed = dot(onehot((iota((80, 1), 0) >> 2) == iota((80, K2), 1)), wide.astype(BF))
    keep = ((iota((80, 1), 0) & 3) >> 1) == (iota((1, 48), 1) & 1)
    up_rows[...] = (mixed * onehot(keep, F32)).astype(BF)


def build(fine_blocks, coarse_blocks, child):
    def s(*shape):
        return jax.ShapeDtypeStruct(shape, BF)

    out_shape = ()
    for rows in (FINE_ROWS, COARSE_ROWS):
        out_shape += (s(TERMS, 2, rows, 128), s(TERMS, 3, 128, 128), s(3, TERMS, 128, 128))
    out_shape += (s(96, 160), s(256, 128), s(256, 128), s(80, 48), s(128, 128), s(2, 128, 128))
    return pl.pallas_call(
        build_kernel, out_shape=out_shape, name="build",
        in_specs=[pl.BlockSpec(memory_space=pltpu.HBM)] * 3,
        scratch_shapes=[
            pltpu.VMEM((3, TERMS, K2, K2), BF), pltpu.VMEM((3, TERMS, K2, K2), BF),
            pltpu.VMEM((K2, 2, K2), BF),
            pltpu.VMEM((2, 3, TERMS, 32, K2), F32), pltpu.VMEM((2, 3, TERMS, 32, K2), F32),
            pltpu.VMEM((2, 3, TERMS, 32, 128), BF), pltpu.VMEM((2, 3, TERMS, 32, 128), BF),
            pltpu.VMEM((TERMS, 32, 256), BF), pltpu.SemaphoreType.DMA((3,)),
        ],
        compiler_params=pltpu.CompilerParams(vmem_limit_bytes=32 << 20),
        cost_estimate=pl.CostEstimate(flops=4 * 10**9, bytes_accessed=10 * 10**6, transcendentals=0),
    )(*(
        pltpu.with_memory_space_constraint(x, pltpu.HBM)
        for x in (fine_blocks, coarse_blocks, jnp.transpose(child, (1, 0, 2)))
    ))


def source_kernel(own, xnear, xfar, ynear, yfar, corner, down_rows, down_y, down_z,
                  along_x, along_y, parent, natural, pair, mixed, turned):
    select = onehot(iota((400, 512), 0) == natural_place(iota((1, 512), 1), True))

    def converted(ref, slot):
        values = ref[0, 0].astype(F32)
        for i in range(K2):
            natural[slot, 4 * i:4 * i + 4, :] = values[:, 400 * i:400 * i + 400]
        return dot(natural[slot].astype(BF), select).astype(BF)

    centre = converted(own, 0)
    x_near, y_near = converted(xnear, 1), converted(ynear, 2)
    diagonal = converted(corner, 3)
    along_x[0:80, :] = centre
    along_x[80:160, :] = x_near
    along_x[160:240, :] = converted(xfar, 4)
    along_y[:, 0:512] = centre
    along_y[:, 512:1024] = y_near
    along_y[:, 1024:1536] = converted(yfar, 5)
    pair[0:80, 0:512] = centre
    pair[80:160, 0:512] = x_near
    pair[0:80, 512:1024] = y_near
    pair[80:160, 512:1024] = diagonal
    rows = dot(down_rows[...], pair[...]).astype(BF)
    for b in range(4):
        for c in range(2):
            mixed[96 * b:96 * b + 96, 128 * c:128 * c + 128] = rows[:, 512 * c + 128 * b:512 * c + 128 * b + 128]
    summed = dot(mixed[...], down_y[...])
    blocks = exchange([summed[96 * b:96 * b + 96, :] for b in range(4)])
    for b in range(4):
        for c in range(2):
            turned[48 * b:48 * b + 48, 128 * c:128 * c + 128] = blocks[b][48 * c:48 * c + 48, :].astype(BF)
    total = dot(turned[...], down_z[...])
    blocks = exchange([total[48 * b:48 * b + 48, :] for b in range(4)])
    for b in range(4):
        parent[:, 128 * b:128 * b + 128] = blocks[b].astype(BF)


def source(columns, down_rows, down_y, down_z):
    out_shape = (
        jax.ShapeDtypeStruct((3 * FINE_ROWS, 512), BF),
        jax.ShapeDtypeStruct((FINE_ROWS, 1536), BF),
        jax.ShapeDtypeStruct((COARSE_ROWS, 512), BF),
    )
    scratch = [
        pltpu.VMEM((6, FINE_ROWS, 400), F32),
        pltpu.VMEM((2 * FINE_ROWS, 1024), BF),
        pltpu.VMEM((8 * COARSE_ROWS, 256), BF),
        pltpu.VMEM((4 * COARSE_ROWS, 256), BF),
    ]
    return pl.pallas_call(
        source_kernel, out_shape=out_shape, scratch_shapes=scratch, name="source",
        compiler_params=pltpu.CompilerParams(vmem_limit_bytes=16 << 20),
        cost_estimate=pl.CostEstimate(flops=10**9, bytes_accessed=10**6, transcendentals=0),
    )(*columns, down_rows, down_y, down_z)


def level_first(rows, along_x, along_y, row_mats, first):
    for m in range(TERMS):
        mats = jnp.concatenate([row_mats[m, 0], row_mats[m, 1]], axis=1)[:, 0:3 * rows]
        both = dot(mats, along_x)
        sides = dot(mats[:, 0:rows], along_y)
        for b in range(4):
            here = pl.ds(b * rows, rows)
            first[m, 0, here, :] = both[:, 128 * b:128 * b + 128].astype(BF)
            for part, start in ((1, 512), (2, 1024), (3, 0)):
                first[m, part, here, :] = sides[:, start + 128 * b:start + 128 * b + 128].astype(BF)


def level_rest(rows, nz, first, y_mats, z_mats, sums, centres):
    zero = jnp.zeros((128, 128), BF)
    for m in range(TERMS):
        mats = jnp.concatenate([
            jnp.concatenate([y_mats[m, 0], y_mats[m, 1], y_mats[m, 2], zero], axis=0),
            jnp.concatenate([zero, zero, zero, y_mats[m, 0]], axis=0),
        ], axis=1)
        result = dot(jnp.concatenate([first[m, part] for part in range(4)], axis=1), mats)
        for n, target in enumerate((sums, centres)):
            blocks = exchange([result[b * rows:(b + 1) * rows, 128 * n:128 * n + 128] for b in range(4)])
            for b in range(4):
                target[m, b * rows:(b + 1) * rows, :] = blocks[b].astype(BF)
    total = dot(jnp.concatenate([sums[m] for m in range(TERMS)], axis=1), z_mats[0].reshape(TERMS * 128, 128))
    sides = dot(
        jnp.concatenate([centres[m] for m in range(TERMS)], axis=1),
        jnp.concatenate([z_mats[n].reshape(TERMS * 128, 128) for n in (1, 2)], axis=1),
    )
    z = iota((4 * rows, 128), 0) & (nz - 1)
    total = total + jnp.where(z == nz - 1, 0.0, pltpu.roll(sides[:, 0:128], 4 * rows - 1, 0))
    return total + jnp.where(z == 0, 0.0, pltpu.roll(sides[:, 128:256], 1, 0))


def level_scratch(rows):
    return [
        pltpu.VMEM((TERMS, 4 * rows, 128), BF),
        pltpu.VMEM((TERMS, 4 * rows, 128), BF),
    ]


def fine_first_kernel(along_x, along_y, row_mats, first):
    level_first(FINE_ROWS, along_x[...], along_y[...], row_mats, first)


def fine_first(along_x, along_y, row_mats):
    return pl.pallas_call(
        fine_first_kernel, out_shape=jax.ShapeDtypeStruct((TERMS, 4, 4 * FINE_ROWS, 128), BF), name="fine_first",
        compiler_params=pltpu.CompilerParams(vmem_limit_bytes=16 << 20),
        cost_estimate=pl.CostEstimate(flops=2 * 10**9, bytes_accessed=10 * 10**6, transcendentals=0),
    )(along_x, along_y, row_mats)


def fine_rest_kernel(first, y_mats, z_mats, out, sums, centres):
    out[...] = level_rest(FINE_ROWS, 4, first, y_mats, z_mats, sums, centres)


def fine_rest(first, mats):
    return pl.pallas_call(
        fine_rest_kernel, out_shape=jax.ShapeDtypeStruct((4 * FINE_ROWS, 128), F32),
        scratch_shapes=level_scratch(FINE_ROWS), name="fine_rest",
        compiler_params=pltpu.CompilerParams(vmem_limit_bytes=16 << 20),
        cost_estimate=pl.CostEstimate(flops=4 * 10**9, bytes_accessed=10 * 10**6, transcendentals=0),
    )(first, *mats)


def coarse_kernel(own, xfar, xother, yfar, yother, row_mats, y_mats, z_mats,
                  up_rows, up_y, up_z, fine_term, out, along_x, along_y, wide, grown, turned, split, first, *scratch):
    along_x[0:48, :] = own[...]
    along_x[48:96, :] = xfar[...]
    along_x[96:144, :] = xother[...]
    along_y[:, 0:512] = own[...]
    along_y[:, 512:1024] = yfar[...]
    along_y[:, 1024:1536] = yother[...]
    level_first(COARSE_ROWS, along_x[...], along_y[...], row_mats, first)
    result = level_rest(COARSE_ROWS, 2, first, y_mats, z_mats, *scratch)
    blocks = exchange([result[48 * b:48 * b + 48, :] for b in range(4)])
    for b in range(4):
        wide[:, 128 * b:128 * b + 128] = blocks[b].astype(BF)
    part = dot(up_rows[...], wide[...]).astype(BF)
    for b in range(4):
        grown[80 * b:80 * b + 80, :] = part[:, 128 * b:128 * b + 128]
    part = dot(grown[...], up_y[...])
    blocks = exchange([part[80 * b:80 * b + 80, :] for b in range(4)])
    for b in range(4):
        turned[80 * b:80 * b + 80, :] = blocks[b].astype(BF)
    both = dot(turned[...], jnp.concatenate([up_z[0], up_z[1]], axis=1))
    expanded = jnp.where((iota((320, 128), 0) & 1) == 0, both[:, 0:128], both[:, 128:256])
    total = fine_term[...] + expanded
    high = total.astype(BF)
    low = (total - high.astype(F32)).astype(BF)
    for b in range(4):
        split[0:80, 128 * b:128 * b + 128] = high[80 * b:80 * b + 80, :]
        split[80:160, 128 * b:128 * b + 128] = low[80 * b:80 * b + 80, :]
    select = onehot(natural_place(iota((512, 1), 0), False) == iota((512, 400), 1))
    natural = dot(split[...], select)
    natural = natural[0:80, :] + natural[80:160, :]
    for i in range(K2):
        out[0, 0, :, 400 * i:400 * i + 400] = natural[4 * i:4 * i + 4, :]


def coarse(parents, mats, up_rows, up_y, up_z, fine_term):
    scratch = [
        pltpu.VMEM((3 * COARSE_ROWS, 512), BF),
        pltpu.VMEM((COARSE_ROWS, 1536), BF),
        pltpu.VMEM((COARSE_ROWS, 512), BF),
        pltpu.VMEM((320, 128), BF),
        pltpu.VMEM((320, 128), BF),
        pltpu.VMEM((160, 512), BF),
        pltpu.VMEM((TERMS, 4, 4 * COARSE_ROWS, 128), BF),
    ] + level_scratch(COARSE_ROWS)
    return pl.pallas_call(
        coarse_kernel, out_shape=jax.ShapeDtypeStruct((1, 1, 4, 8000), F32),
        scratch_shapes=scratch, name="coarse",
        compiler_params=pltpu.CompilerParams(vmem_limit_bytes=32 << 20),
        cost_estimate=pl.CostEstimate(flops=4 * 10**9, bytes_accessed=10 * 10**6, transcendentals=0),
    )(*parents, *mats, up_rows, up_y, up_z, fine_term)


def near(block, axis):
    return lax.ppermute(block, axis, [(i, i ^ 1) for i in range(lax.axis_size(axis))])


def far(block, axis):
    count = lax.axis_size(axis)
    return lax.ppermute(block, axis, [(i, ((i + 1) ^ 1) - 1) for i in range(1, count - 1)])


def corner(block):
    nx, ny = lax.axis_size("gx"), lax.axis_size("gy")
    route = [(x * ny + y, (x ^ 1) * ny + (y ^ 1)) for x in range(nx) for y in range(ny)]
    return lax.ppermute(block, ("gx", "gy"), route)


def shards(fine_source, fine_blocks, coarse_blocks, child_filter_matrices):
    columns = [fine_source, near(fine_source, "gx"), far(fine_source, "gx"),
               near(fine_source, "gy"), far(fine_source, "gy"), corner(fine_source)]
    built = build(fine_blocks, coarse_blocks, child_filter_matrices)
    along_x, along_y, parent = source(columns, *built[6:9])
    x_far, y_far = far(parent, "gx"), far(parent, "gy")
    first = fine_first(along_x, along_y, built[0])
    x_far, y_far, first = lax.optimization_barrier((x_far, y_far, first))
    fine_term = fine_rest(first, built[1:3])
    parents = [parent, x_far, near(x_far, "gx"), y_far, near(y_far, "gy")]
    return coarse(parents, built[3:6], *built[9:12], fine_term)


def solution(mesh):
    in_specs = (P("gx", "gy", None, None), P(), P(), P())
    out_specs = P("gx", "gy", None, None)
    return jax.shard_map(shards, mesh=mesh, in_specs=in_specs, out_specs=out_specs, check_vma=False)
```

```python
import jax
import jax.numpy as jnp
from jax import lax
from jax.experimental import pallas as pl
from jax.experimental.pallas import tpu as pltpu
from jax.sharding import PartitionSpec as P

K2 = 20
TERMS = 12
BF = jnp.bfloat16
F32 = jnp.float32
FINE_ROWS = 80
COARSE_ROWS = 48


def iota(shape, dim):
    return lax.broadcasted_iota(jnp.int32, shape, dim)


def dot(a, b):
    return jnp.dot(a, b, preferred_element_type=F32)


def place(n):
    piece, t = n >> 5, n & 31
    jj = (t * 13) >> 6
    return piece, jj, t - 5 * jj, t < 25


def natural_place(n, y_order):
    block = n >> 7
    piece, jj, kk, ok = place(n & 127)
    j, k = (piece, block) if y_order else (block, piece)
    return jnp.where(ok, (5 * j + jj) * 20 + 5 * k + kk, -1)


def onehot(condition, dtype=BF):
    return jnp.where(condition, 1.0, 0.0).astype(dtype)


def lane_constants(on_j):
    def index(n):
        piece, jj, kk, ok = place(n)
        return jnp.where(ok, piece * 5 + (jj if on_j else kk), -1)

    def fixed(n, none):
        _, jj, kk, ok = place(n)
        return jnp.where(ok, kk if on_j else jj, none)

    spread_rows = onehot(index(iota((128, 1), 0)) == iota((128, 32), 1))
    spread_lanes = onehot(index(iota((1, 128), 1)) == iota((K2, 128), 0))
    mask = onehot(fixed(iota((128, 1), 0), -1) == fixed(iota((1, 128), 1), -2), F32)
    return spread_rows, spread_lanes, mask


def row_constants(rows, nz):
    shift = nz.bit_length() - 1
    spread_rows = onehot((iota((rows, 1), 0) >> shift) == iota((rows, 32), 1))
    wide = 256
    lane = iota((1, wide), 1)
    which = sum(jnp.where(lane >= c * rows, 1, 0) for c in range(1, 4))
    lane = lane - which * rows
    spreads = [
        onehot(jnp.where(which == c, lane >> shift, -1) == iota((K2, wide), 0)) for c in range(3)
    ]
    mask = onehot((iota((rows, 1), 0) & (nz - 1)) == (lane & (nz - 1)), F32)
    return spread_rows, spreads, mask


def flipped(matrix):
    return matrix.astype(F32).T.astype(BF)


def exchange(tiles):
    lane = iota((1, 128), 1)
    low = (lane & 64) == 0
    a, b, c, d = tiles
    a, c = jnp.where(low, a, pltpu.roll(c, 64, 1)), jnp.where(low, pltpu.roll(a, 64, 1), c)
    b, d = jnp.where(low, b, pltpu.roll(d, 64, 1)), jnp.where(low, pltpu.roll(b, 64, 1), d)
    low = (lane & 32) == 0
    a, b = jnp.where(low, a, pltpu.roll(b, 32, 1)), jnp.where(low, pltpu.roll(a, 96, 1), b)
    c, d = jnp.where(low, c, pltpu.roll(d, 32, 1)), jnp.where(low, pltpu.roll(c, 96, 1), d)
    return a, b, c, d


def build_kernel(fine_hbm, coarse_hbm, child_hbm, *refs):
    (fine_rows, fine_y, fine_z, coarse_rows, coarse_y, coarse_z,
     down_rows, down_y, down_z, up_rows, up_y, up_z,
     fine_ref, coarse_ref, child_ref, plain, turned, wide_y, wide_z, wide_rows, sems) = refs
    copies = [
        pltpu.make_async_copy(src, dst, sems.at[n])
        for n, (src, dst) in enumerate(((fine_hbm, fine_ref), (coarse_hbm, coarse_ref), (child_hbm, child_ref)))
    ]
    for copy in copies:
        copy.start()
    plain[...] = jnp.zeros(plain.shape, F32)
    turned[...] = jnp.zeros(turned.shape, F32)
    px, py = lax.axis_index("gx") & 1, lax.axis_index("gy") & 1
    rows_y, lanes_y, mask_y = lane_constants(True)
    rows_z, lanes_z, mask_z = lane_constants(False)
    both = jnp.concatenate([lanes_y, lanes_z], axis=1)
    near_x, near_y = 2 - 2 * px, 2 - 2 * py
    levels = (
        (fine_ref, fine_rows, fine_y, fine_z, FINE_ROWS, 4, (1, near_x, 2 - near_x), (1, near_y, 2 - near_y)),
        (coarse_ref, coarse_rows, coarse_y, coarse_z, COARSE_ROWS, 2, (1, 2 - near_x, near_x), (1, 2 - near_y, near_y)),
    )
    for copy in copies:
        copy.wait()
    for n, blocks in enumerate((fine_ref, coarse_ref)):
        for d in range(3):
            for m in range(TERMS):
                matrix = blocks[d, m].astype(F32)
                plain[n, d, m, 0:K2, :] = matrix
                turned[n, d, m, 0:K2, :] = matrix.T
    for n, (blocks, rows_out, y_out, z_out, rows, nz, order_x, order_y) in enumerate(levels):
        spread_rows, spreads, mask = row_constants(rows, nz)
        count = 3 * TERMS * 32
        wide = dot(turned[n].reshape(count, K2).astype(BF), both).astype(BF)
        wide_y[n] = wide[:, 0:128].reshape(3, TERMS, 32, 128)
        wide_z[n] = wide[:, 128:256].reshape(3, TERMS, 32, 128)
        wide = sum(dot(plain[n, d].reshape(TERMS * 32, K2).astype(BF), spreads[c]) for c, d in enumerate(order_x))
        wide_rows[...] = wide.astype(BF).reshape(TERMS, 32, 256)
        for m in range(TERMS):
            mats = (dot(spread_rows, wide_rows[m]) * mask).astype(BF)
            for c in range(2):
                rows_out[m, c] = mats[:, 128 * c:128 * c + 128]
        for spread, mask, source_ref, order, out in (
            (rows_y, mask_y, wide_y, order_y, y_out), (rows_z, mask_z, wide_z, (1, 2, 0), z_out),
        ):
            for m in range(0, TERMS, 2):
                tiles = [source_ref[n, d, m + c] for c in range(2) for d in order]
                mats = dot(spread, jnp.concatenate(tiles, axis=1))
                for c in range(2):
                    for e in range(3):
                        lane = 384 * c + 128 * e
                        tile = (mats[:, lane:lane + 128] * mask).astype(BF)
                        if out is y_out:
                            out[m + c, e] = tile
                        else:
                            out[e, m + c] = tile

    first_child, second_child = child_ref[:, 0, :], child_ref[:, 1, :]

    def chosen(condition, a, b):
        return jnp.where(condition, a.astype(F32), b.astype(F32)).astype(BF)

    own_x, other_x = chosen(px == 0, first_child, second_child), chosen(px == 0, second_child, first_child)
    own_y, other_y = chosen(py == 0, first_child, second_child), chosen(py == 0, second_child, first_child)

    def lane_matrix(transposed, spread_rows, spread_lanes, mask):
        return (dot(spread_rows[:, 0:K2], dot(transposed, spread_lanes).astype(BF)) * mask).astype(BF)

    down_y[0:128, :] = lane_matrix(flipped(own_y), rows_y, lanes_y, mask_y)
    down_y[128:256, :] = lane_matrix(flipped(other_y), rows_y, lanes_y, mask_y)
    up_y[...] = lane_matrix(own_y, rows_y, lanes_y, mask_y)
    for c, child in enumerate((first_child, second_child)):
        down_z[128 * c:128 * c + 128, :] = lane_matrix(flipped(child), rows_z, lanes_z, mask_z)
        up_z[c] = lane_matrix(child, rows_z, lanes_z, mask_z)
    lane = iota((1, 160), 1)
    far = lane >= 80
    lane = jnp.where(far, lane - 80, lane)
    wide = dot(own_x, onehot(jnp.where(far, -1, lane >> 2) == iota((K2, 160), 0)))
    wide = wide + dot(other_x, onehot(jnp.where(far, lane >> 2, -1) == iota((K2, 160), 0)))
    r = iota((96, 1), 0)
    cz = jnp.where(r >= 48, 1, 0)
    r = r - 48 * cz
    mixed = dot(onehot((r >> 1) == iota((96, K2), 1)), wide.astype(BF))
    down_rows[...] = (mixed * onehot((2 * (r & 1) + cz) == (lane & 3), F32)).astype(BF)
    wide = dot(flipped(own_x), onehot((iota((1, 48), 1) >> 1) == iota((K2, 48), 0)))
    mixed = dot(onehot((iota((80, 1), 0) >> 2) == iota((80, K2), 1)), wide.astype(BF))
    keep = ((iota((80, 1), 0) & 3) >> 1) == (iota((1, 48), 1) & 1)
    up_rows[...] = (mixed * onehot(keep, F32)).astype(BF)


def build(fine_blocks, coarse_blocks, child):
    def s(*shape):
        return jax.ShapeDtypeStruct(shape, BF)

    out_shape = ()
    for rows in (FINE_ROWS, COARSE_ROWS):
        out_shape += (s(TERMS, 2, rows, 128), s(TERMS, 3, 128, 128), s(3, TERMS, 128, 128))
    out_shape += (s(96, 160), s(256, 128), s(256, 128), s(80, 48), s(128, 128), s(2, 128, 128))
    return pl.pallas_call(
        build_kernel, out_shape=out_shape, name="build",
        in_specs=[pl.BlockSpec(memory_space=pltpu.HBM)] * 3,
        scratch_shapes=[
            pltpu.VMEM((3, TERMS, K2, K2), BF), pltpu.VMEM((3, TERMS, K2, K2), BF),
            pltpu.VMEM((K2, 2, K2), BF),
            pltpu.VMEM((2, 3, TERMS, 32, K2), F32), pltpu.VMEM((2, 3, TERMS, 32, K2), F32),
            pltpu.VMEM((2, 3, TERMS, 32, 128), BF), pltpu.VMEM((2, 3, TERMS, 32, 128), BF),
            pltpu.VMEM((TERMS, 32, 256), BF), pltpu.SemaphoreType.DMA((3,)),
        ],
        compiler_params=pltpu.CompilerParams(vmem_limit_bytes=32 << 20),
        cost_estimate=pl.CostEstimate(flops=4 * 10**9, bytes_accessed=10 * 10**6, transcendentals=0),
    )(*(
        pltpu.with_memory_space_constraint(x, pltpu.HBM)
        for x in (fine_blocks, coarse_blocks, jnp.transpose(child, (1, 0, 2)))
    ))


def source_kernel(own, xnear, ynear, corner, down_rows, down_y, down_z,
                  packet, nears, natural, mixed, turned):
    select = onehot(iota((400, 512), 0) == natural_place(iota((1, 512), 1), True))

    def converted(ref, slot):
        values = ref[0, 0].astype(F32)
        for i in range(K2):
            natural[slot, 4 * i:4 * i + 4, :] = values[:, 400 * i:400 * i + 400]
        return dot(natural[slot].astype(BF), select).astype(BF)

    centre, diagonal = converted(own, 0), converted(corner, 1)
    x_near, y_near = converted(xnear, 2), converted(ynear, 3)
    for b in range(4):
        here = slice(128 * b, 128 * b + 128)
        packet[b, 0:80, :] = centre[:, here]
        nears[0, b] = x_near[:, here]
        nears[1, b] = y_near[:, here]
    for c, (one, two) in enumerate(((centre, x_near), (y_near, diagonal))):
        rows = dot(down_rows[...], jnp.concatenate([one, two], axis=0)).astype(BF)
        for b in range(4):
            mixed[c, 96 * b:96 * b + 96, :] = rows[:, 128 * b:128 * b + 128]
    summed = dot(jnp.concatenate([mixed[0], mixed[1]], axis=1), down_y[...])
    blocks = exchange([summed[96 * b:96 * b + 96, :] for b in range(4)])
    for b in range(4):
        for c in range(2):
            turned[c, 48 * b:48 * b + 48, :] = blocks[b][48 * c:48 * c + 48, :].astype(BF)
    total = dot(jnp.concatenate([turned[0], turned[1]], axis=1), down_z[...])
    blocks = exchange([total[48 * b:48 * b + 48, :] for b in range(4)])
    for b in range(4):
        packet[b, 80:128, :] = blocks[b].astype(BF)


def source(columns, down_rows, down_y, down_z):
    out_shape = (
        jax.ShapeDtypeStruct((4, FINE_ROWS + COARSE_ROWS, 128), BF),
        jax.ShapeDtypeStruct((2, 4, FINE_ROWS, 128), BF),
    )
    scratch = [
        pltpu.VMEM((4, FINE_ROWS, 400), F32),
        pltpu.VMEM((2, 8 * COARSE_ROWS, 128), BF),
        pltpu.VMEM((2, 4 * COARSE_ROWS, 128), BF),
    ]
    return pl.pallas_call(
        source_kernel, out_shape=out_shape, scratch_shapes=scratch, name="source",
        compiler_params=pltpu.CompilerParams(vmem_limit_bytes=16 << 20),
        cost_estimate=pl.CostEstimate(flops=10**9, bytes_accessed=10**6, transcendentals=0),
    )(*columns, down_rows, down_y, down_z)


def joined(blocks):
    return jnp.concatenate(blocks, axis=1)


def row_pass(rows, row_mats, stacks, targets):
    stacks = [[joined(column) for column in stack] for stack in stacks]
    stacks = [stack[0] if len(stack) == 1 else jnp.concatenate(stack, axis=0) for stack in stacks]
    for m in range(TERMS):
        mats = jnp.concatenate([row_mats[m, 0], row_mats[m, 1]], axis=1)
        for stack, target in zip(stacks, targets):
            result = dot(mats[:, 0:stack.shape[0]], stack)
            for b in range(4):
                target[m, b * rows:b * rows + rows, :] = result[:, 128 * b:128 * b + 128].astype(BF)


def level_rest(rows, nz, parts, y_mats, z_mats, sums, centres):
    zero = jnp.zeros((128, 128), BF)
    for m in range(TERMS):
        mats = jnp.concatenate([
            jnp.concatenate([y_mats[m, 0], y_mats[m, 1], y_mats[m, 2], zero], axis=0),
            jnp.concatenate([zero, zero, zero, y_mats[m, 0]], axis=0),
        ], axis=1)
        result = dot(jnp.concatenate([part[m] for part in parts], axis=1), mats)
        for n, target in enumerate((sums, centres)):
            blocks = exchange([result[b * rows:(b + 1) * rows, 128 * n:128 * n + 128] for b in range(4)])
            for b in range(4):
                target[m, b * rows:(b + 1) * rows, :] = blocks[b].astype(BF)
    total = dot(jnp.concatenate([sums[m] for m in range(TERMS)], axis=1), z_mats[0].reshape(TERMS * 128, 128))
    sides = dot(
        jnp.concatenate([centres[m] for m in range(TERMS)], axis=1),
        jnp.concatenate([z_mats[n].reshape(TERMS * 128, 128) for n in (1, 2)], axis=1),
    )
    z = iota((4 * rows, 128), 0) & (nz - 1)
    total = total + jnp.where(z == nz - 1, 0.0, pltpu.roll(sides[:, 0:128], 4 * rows - 1, 0))
    return total + jnp.where(z == 0, 0.0, pltpu.roll(sides[:, 128:256], 1, 0))


def level_scratch(rows):
    return [
        pltpu.VMEM((TERMS, 4 * rows, 128), BF),
        pltpu.VMEM((TERMS, 4 * rows, 128), BF),
    ]


def fine_near_kernel(packet, nears, row_mats, y_near, centre):
    own = [packet[b, 0:80, :] for b in range(4)]
    row_pass(FINE_ROWS, row_mats, ([[nears[1, b] for b in range(4)]], [own]), (y_near, centre))


def fine_far_kernel(packet, nears, x_packet, y_packet, row_mats, x_sum, y_far, x_parent, y_parent):
    for b in range(4):
        x_parent[b] = x_packet[b, 80:128, :]
        y_parent[b] = y_packet[b, 80:128, :]
    own, x_far, y_column = ([ref[b, 0:80, :] for b in range(4)] for ref in (packet, x_packet, y_packet))
    stacks = ([own, [nears[0, b] for b in range(4)], x_far], [y_column])
    row_pass(FINE_ROWS, row_mats, stacks, (x_sum, y_far))


def fine_rest_kernel(x_sum, y_near, y_far, centre, y_mats, z_mats, out, sums, centres):
    out[...] = level_rest(FINE_ROWS, 4, (x_sum, y_near, y_far, centre), y_mats, z_mats, sums, centres)


def small_call(kernel, name, out_shape, flops, *operands, scratch=()):
    return pl.pallas_call(
        kernel, out_shape=out_shape, name=name, scratch_shapes=scratch,
        compiler_params=pltpu.CompilerParams(vmem_limit_bytes=16 << 20),
        cost_estimate=pl.CostEstimate(flops=flops, bytes_accessed=4 * 10**6, transcendentals=0),
    )(*operands)


def coarse_kernel(packet, xfar, xother, yfar, yother, row_mats, y_mats, z_mats,
                  up_rows, up_y, up_z, fine_term, out, wide, grown, turned, split,
                  x_sum, far_side, other_side, centre, *scratch):
    own = [packet[b, 80:128, :] for b in range(4)]
    others = [[ref[b] for b in range(4)] for ref in (xfar, xother, yfar, yother)]
    stacks = ([own, others[0], others[1]], [others[2]], [others[3]], [own])
    parts = (x_sum, far_side, other_side, centre)
    row_pass(COARSE_ROWS, row_mats, stacks, parts)
    result = level_rest(COARSE_ROWS, 2, parts, y_mats, z_mats, *scratch)
    blocks = exchange([result[48 * b:48 * b + 48, :] for b in range(4)])
    for b in range(4):
        wide[:, 128 * b:128 * b + 128] = blocks[b].astype(BF)
    part = dot(up_rows[...], wide[...]).astype(BF)
    for b in range(4):
        grown[80 * b:80 * b + 80, :] = part[:, 128 * b:128 * b + 128]
    part = dot(grown[...], up_y[...])
    blocks = exchange([part[80 * b:80 * b + 80, :] for b in range(4)])
    for b in range(4):
        turned[80 * b:80 * b + 80, :] = blocks[b].astype(BF)
    both = dot(turned[...], jnp.concatenate([up_z[0], up_z[1]], axis=1))
    expanded = jnp.where((iota((320, 128), 0) & 1) == 0, both[:, 0:128], both[:, 128:256])
    total = fine_term[...] + expanded
    high = total.astype(BF)
    low = (total - high.astype(F32)).astype(BF)
    for b in range(4):
        split[0:80, 128 * b:128 * b + 128] = high[80 * b:80 * b + 80, :]
        split[80:160, 128 * b:128 * b + 128] = low[80 * b:80 * b + 80, :]
    select = onehot(natural_place(iota((512, 1), 0), False) == iota((512, 400), 1))
    natural = dot(split[...], select)
    natural = natural[0:80, :] + natural[80:160, :]
    for i in range(K2):
        out[0, 0, :, 400 * i:400 * i + 400] = natural[4 * i:4 * i + 4, :]


def coarse(operands):
    part = pltpu.VMEM((TERMS, 4 * COARSE_ROWS, 128), BF)
    scratch = [
        pltpu.VMEM((COARSE_ROWS, 512), BF),
        pltpu.VMEM((320, 128), BF),
        pltpu.VMEM((320, 128), BF),
        pltpu.VMEM((160, 512), BF),
    ] + [part] * 4 + level_scratch(COARSE_ROWS)
    return small_call(
        coarse_kernel, "coarse", jax.ShapeDtypeStruct((1, 1, 4, 8000), F32), 4 * 10**9, *operands, scratch=scratch
    )


def near(block, axis):
    return lax.ppermute(block, axis, [(i, i ^ 1) for i in range(lax.axis_size(axis))])


def far(block, axis):
    count = lax.axis_size(axis)
    return lax.ppermute(block, axis, [(i, ((i + 1) ^ 1) - 1) for i in range(1, count - 1)])


def corner(block):
    nx, ny = lax.axis_size("gx"), lax.axis_size("gy")
    route = [(x * ny + y, (x ^ 1) * ny + (y ^ 1)) for x in range(nx) for y in range(ny)]
    return lax.ppermute(block, ("gx", "gy"), route)


def shards(fine_source, fine_blocks, coarse_blocks, child_filter_matrices):
    columns = [fine_source, near(fine_source, "gx"), near(fine_source, "gy"), corner(fine_source)]
    built = build(fine_blocks, coarse_blocks, child_filter_matrices)
    packet, nears = source(columns, *built[6:9])
    x_packet, y_packet = far(packet, "gx"), far(packet, "gy")
    part = jax.ShapeDtypeStruct((TERMS, 4 * FINE_ROWS, 128), BF)
    parent = jax.ShapeDtypeStruct((4, COARSE_ROWS, 128), BF)
    y_near, centre = small_call(fine_near_kernel, "fine_near", (part, part), 10**9, packet, nears, built[0])
    x_sum, y_far, x_parent, y_parent = small_call(
        fine_far_kernel, "fine_far", (part, part, parent, parent), 10**9,
        packet, nears, x_packet, y_packet, built[0],
    )
    x_other, y_other = near(x_parent, "gx"), near(y_parent, "gy")
    fine_term = small_call(
        fine_rest_kernel, "fine_rest", jax.ShapeDtypeStruct((4 * FINE_ROWS, 128), F32), 4 * 10**9,
        x_sum, y_near, y_far, centre, *built[1:3], scratch=level_scratch(FINE_ROWS),
    )
    return coarse((packet, x_parent, x_other, y_parent, y_other, *built[3:6], *built[9:12], fine_term))


def solution(mesh):
    in_specs = (P("gx", "gy", None, None), P(), P(), P())
    out_specs = P("gx", "gy", None, None)
    return jax.shard_map(shards, mesh=mesh, in_specs=in_specs, out_specs=out_specs, check_vma=False)
```

```python
import jax
import jax.numpy as jnp
from jax import lax
from jax.experimental import pallas as pl
from jax.experimental.pallas import tpu as pltpu
from jax.sharding import PartitionSpec as P

K2 = 20
TERMS = 12
BF = jnp.bfloat16
F32 = jnp.float32
FINE_ROWS = 80
COARSE_ROWS = 48


def iota(shape, dim):
    return lax.broadcasted_iota(jnp.int32, shape, dim)


def dot(a, b):
    return jnp.dot(a, b, preferred_element_type=F32)


def place(n):
    piece, t = n >> 5, n & 31
    jj = (t * 13) >> 6
    return piece, jj, t - 5 * jj, t < 25


def natural_place(n):
    piece, jj, kk, ok = place(n & 127)
    return jnp.where(ok, (5 * piece + jj) * 20 + 5 * (n >> 7) + kk, -1)


def onehot(condition, dtype=BF):
    return jnp.where(condition, 1.0, 0.0).astype(dtype)


def lane_constants(on_j, natural=False):
    def index(n):
        piece, jj, kk, ok = place(n)
        return jnp.where(ok, piece * 5 + (jj if on_j else kk), -1)

    def fixed(n, none):
        _, jj, kk, ok = place(n)
        return jnp.where(ok, kk if on_j else jj, none)

    spread_rows = onehot(index(iota((128, 1), 0)) == iota((128, 32), 1))
    lane = iota((1, 128), 1)
    lane_index, lane_fixed = index(lane), fixed(lane, -2)
    if natural:
        lane_fixed = (lane * 205) >> 12
        lane_index = jnp.where(lane < 100, lane - 20 * lane_fixed, -1)
        lane_fixed = jnp.where(lane < 100, lane_fixed, -2)
    spread_lanes = onehot(lane_index == iota((K2, 128), 0))
    mask = onehot(fixed(iota((128, 1), 0), -1) == lane_fixed, F32)
    return spread_rows, spread_lanes, mask


def row_constants(rows, nz):
    shift = nz.bit_length() - 1
    spread_rows = onehot((iota((rows, 1), 0) >> shift) == iota((rows, 32), 1))
    wide = 256
    lane = iota((1, wide), 1)
    which = sum(jnp.where(lane >= c * rows, 1, 0) for c in range(1, 4))
    lane = lane - which * rows
    spreads = [
        onehot(jnp.where(which == c, lane >> shift, -1) == iota((K2, wide), 0)) for c in range(3)
    ]
    mask = onehot((iota((rows, 1), 0) & (nz - 1)) == (lane & (nz - 1)), F32)
    return spread_rows, spreads, mask


def flipped(matrix):
    return matrix.astype(F32).T.astype(BF)


def exchange(tiles):
    lane = iota((1, 128), 1)
    low = (lane & 64) == 0
    a, b, c, d = tiles
    a, c = jnp.where(low, a, pltpu.roll(c, 64, 1)), jnp.where(low, pltpu.roll(a, 64, 1), c)
    b, d = jnp.where(low, b, pltpu.roll(d, 64, 1)), jnp.where(low, pltpu.roll(b, 64, 1), d)
    low = (lane & 32) == 0
    a, b = jnp.where(low, a, pltpu.roll(b, 32, 1)), jnp.where(low, pltpu.roll(a, 96, 1), b)
    c, d = jnp.where(low, c, pltpu.roll(d, 32, 1)), jnp.where(low, pltpu.roll(c, 96, 1), d)
    return a, b, c, d


def spread_rows_of(out, plain, rows, nz, order):
    spread_rows, spreads, mask = row_constants(rows, nz)
    wide = sum(dot(plain[d].reshape(TERMS * 32, K2).astype(BF), spreads[c]) for c, d in enumerate(order))
    wide = wide.astype(BF).reshape(TERMS, 32, 256)
    for m in range(TERMS):
        mats = (dot(spread_rows, wide[m]) * mask).astype(BF)
        for c in range(2):
            out[m, c] = mats[:, 128 * c:128 * c + 128]


def lane_matrix(transposed, constants):
    spread_rows, spread_lanes, mask = constants
    return (dot(spread_rows[:, 0:K2], dot(transposed, spread_lanes).astype(BF)) * mask).astype(BF)


def parity():
    return lax.axis_index("gx") & 1, lax.axis_index("gy") & 1


def chosen(child_ref, which):
    first, second = child_ref[:, 0, :].astype(F32), child_ref[:, 1, :].astype(F32)
    return jnp.where(which == 0, first, second).astype(BF), jnp.where(which == 0, second, first).astype(BF)


def early_kernel(fine_hbm, coarse_hbm, child_hbm, fine_ref, coarse_ref, child_ref,
                 fine_rows, down_rows, down_y, down_z, plain, sems):
    copies = [
        pltpu.make_async_copy(src, dst, sems.at[n])
        for n, (src, dst) in enumerate(((fine_hbm, fine_ref), (coarse_hbm, coarse_ref), (child_hbm, child_ref)))
    ]
    for copy in copies:
        copy.start()
    plain[...] = jnp.zeros(plain.shape, F32)
    px, py = parity()
    on_j, on_k = lane_constants(True), lane_constants(False)
    for copy in copies:
        copy.wait()
    for d in range(3):
        for m in range(TERMS):
            plain[d, m, 0:K2, :] = fine_ref[d, m].astype(F32)
    near_x = 2 - 2 * px
    spread_rows_of(fine_rows, plain, FINE_ROWS, 4, (1, near_x, 2 - near_x))
    own_x, other_x = chosen(child_ref, px)
    own_y, other_y = chosen(child_ref, py)
    down_y[0:128, :] = lane_matrix(flipped(own_y), on_j)
    down_y[128:256, :] = lane_matrix(flipped(other_y), on_j)
    for c in range(2):
        down_z[128 * c:128 * c + 128, :] = lane_matrix(flipped(child_ref[:, c, :]), on_k)
    lane = iota((1, 160), 1)
    far = lane >= 80
    lane = jnp.where(far, lane - 80, lane)
    wide = dot(own_x, onehot(jnp.where(far, -1, lane >> 2) == iota((K2, 160), 0)))
    wide = wide + dot(other_x, onehot(jnp.where(far, lane >> 2, -1) == iota((K2, 160), 0)))
    r = iota((96, 1), 0)
    cz = jnp.where(r >= 48, 1, 0)
    r = r - 48 * cz
    mixed = dot(onehot((r >> 1) == iota((96, K2), 1)), wide.astype(BF))
    down_rows[...] = (mixed * onehot((2 * (r & 1) + cz) == (lane & 3), F32)).astype(BF)


def late_kernel(fine_ref, coarse_ref, child_ref, fine_y, fine_z, coarse_rows, coarse_y, coarse_z,
                up_rows, up_y, up_z, plain, turned, wide_y, wide_z):
    plain[...] = jnp.zeros(plain.shape, F32)
    turned[...] = jnp.zeros(turned.shape, F32)
    px, py = parity()
    on_j, on_k, to_natural = lane_constants(True), lane_constants(False), lane_constants(False, True)
    near_x, near_y = 2 - 2 * px, 2 - 2 * py
    for n, blocks in enumerate((fine_ref, coarse_ref)):
        for d in range(3):
            for m in range(TERMS):
                matrix = blocks[d, m].astype(F32)
                turned[n, d, m, 0:K2, :] = matrix.T
                if n == 1:
                    plain[d, m, 0:K2, :] = matrix
    levels = (
        (fine_y, fine_z, to_natural, (1, near_y, 2 - near_y)), (coarse_y, coarse_z, on_k, (1, 2 - near_y, near_y)),
    )
    for n, (y_out, z_out, along_k, order_y) in enumerate(levels):
        both = jnp.concatenate([on_j[1], along_k[1]], axis=1)
        wide = dot(turned[n].reshape(3 * TERMS * 32, K2).astype(BF), both).astype(BF)
        wide_y[n] = wide[:, 0:128].reshape(3, TERMS, 32, 128)
        wide_z[n] = wide[:, 128:256].reshape(3, TERMS, 32, 128)
        for (spread, _, mask), source_ref, order, out in (
            (on_j, wide_y, order_y, y_out), (along_k, wide_z, (1, 2, 0), z_out),
        ):
            for m in range(0, TERMS, 2):
                tiles = [source_ref[n, d, m + c] for c in range(2) for d in order]
                mats = dot(spread, jnp.concatenate(tiles, axis=1))
                for c in range(2):
                    for e in range(3):
                        lane = 384 * c + 128 * e
                        tile = (mats[:, lane:lane + 128] * mask).astype(BF)
                        if out is y_out:
                            out[m + c, e] = tile
                        else:
                            out[e, m + c] = tile
    spread_rows_of(coarse_rows, plain, COARSE_ROWS, 2, (1, 2 - near_x, near_x))
    own_x, _ = chosen(child_ref, px)
    own_y, _ = chosen(child_ref, py)
    up_y[...] = lane_matrix(own_y, on_j)
    for c in range(2):
        up_z[c] = lane_matrix(child_ref[:, c, :], to_natural)
    wide = dot(flipped(own_x), onehot((iota((1, 48), 1) >> 1) == iota((K2, 48), 0)))
    mixed = dot(onehot((iota((80, 1), 0) >> 2) == iota((80, K2), 1)), wide.astype(BF))
    keep = ((iota((80, 1), 0) & 3) >> 1) == (iota((1, 48), 1) & 1)
    up_rows[...] = (mixed * onehot(keep, F32)).astype(BF)


def bf16(*shape):
    return jax.ShapeDtypeStruct(shape, BF)


def early(fine_blocks, coarse_blocks, child):
    operands = [
        pltpu.with_memory_space_constraint(x, pltpu.HBM)
        for x in (fine_blocks, coarse_blocks, jnp.transpose(child, (1, 0, 2)))
    ]
    out_shape = tuple(bf16(*x.shape) for x in operands) + (
        bf16(TERMS, 2, FINE_ROWS, 128), bf16(96, 160), bf16(256, 128), bf16(256, 128),
    )
    return pl.pallas_call(
        early_kernel, out_shape=out_shape, name="early",
        in_specs=[pl.BlockSpec(memory_space=pltpu.HBM)] * 3,
        scratch_shapes=[pltpu.VMEM((3, TERMS, 32, K2), F32), pltpu.SemaphoreType.DMA((3,))],
        compiler_params=pltpu.CompilerParams(vmem_limit_bytes=16 << 20),
        cost_estimate=pl.CostEstimate(flops=2 * 10**9, bytes_accessed=4 * 10**6, transcendentals=0),
    )(*operands)


def late(blocks):
    level = (bf16(TERMS, 3, 128, 128), bf16(3, TERMS, 128, 128))
    out_shape = level + (bf16(TERMS, 2, COARSE_ROWS, 128),) + level
    out_shape += (bf16(80, 48), bf16(128, 128), bf16(2, 128, 128))
    scratch = [
        pltpu.VMEM((3, TERMS, 32, K2), F32), pltpu.VMEM((2, 3, TERMS, 32, K2), F32),
        pltpu.VMEM((2, 3, TERMS, 32, 128), BF), pltpu.VMEM((2, 3, TERMS, 32, 128), BF),
    ]
    return small_call(late_kernel, "late", out_shape, 2 * 10**9, *blocks, scratch=scratch)


def source_kernel(own, xnear, ynear, corner, down_rows, down_y, down_z,
                  packet, nears, natural, mixed, turned):
    select = onehot(iota((400, 512), 0) == natural_place(iota((1, 512), 1)))

    def converted(ref, slot):
        values = ref[0, 0].astype(F32)
        for i in range(K2):
            natural[slot, 4 * i:4 * i + 4, :] = values[:, 400 * i:400 * i + 400]
        return dot(natural[slot].astype(BF), select).astype(BF)

    centre, diagonal = converted(own, 0), converted(corner, 1)
    x_near, y_near = converted(xnear, 2), converted(ynear, 3)
    for b in range(4):
        here = slice(128 * b, 128 * b + 128)
        packet[b, 0:80, :] = centre[:, here]
        nears[0, b] = x_near[:, here]
        nears[1, b] = y_near[:, here]
    for c, (one, two) in enumerate(((centre, x_near), (y_near, diagonal))):
        rows = dot(down_rows[...], jnp.concatenate([one, two], axis=0)).astype(BF)
        for b in range(4):
            mixed[c, 96 * b:96 * b + 96, :] = rows[:, 128 * b:128 * b + 128]
    summed = dot(jnp.concatenate([mixed[0], mixed[1]], axis=1), down_y[...])
    blocks = exchange([summed[96 * b:96 * b + 96, :] for b in range(4)])
    for b in range(4):
        for c in range(2):
            turned[c, 48 * b:48 * b + 48, :] = blocks[b][48 * c:48 * c + 48, :].astype(BF)
    total = dot(jnp.concatenate([turned[0], turned[1]], axis=1), down_z[...])
    blocks = exchange([total[48 * b:48 * b + 48, :] for b in range(4)])
    for b in range(4):
        packet[b, 80:128, :] = blocks[b].astype(BF)


def source(columns, down_rows, down_y, down_z):
    out_shape = (
        jax.ShapeDtypeStruct((4, FINE_ROWS + COARSE_ROWS, 128), BF),
        jax.ShapeDtypeStruct((2, 4, FINE_ROWS, 128), BF),
    )
    scratch = [
        pltpu.VMEM((4, FINE_ROWS, 400), F32),
        pltpu.VMEM((2, 8 * COARSE_ROWS, 128), BF),
        pltpu.VMEM((2, 4 * COARSE_ROWS, 128), BF),
    ]
    return pl.pallas_call(
        source_kernel, out_shape=out_shape, scratch_shapes=scratch, name="source",
        compiler_params=pltpu.CompilerParams(vmem_limit_bytes=16 << 20),
        cost_estimate=pl.CostEstimate(flops=10**9, bytes_accessed=10**6, transcendentals=0),
    )(*columns, down_rows, down_y, down_z)


def joined(blocks):
    return jnp.concatenate(blocks, axis=1)


def row_pass(rows, row_mats, stacks, targets):
    stacks = [[joined(column) for column in stack] for stack in stacks]
    stacks = [stack[0] if len(stack) == 1 else jnp.concatenate(stack, axis=0) for stack in stacks]
    for m in range(TERMS):
        mats = jnp.concatenate([row_mats[m, 0], row_mats[m, 1]], axis=1)
        for stack, target in zip(stacks, targets):
            result = dot(mats[:, 0:stack.shape[0]], stack)
            for b in range(4):
                target[m, b * rows:b * rows + rows, :] = result[:, 128 * b:128 * b + 128].astype(BF)


def level_rest(rows, nz, parts, y_mats, z_mats, sums, centres):
    zero = jnp.zeros((128, 128), BF)
    for m in range(TERMS):
        mats = jnp.concatenate([
            jnp.concatenate([y_mats[m, 0], y_mats[m, 1], y_mats[m, 2], zero], axis=0),
            jnp.concatenate([zero, zero, zero, y_mats[m, 0]], axis=0),
        ], axis=1)
        result = dot(jnp.concatenate([part[m] for part in parts], axis=1), mats)
        for n, target in enumerate((sums, centres)):
            blocks = exchange([result[b * rows:(b + 1) * rows, 128 * n:128 * n + 128] for b in range(4)])
            for b in range(4):
                target[m, b * rows:(b + 1) * rows, :] = blocks[b].astype(BF)
    total = dot(jnp.concatenate([sums[m] for m in range(TERMS)], axis=1), z_mats[0].reshape(TERMS * 128, 128))
    sides = dot(
        jnp.concatenate([centres[m] for m in range(TERMS)], axis=1),
        jnp.concatenate([z_mats[n].reshape(TERMS * 128, 128) for n in (1, 2)], axis=1),
    )
    z = iota((4 * rows, 128), 0) & (nz - 1)
    total = total + jnp.where(z == nz - 1, 0.0, pltpu.roll(sides[:, 0:128], 4 * rows - 1, 0))
    return total + jnp.where(z == 0, 0.0, pltpu.roll(sides[:, 128:256], 1, 0))


def level_scratch(rows):
    return [
        pltpu.VMEM((TERMS, 4 * rows, 128), BF),
        pltpu.VMEM((TERMS, 4 * rows, 128), BF),
    ]


def fine_near_kernel(packet, nears, row_mats, y_near, centre):
    own = [packet[b, 0:80, :] for b in range(4)]
    row_pass(FINE_ROWS, row_mats, ([[nears[1, b] for b in range(4)]], [own]), (y_near, centre))


def fine_far_kernel(packet, nears, x_packet, y_packet, row_mats, x_sum, y_far, x_parent, y_parent):
    for b in range(4):
        x_parent[b] = x_packet[b, 80:128, :]
        y_parent[b] = y_packet[b, 80:128, :]
    own, x_far, y_column = ([ref[b, 0:80, :] for b in range(4)] for ref in (packet, x_packet, y_packet))
    stacks = ([own, [nears[0, b] for b in range(4)], x_far], [y_column])
    row_pass(FINE_ROWS, row_mats, stacks, (x_sum, y_far))


def fine_rest_kernel(x_sum, y_near, y_far, centre, y_mats, z_mats, out, sums, centres):
    out[...] = level_rest(FINE_ROWS, 4, (x_sum, y_near, y_far, centre), y_mats, z_mats, sums, centres)


def small_call(kernel, name, out_shape, flops, *operands, scratch=()):
    return pl.pallas_call(
        kernel, out_shape=out_shape, name=name, scratch_shapes=scratch,
        compiler_params=pltpu.CompilerParams(vmem_limit_bytes=16 << 20),
        cost_estimate=pl.CostEstimate(flops=flops, bytes_accessed=4 * 10**6, transcendentals=0),
    )(*operands)


def coarse_kernel(packet, xfar, xother, yfar, yother, row_mats, y_mats, z_mats,
                  up_rows, up_y, up_z, fine_term, out, wide, grown, turned,
                  x_sum, far_side, other_side, centre, *scratch):
    own = [packet[b, 80:128, :] for b in range(4)]
    others = [[ref[b] for b in range(4)] for ref in (xfar, xother, yfar, yother)]
    stacks = ([own, others[0], others[1]], [others[2]], [others[3]], [own])
    parts = (x_sum, far_side, other_side, centre)
    row_pass(COARSE_ROWS, row_mats, stacks, parts)
    result = level_rest(COARSE_ROWS, 2, parts, y_mats, z_mats, *scratch)
    blocks = exchange([result[48 * b:48 * b + 48, :] for b in range(4)])
    for b in range(4):
        wide[:, 128 * b:128 * b + 128] = blocks[b].astype(BF)
    part = dot(up_rows[...], wide[...]).astype(BF)
    for b in range(4):
        grown[80 * b:80 * b + 80, :] = part[:, 128 * b:128 * b + 128]
    part = dot(grown[...], up_y[...])
    blocks = exchange([part[80 * b:80 * b + 80, :] for b in range(4)])
    for b in range(4):
        turned[80 * b:80 * b + 80, :] = blocks[b].astype(BF)
    both = dot(turned[...], jnp.concatenate([up_z[0], up_z[1]], axis=1))
    expanded = jnp.where((iota((320, 128), 0) & 1) == 0, both[:, 0:128], both[:, 128:256])
    total = fine_term[...] + expanded
    for i in range(K2):
        for b in range(4):
            here = 400 * i + 100 * b
            out[0, 0, :, here:here + 100] = total[80 * b + 4 * i:80 * b + 4 * i + 4, 0:100]


def coarse(operands):
    part = pltpu.VMEM((TERMS, 4 * COARSE_ROWS, 128), BF)
    scratch = [
        pltpu.VMEM((COARSE_ROWS, 512), BF),
        pltpu.VMEM((320, 128), BF),
        pltpu.VMEM((320, 128), BF),
    ] + [part] * 4 + level_scratch(COARSE_ROWS)
    return small_call(
        coarse_kernel, "coarse", jax.ShapeDtypeStruct((1, 1, 4, 8000), F32), 4 * 10**9, *operands, scratch=scratch
    )


def near(block, axis):
    return lax.ppermute(block, axis, [(i, i ^ 1) for i in range(lax.axis_size(axis))])


def far(block, axis):
    count = lax.axis_size(axis)
    return lax.ppermute(block, axis, [(i, ((i + 1) ^ 1) - 1) for i in range(1, count - 1)])


def corner(block):
    nx, ny = lax.axis_size("gx"), lax.axis_size("gy")
    route = [(x * ny + y, (x ^ 1) * ny + (y ^ 1)) for x in range(nx) for y in range(ny)]
    return lax.ppermute(block, ("gx", "gy"), route)


def shards(fine_source, fine_blocks, coarse_blocks, child_filter_matrices):
    columns = [fine_source, near(fine_source, "gx"), near(fine_source, "gy"), corner(fine_source)]
    *blocks, fine_rows, down_rows, down_y, down_z = early(fine_blocks, coarse_blocks, child_filter_matrices)
    packet, nears = source(columns, down_rows, down_y, down_z)
    x_packet, y_packet = far(packet, "gx"), far(packet, "gy")
    fine_y, fine_z, *mats = late(blocks)
    part = jax.ShapeDtypeStruct((TERMS, 4 * FINE_ROWS, 128), BF)
    parent = jax.ShapeDtypeStruct((4, COARSE_ROWS, 128), BF)
    y_near, centre = small_call(fine_near_kernel, "fine_near", (part, part), 10**9, packet, nears, fine_rows)
    x_sum, y_far, x_parent, y_parent = small_call(
        fine_far_kernel, "fine_far", (part, part, parent, parent), 10**9,
        packet, nears, x_packet, y_packet, fine_rows,
    )
    x_other, y_other = near(x_parent, "gx"), near(y_parent, "gy")
    fine_term = small_call(
        fine_rest_kernel, "fine_rest", jax.ShapeDtypeStruct((4 * FINE_ROWS, 128), F32), 4 * 10**9,
        x_sum, y_near, y_far, centre, fine_y, fine_z, scratch=level_scratch(FINE_ROWS),
    )
    return coarse((packet, x_parent, x_other, y_parent, y_other, *mats, fine_term))


def solution(mesh):
    in_specs = (P("gx", "gy", None, None), P(), P(), P())
    out_specs = P("gx", "gy", None, None)
    return jax.shard_map(shards, mesh=mesh, in_specs=in_specs, out_specs=out_specs, check_vma=False)
```

```python
import jax
import jax.numpy as jnp
from jax import lax
from jax.experimental import pallas as pl
from jax.experimental.pallas import tpu as pltpu
from jax.sharding import PartitionSpec as P

K2 = 20
TERMS = 12
BF = jnp.bfloat16
F32 = jnp.float32
FINE_ROWS = 80
COARSE_ROWS = 48
PARENT_ROWS = 40


def iota(shape, dim):
    return lax.broadcasted_iota(jnp.int32, shape, dim)


def dot(a, b):
    return jnp.dot(a, b, preferred_element_type=F32)


def place(n):
    piece, t = n >> 5, n & 31
    jj = (t * 13) >> 6
    return piece, jj, t - 5 * jj, t < 25


def natural_place(n):
    piece, jj, kk, ok = place(n & 127)
    return jnp.where(ok, (5 * piece + jj) * 20 + 5 * (n >> 7) + kk, -1)


def onehot(condition, dtype=BF):
    return jnp.where(condition, 1.0, 0.0).astype(dtype)


def lane_constants(on_j, natural=False):
    def index(n):
        piece, jj, kk, ok = place(n)
        return jnp.where(ok, piece * 5 + (jj if on_j else kk), -1)

    def fixed(n, none):
        _, jj, kk, ok = place(n)
        return jnp.where(ok, kk if on_j else jj, none)

    spread_rows = onehot(index(iota((128, 1), 0)) == iota((128, 32), 1))
    lane = iota((1, 128), 1)
    lane_index, lane_fixed = index(lane), fixed(lane, -2)
    if natural:
        lane_fixed = (lane * 205) >> 12
        lane_index = jnp.where(lane < 100, lane - 20 * lane_fixed, -1)
        lane_fixed = jnp.where(lane < 100, lane_fixed, -2)
    spread_lanes = onehot(lane_index == iota((K2, 128), 0))
    mask = onehot(fixed(iota((128, 1), 0), -1) == lane_fixed, F32)
    return spread_rows, spread_lanes, mask


def row_constants(rows, nz):
    taken = K2 * nz
    shift = nz.bit_length() - 1
    spread_rows = onehot((iota((rows, 1), 0) >> shift) == iota((rows, 32), 1))
    wide = 256
    lane = iota((1, wide), 1)
    which = sum(jnp.where(lane >= c * taken, 1, 0) for c in range(1, 4))
    lane = lane - which * taken
    spreads = [
        onehot(jnp.where(which == c, lane >> shift, -1) == iota((K2, wide), 0)) for c in range(3)
    ]
    mask = onehot((iota((rows, 1), 0) & (nz - 1)) == (lane & (nz - 1)), F32)
    return spread_rows, spreads, mask


def flipped(matrix):
    return matrix.astype(F32).T.astype(BF)


def exchange(tiles):
    lane = iota((1, 128), 1)
    low = (lane & 64) == 0
    a, b, c, d = tiles
    a, c = jnp.where(low, a, pltpu.roll(c, 64, 1)), jnp.where(low, pltpu.roll(a, 64, 1), c)
    b, d = jnp.where(low, b, pltpu.roll(d, 64, 1)), jnp.where(low, pltpu.roll(b, 64, 1), d)
    low = (lane & 32) == 0
    a, b = jnp.where(low, a, pltpu.roll(b, 32, 1)), jnp.where(low, pltpu.roll(a, 96, 1), b)
    c, d = jnp.where(low, c, pltpu.roll(d, 32, 1)), jnp.where(low, pltpu.roll(c, 96, 1), d)
    return a, b, c, d


def spread_rows_of(out, plain, rows, nz, order):
    spread_rows, spreads, mask = row_constants(rows, nz)
    wide = sum(dot(plain[d].reshape(TERMS * 32, K2).astype(BF), spreads[c]) for c, d in enumerate(order))
    wide = wide.astype(BF).reshape(TERMS, 32, 256)
    for m in range(TERMS):
        mats = (dot(spread_rows, wide[m]) * mask).astype(BF)
        for c in range(2):
            out[m, c] = mats[:, 128 * c:128 * c + 128]


def lane_matrix(transposed, constants):
    spread_rows, spread_lanes, mask = constants
    return (dot(spread_rows[:, 0:K2], dot(transposed, spread_lanes).astype(BF)) * mask).astype(BF)


def parity():
    return lax.axis_index("gx") & 1, lax.axis_index("gy") & 1


def chosen(child_ref, which):
    first, second = child_ref[:, 0, :].astype(F32), child_ref[:, 1, :].astype(F32)
    return jnp.where(which == 0, first, second).astype(BF), jnp.where(which == 0, second, first).astype(BF)


def early_kernel(fine_hbm, coarse_hbm, child_hbm, fine_ref, coarse_ref, child_ref,
                 fine_rows, down_rows, down_y, down_z, plain, sems):
    copies = [
        pltpu.make_async_copy(src, dst, sems.at[n])
        for n, (src, dst) in enumerate(((fine_hbm, fine_ref), (coarse_hbm, coarse_ref), (child_hbm, child_ref)))
    ]
    for copy in copies:
        copy.start()
    plain[...] = jnp.zeros(plain.shape, F32)
    px, py = parity()
    on_j, on_k = lane_constants(True), lane_constants(False)
    for copy in copies:
        copy.wait()
    for d in range(3):
        for m in range(TERMS):
            plain[d, m, 0:K2, :] = fine_ref[d, m].astype(F32)
    near_x = 2 - 2 * px
    spread_rows_of(fine_rows, plain, FINE_ROWS, 4, (1, near_x, 2 - near_x))
    own_x, other_x = chosen(child_ref, px)
    own_y, other_y = chosen(child_ref, py)
    down_y[0:128, :] = lane_matrix(flipped(own_y), on_j)
    down_y[128:256, :] = lane_matrix(flipped(other_y), on_j)
    for c in range(2):
        down_z[128 * c:128 * c + 128, :] = lane_matrix(flipped(child_ref[:, c, :]), on_k)
    lane = iota((1, 160), 1)
    far = lane >= 80
    lane = jnp.where(far, lane - 80, lane)
    wide = dot(own_x, onehot(jnp.where(far, -1, lane >> 2) == iota((K2, 160), 0)))
    wide = wide + dot(other_x, onehot(jnp.where(far, lane >> 2, -1) == iota((K2, 160), 0)))
    r = iota((96, 1), 0)
    cz = jnp.where(r >= 48, 1, 0)
    r = r - 48 * cz
    mixed = dot(onehot((r >> 1) == iota((96, K2), 1)), wide.astype(BF))
    down_rows[...] = (mixed * onehot((2 * (r & 1) + cz) == (lane & 3), F32)).astype(BF)


def late_kernel(fine_ref, coarse_ref, child_ref, fine_y, fine_z, coarse_rows, coarse_y, coarse_z,
                up_rows, up_y, up_z, plain, turned, wide_y, wide_z):
    plain[...] = jnp.zeros(plain.shape, F32)
    turned[...] = jnp.zeros(turned.shape, F32)
    px, py = parity()
    on_j, on_k, to_natural = lane_constants(True), lane_constants(False), lane_constants(False, True)
    near_x, near_y = 2 - 2 * px, 2 - 2 * py
    for n, blocks in enumerate((fine_ref, coarse_ref)):
        for d in range(3):
            for m in range(TERMS):
                matrix = blocks[d, m].astype(F32)
                turned[n, d, m, 0:K2, :] = matrix.T
                if n == 1:
                    plain[d, m, 0:K2, :] = matrix
    levels = (
        (fine_y, fine_z, to_natural, (1, near_y, 2 - near_y)), (coarse_y, coarse_z, on_k, (1, 2 - near_y, near_y)),
    )
    for n, (y_out, z_out, along_k, order_y) in enumerate(levels):
        both = jnp.concatenate([on_j[1], along_k[1]], axis=1)
        wide = dot(turned[n].reshape(3 * TERMS * 32, K2).astype(BF), both).astype(BF)
        wide_y[n] = wide[:, 0:128].reshape(3, TERMS, 32, 128)
        wide_z[n] = wide[:, 128:256].reshape(3, TERMS, 32, 128)
        for (spread, _, mask), source_ref, order, out in (
            (on_j, wide_y, order_y, y_out), (along_k, wide_z, (1, 2, 0), z_out),
        ):
            for m in range(0, TERMS, 2):
                tiles = [source_ref[n, d, m + c] for c in range(2) for d in order]
                mats = dot(spread, jnp.concatenate(tiles, axis=1))
                for c in range(2):
                    for e in range(3):
                        lane = 384 * c + 128 * e
                        tile = (mats[:, lane:lane + 128] * mask).astype(BF)
                        if out is y_out:
                            out[m + c, e] = tile
                        else:
                            out[e, m + c] = tile
    spread_rows_of(coarse_rows, plain, COARSE_ROWS, 2, (1, 2 - near_x, near_x))
    own_x, _ = chosen(child_ref, px)
    own_y, _ = chosen(child_ref, py)
    up_y[...] = lane_matrix(own_y, on_j)
    for c in range(2):
        up_z[c] = lane_matrix(child_ref[:, c, :], to_natural)
    wide = dot(flipped(own_x), onehot((iota((1, 48), 1) >> 1) == iota((K2, 48), 0)))
    mixed = dot(onehot((iota((80, 1), 0) >> 2) == iota((80, K2), 1)), wide.astype(BF))
    keep = ((iota((80, 1), 0) & 3) >> 1) == (iota((1, 48), 1) & 1)
    up_rows[...] = (mixed * onehot(keep, F32)).astype(BF)


def bf16(*shape):
    return jax.ShapeDtypeStruct(shape, BF)


def early(fine_blocks, coarse_blocks, child):
    operands = [
        pltpu.with_memory_space_constraint(x, pltpu.HBM)
        for x in (fine_blocks, coarse_blocks, jnp.transpose(child, (1, 0, 2)))
    ]
    out_shape = tuple(bf16(*x.shape) for x in operands) + (
        bf16(TERMS, 2, FINE_ROWS, 128), bf16(96, 160), bf16(256, 128), bf16(256, 128),
    )
    return pl.pallas_call(
        early_kernel, out_shape=out_shape, name="early",
        in_specs=[pl.BlockSpec(memory_space=pltpu.HBM)] * 3,
        scratch_shapes=[pltpu.VMEM((3, TERMS, 32, K2), F32), pltpu.SemaphoreType.DMA((3,))],
        compiler_params=pltpu.CompilerParams(vmem_limit_bytes=16 << 20),
        cost_estimate=pl.CostEstimate(flops=2 * 10**9, bytes_accessed=4 * 10**6, transcendentals=0),
    )(*operands)


def late(blocks):
    level = (bf16(TERMS, 3, 128, 128), bf16(3, TERMS, 128, 128))
    out_shape = level + (bf16(TERMS, 2, COARSE_ROWS, 128),) + level
    out_shape += (bf16(80, 48), bf16(128, 128), bf16(2, 128, 128))
    scratch = [
        pltpu.VMEM((3, TERMS, 32, K2), F32), pltpu.VMEM((2, 3, TERMS, 32, K2), F32),
        pltpu.VMEM((2, 3, TERMS, 32, 128), BF), pltpu.VMEM((2, 3, TERMS, 32, 128), BF),
    ]
    return small_call(late_kernel, "late", out_shape, 2 * 10**9, *blocks, scratch=scratch)


def source_kernel(own, xnear, ynear, corner, down_rows, down_y, down_z,
                  packet, nears, natural, mixed, turned):
    select = onehot(iota((400, 512), 0) == natural_place(iota((1, 512), 1)))

    def converted(ref, slot):
        values = ref[0, 0].astype(F32)
        for i in range(K2):
            natural[slot, 4 * i:4 * i + 4, :] = values[:, 400 * i:400 * i + 400]
        return dot(natural[slot].astype(BF), select).astype(BF)

    centre, diagonal = converted(own, 0), converted(corner, 1)
    x_near, y_near = converted(xnear, 2), converted(ynear, 3)
    for b in range(4):
        here = slice(128 * b, 128 * b + 128)
        packet[b, 0:80, :] = centre[:, here]
        nears[0, b] = x_near[:, here]
        nears[1, b] = y_near[:, here]
    for c, (one, two) in enumerate(((centre, x_near), (y_near, diagonal))):
        rows = dot(down_rows[...], jnp.concatenate([one, two], axis=0)).astype(BF)
        for b in range(4):
            mixed[c, 96 * b:96 * b + 96, :] = rows[:, 128 * b:128 * b + 128]
    summed = dot(jnp.concatenate([mixed[0], mixed[1]], axis=1), down_y[...])
    blocks = exchange([summed[96 * b:96 * b + 96, :] for b in range(4)])
    for b in range(4):
        for c in range(2):
            turned[c, 48 * b:48 * b + 48, :] = blocks[b][48 * c:48 * c + 48, :].astype(BF)
    total = dot(jnp.concatenate([turned[0], turned[1]], axis=1), down_z[...])
    blocks = exchange([total[48 * b:48 * b + 48, :] for b in range(4)])
    for b in range(4):
        packet[b, 80:120, :] = blocks[b][0:PARENT_ROWS, :].astype(BF)


def source(columns, down_rows, down_y, down_z):
    out_shape = (
        jax.ShapeDtypeStruct((4, FINE_ROWS + PARENT_ROWS, 128), BF),
        jax.ShapeDtypeStruct((2, 4, FINE_ROWS, 128), BF),
    )
    scratch = [
        pltpu.VMEM((4, FINE_ROWS, 400), F32),
        pltpu.VMEM((2, 8 * COARSE_ROWS, 128), BF),
        pltpu.VMEM((2, 4 * COARSE_ROWS, 128), BF),
    ]
    return pl.pallas_call(
        source_kernel, out_shape=out_shape, scratch_shapes=scratch, name="source",
        compiler_params=pltpu.CompilerParams(vmem_limit_bytes=16 << 20),
        cost_estimate=pl.CostEstimate(flops=10**9, bytes_accessed=10**6, transcendentals=0),
    )(*columns, down_rows, down_y, down_z)


def joined(blocks):
    return jnp.concatenate(blocks, axis=1)


def row_pass(rows, row_mats, stacks, targets):
    stacks = [[joined(column) for column in stack] for stack in stacks]
    stacks = [(stack[0] if len(stack) == 1 else jnp.concatenate(stack, axis=0)).astype(BF) for stack in stacks]
    for m in range(TERMS):
        mats = jnp.concatenate([row_mats[m, 0], row_mats[m, 1]], axis=1)
        for stack, target in zip(stacks, targets):
            result = dot(mats[:, 0:stack.shape[0]], stack)
            for b in range(4):
                target[m, b * rows:b * rows + rows, :] = result[:, 128 * b:128 * b + 128].astype(BF)


def level_rest(rows, nz, parts, y_mats, z_mats, sums, centres):
    zero = jnp.zeros((128, 128), BF)
    for m in range(TERMS):
        mats = jnp.concatenate([
            jnp.concatenate([y_mats[m, 0], y_mats[m, 1], y_mats[m, 2], zero], axis=0),
            jnp.concatenate([zero, zero, zero, y_mats[m, 0]], axis=0),
        ], axis=1)
        result = dot(jnp.concatenate([part[m] for part in parts], axis=1), mats)
        for n, target in enumerate((sums, centres)):
            blocks = exchange([result[b * rows:(b + 1) * rows, 128 * n:128 * n + 128] for b in range(4)])
            for b in range(4):
                target[m, b * rows:(b + 1) * rows, :] = blocks[b].astype(BF)
    total = dot(jnp.concatenate([sums[m] for m in range(TERMS)], axis=1), z_mats[0].reshape(TERMS * 128, 128))
    sides = dot(
        jnp.concatenate([centres[m] for m in range(TERMS)], axis=1),
        jnp.concatenate([z_mats[n].reshape(TERMS * 128, 128) for n in (1, 2)], axis=1),
    )
    z = iota((4 * rows, 128), 0) & (nz - 1)
    total = total + jnp.where(z == nz - 1, 0.0, pltpu.roll(sides[:, 0:128], 4 * rows - 1, 0))
    return total + jnp.where(z == 0, 0.0, pltpu.roll(sides[:, 128:256], 1, 0))


def level_scratch(rows):
    return [
        pltpu.VMEM((TERMS, 4 * rows, 128), BF),
        pltpu.VMEM((TERMS, 4 * rows, 128), BF),
    ]


def fine_near_kernel(packet, nears, row_mats, y_near, centre):
    own = [packet[b, 0:80, :] for b in range(4)]
    row_pass(FINE_ROWS, row_mats, ([[nears[1, b] for b in range(4)]], [own]), (y_near, centre))


def fine_far_kernel(packet, nears, y_packet, x_packet, row_mats, x_sum, y_far, x_parent, y_parent):
    for b in range(4):
        x_parent[b] = x_packet[b, 80:120, :]
        y_parent[b] = y_packet[b, 80:120, :]
    own, x_far, y_column = ([ref[b, 0:80, :] for b in range(4)] for ref in (packet, x_packet, y_packet))
    stacks = ([own, [nears[0, b] for b in range(4)], x_far], [y_column])
    row_pass(FINE_ROWS, row_mats, stacks, (x_sum, y_far))


def fine_rest_kernel(x_sum, y_near, y_far, centre, y_mats, z_mats, out, sums, centres):
    out[...] = level_rest(FINE_ROWS, 4, (x_sum, y_near, y_far, centre), y_mats, z_mats, sums, centres)


def small_call(kernel, name, out_shape, flops, *operands, scratch=()):
    return pl.pallas_call(
        kernel, out_shape=out_shape, name=name, scratch_shapes=scratch,
        compiler_params=pltpu.CompilerParams(vmem_limit_bytes=16 << 20),
        cost_estimate=pl.CostEstimate(flops=flops, bytes_accessed=4 * 10**6, transcendentals=0),
    )(*operands)


def coarse_kernel(packet, xfar, xother, yfar, yother, row_mats, y_mats, z_mats,
                  up_rows, up_y, up_z, fine_term, out, wide, grown, turned,
                  x_sum, far_side, other_side, centre, *scratch):
    own = [packet[b, 80:120, :].astype(F32) for b in range(4)]
    others = [[ref[b].astype(F32) for b in range(4)] for ref in (xfar, xother, yfar, yother)]
    stacks = ([own, others[0], others[1]], [others[2]], [others[3]], [own])
    parts = (x_sum, far_side, other_side, centre)
    row_pass(COARSE_ROWS, row_mats, stacks, parts)
    result = level_rest(COARSE_ROWS, 2, parts, y_mats, z_mats, *scratch)
    blocks = exchange([result[48 * b:48 * b + 48, :] for b in range(4)])
    for b in range(4):
        wide[:, 128 * b:128 * b + 128] = blocks[b].astype(BF)
    part = dot(up_rows[...], wide[...]).astype(BF)
    for b in range(4):
        grown[80 * b:80 * b + 80, :] = part[:, 128 * b:128 * b + 128]
    part = dot(grown[...], up_y[...])
    blocks = exchange([part[80 * b:80 * b + 80, :] for b in range(4)])
    for b in range(4):
        turned[80 * b:80 * b + 80, :] = blocks[b].astype(BF)
    both = dot(turned[...], jnp.concatenate([up_z[0], up_z[1]], axis=1))
    expanded = jnp.where((iota((320, 128), 0) & 1) == 0, both[:, 0:128], both[:, 128:256])
    total = fine_term[...] + expanded
    for i in range(K2):
        for b in range(4):
            here = 400 * i + 100 * b
            out[0, 0, :, here:here + 100] = total[80 * b + 4 * i:80 * b + 4 * i + 4, 0:100]


def coarse(operands):
    part = pltpu.VMEM((TERMS, 4 * COARSE_ROWS, 128), BF)
    scratch = [
        pltpu.VMEM((COARSE_ROWS, 512), BF),
        pltpu.VMEM((320, 128), BF),
        pltpu.VMEM((320, 128), BF),
    ] + [part] * 4 + level_scratch(COARSE_ROWS)
    return small_call(
        coarse_kernel, "coarse", jax.ShapeDtypeStruct((1, 1, 4, 8000), F32), 4 * 10**9, *operands, scratch=scratch
    )


def near(block, axis):
    return lax.ppermute(block, axis, [(i, i ^ 1) for i in range(lax.axis_size(axis))])


def far(block, axis):
    count = lax.axis_size(axis)
    return lax.ppermute(block, axis, [(i, ((i + 1) ^ 1) - 1) for i in range(1, count - 1)])


def corner(block):
    nx, ny = lax.axis_size("gx"), lax.axis_size("gy")
    route = [(x * ny + y, (x ^ 1) * ny + (y ^ 1)) for x in range(nx) for y in range(ny)]
    return lax.ppermute(block, ("gx", "gy"), route)


def shards(fine_source, fine_blocks, coarse_blocks, child_filter_matrices):
    columns = [fine_source, near(fine_source, "gx"), near(fine_source, "gy"), corner(fine_source)]
    *blocks, fine_rows, down_rows, down_y, down_z = early(fine_blocks, coarse_blocks, child_filter_matrices)
    packet, nears = source(columns, down_rows, down_y, down_z)
    y_packet, x_packet = far(packet, "gy"), far(packet, "gx")
    fine_y, fine_z, *mats = late(blocks)
    part = jax.ShapeDtypeStruct((TERMS, 4 * FINE_ROWS, 128), BF)
    parent = jax.ShapeDtypeStruct((4, PARENT_ROWS, 128), BF)
    y_near, centre = small_call(fine_near_kernel, "fine_near", (part, part), 10**9, packet, nears, fine_rows)
    x_sum, y_far, x_parent, y_parent = small_call(
        fine_far_kernel, "fine_far", (part, part, parent, parent), 10**9,
        packet, nears, y_packet, x_packet, fine_rows,
    )
    x_other, y_other = near(x_parent, "gx"), near(y_parent, "gy")
    fine_term = small_call(
        fine_rest_kernel, "fine_rest", jax.ShapeDtypeStruct((4 * FINE_ROWS, 128), F32), 4 * 10**9,
        x_sum, y_near, y_far, centre, fine_y, fine_z, scratch=level_scratch(FINE_ROWS),
    )
    return coarse((packet, x_parent, x_other, y_parent, y_other, *mats, fine_term))


def solution(mesh):
    in_specs = (P("gx", "gy", None, None), P(), P(), P())
    out_specs = P("gx", "gy", None, None)
    return jax.shard_map(shards, mesh=mesh, in_specs=in_specs, out_specs=out_specs, check_vma=False)
```

```python
import jax
import jax.numpy as jnp
from jax import lax
from jax.experimental import pallas as pl
from jax.experimental.pallas import tpu as pltpu
from jax.sharding import PartitionSpec as P

K2 = 20
TERMS = 12
BF = jnp.bfloat16
F32 = jnp.float32
FINE_ROWS = 80
COARSE_ROWS = 48
PARENT_ROWS = 40


def iota(shape, dim):
    return lax.broadcasted_iota(jnp.int32, shape, dim)


def dot(a, b):
    return jnp.dot(a, b, preferred_element_type=F32)


def place(n):
    piece, t = n >> 5, n & 31
    jj = (t * 13) >> 6
    return piece, jj, t - 5 * jj, t < 25


def natural_place(n):
    piece, jj, kk, ok = place(n & 127)
    return jnp.where(ok, (5 * piece + jj) * 20 + 5 * (n >> 7) + kk, -1)


def onehot(condition, dtype=BF):
    return jnp.where(condition, 1.0, 0.0).astype(dtype)


def lane_constants(on_j, natural=False):
    def index(n):
        piece, jj, kk, ok = place(n)
        return jnp.where(ok, piece * 5 + (jj if on_j else kk), -1)

    def fixed(n, none):
        _, jj, kk, ok = place(n)
        return jnp.where(ok, kk if on_j else jj, none)

    spread_rows = onehot(index(iota((128, 1), 0)) == iota((128, 32), 1))
    lane = iota((1, 128), 1)
    lane_index, lane_fixed = index(lane), fixed(lane, -2)
    if natural:
        lane_fixed = (lane * 205) >> 12
        lane_index = jnp.where(lane < 100, lane - 20 * lane_fixed, -1)
        lane_fixed = jnp.where(lane < 100, lane_fixed, -2)
    spread_lanes = onehot(lane_index == iota((K2, 128), 0))
    mask = onehot(fixed(iota((128, 1), 0), -1) == lane_fixed, F32)
    return spread_rows, spread_lanes, mask


def row_constants(rows, nz):
    taken = K2 * nz
    shift = nz.bit_length() - 1
    spread_rows = onehot((iota((rows, 1), 0) >> shift) == iota((rows, 32), 1))
    wide = 256
    lane = iota((1, wide), 1)
    which = sum(jnp.where(lane >= c * taken, 1, 0) for c in range(1, 4))
    lane = lane - which * taken
    spreads = [
        onehot(jnp.where(which == c, lane >> shift, -1) == iota((K2, wide), 0)) for c in range(3)
    ]
    mask = onehot((iota((rows, 1), 0) & (nz - 1)) == (lane & (nz - 1)), F32)
    return spread_rows, spreads, mask


def flipped(matrix):
    return matrix.astype(F32).T.astype(BF)


def exchange(tiles):
    lane = iota((1, 128), 1)
    low = (lane & 64) == 0
    a, b, c, d = tiles
    a, c = jnp.where(low, a, pltpu.roll(c, 64, 1)), jnp.where(low, pltpu.roll(a, 64, 1), c)
    b, d = jnp.where(low, b, pltpu.roll(d, 64, 1)), jnp.where(low, pltpu.roll(b, 64, 1), d)
    low = (lane & 32) == 0
    a, b = jnp.where(low, a, pltpu.roll(b, 32, 1)), jnp.where(low, pltpu.roll(a, 96, 1), b)
    c, d = jnp.where(low, c, pltpu.roll(d, 32, 1)), jnp.where(low, pltpu.roll(c, 96, 1), d)
    return a, b, c, d


def spread_rows_of(out, plain, rows, nz, order):
    spread_rows, spreads, mask = row_constants(rows, nz)
    wide = sum(dot(plain[d].reshape(TERMS * 32, K2).astype(BF), spreads[c]) for c, d in enumerate(order))
    wide = wide.astype(BF).reshape(TERMS, 32, 256)
    for m in range(TERMS):
        mats = (dot(spread_rows, wide[m]) * mask).astype(BF)
        for c in range(2):
            out[m, c] = mats[:, 128 * c:128 * c + 128]


def lane_matrix(transposed, constants):
    spread_rows, spread_lanes, mask = constants
    return (dot(spread_rows[:, 0:K2], dot(transposed, spread_lanes).astype(BF)) * mask).astype(BF)


def parity():
    return lax.axis_index("gx") & 1, lax.axis_index("gy") & 1


def chosen(child_ref, which):
    first, second = child_ref[:, 0, :].astype(F32), child_ref[:, 1, :].astype(F32)
    return jnp.where(which == 0, first, second).astype(BF), jnp.where(which == 0, second, first).astype(BF)


def lane_level(turned, wide_y, wide_z, y_out, z_out, on_j, along_k, order_y):
    both = jnp.concatenate([on_j[1], along_k[1]], axis=1)
    wide = dot(turned[...].reshape(3 * TERMS * 32, K2).astype(BF), both).astype(BF)
    wide_y[...] = wide[:, 0:128].reshape(3, TERMS, 32, 128)
    wide_z[...] = wide[:, 128:256].reshape(3, TERMS, 32, 128)
    for (spread, _, mask), source_ref, order, out in (
        (on_j, wide_y, order_y, y_out), (along_k, wide_z, (1, 2, 0), z_out),
    ):
        for m in range(0, TERMS, 2):
            tiles = [source_ref[d, m + c] for c in range(2) for d in order]
            mats = dot(spread, jnp.concatenate(tiles, axis=1))
            for c in range(2):
                for e in range(3):
                    lane = 384 * c + 128 * e
                    tile = (mats[:, lane:lane + 128] * mask).astype(BF)
                    if out is y_out:
                        out[m + c, e] = tile
                    else:
                        out[e, m + c] = tile


def early_kernel(fine_hbm, coarse_hbm, child_hbm, coarse_ref, child_ref,
                 fine_rows, fine_y, fine_z, down_rows, down_y, down_z, fine_ref, plain, turned, wide_y, wide_z, sems):
    copies = [
        pltpu.make_async_copy(src, dst, sems.at[n])
        for n, (src, dst) in enumerate(((fine_hbm, fine_ref), (coarse_hbm, coarse_ref), (child_hbm, child_ref)))
    ]
    for copy in copies:
        copy.start()
    plain[...] = jnp.zeros(plain.shape, F32)
    turned[...] = jnp.zeros(turned.shape, F32)
    px, py = parity()
    on_j, on_k, to_natural = lane_constants(True), lane_constants(False), lane_constants(False, True)
    for copy in copies:
        copy.wait()
    for d in range(3):
        for m in range(TERMS):
            matrix = fine_ref[d, m].astype(F32)
            plain[d, m, 0:K2, :] = matrix
            turned[d, m, 0:K2, :] = matrix.T
    near_x, near_y = 2 - 2 * px, 2 - 2 * py
    lane_level(turned, wide_y, wide_z, fine_y, fine_z, on_j, to_natural, (1, near_y, 2 - near_y))
    spread_rows_of(fine_rows, plain, FINE_ROWS, 4, (1, near_x, 2 - near_x))
    own_x, other_x = chosen(child_ref, px)
    own_y, other_y = chosen(child_ref, py)
    down_y[0:128, :] = lane_matrix(flipped(own_y), on_j)
    down_y[128:256, :] = lane_matrix(flipped(other_y), on_j)
    for c in range(2):
        down_z[128 * c:128 * c + 128, :] = lane_matrix(flipped(child_ref[:, c, :]), on_k)
    lane = iota((1, 160), 1)
    far = lane >= 80
    lane = jnp.where(far, lane - 80, lane)
    wide = dot(own_x, onehot(jnp.where(far, -1, lane >> 2) == iota((K2, 160), 0)))
    wide = wide + dot(other_x, onehot(jnp.where(far, lane >> 2, -1) == iota((K2, 160), 0)))
    r = iota((96, 1), 0)
    cz = jnp.where(r >= 48, 1, 0)
    r = r - 48 * cz
    mixed = dot(onehot((r >> 1) == iota((96, K2), 1)), wide.astype(BF))
    down_rows[...] = (mixed * onehot((2 * (r & 1) + cz) == (lane & 3), F32)).astype(BF)


def late_kernel(coarse_ref, child_ref, coarse_rows, coarse_y, coarse_z,
                up_rows, up_y, up_z, plain, turned, wide_y, wide_z):
    plain[...] = jnp.zeros(plain.shape, F32)
    turned[...] = jnp.zeros(turned.shape, F32)
    px, py = parity()
    on_j, on_k, to_natural = lane_constants(True), lane_constants(False), lane_constants(False, True)
    near_x, near_y = 2 - 2 * px, 2 - 2 * py
    for d in range(3):
        for m in range(TERMS):
            matrix = coarse_ref[d, m].astype(F32)
            plain[d, m, 0:K2, :] = matrix
            turned[d, m, 0:K2, :] = matrix.T
    lane_level(turned, wide_y, wide_z, coarse_y, coarse_z, on_j, on_k, (1, 2 - near_y, near_y))
    spread_rows_of(coarse_rows, plain, COARSE_ROWS, 2, (1, 2 - near_x, near_x))
    own_x, _ = chosen(child_ref, px)
    own_y, _ = chosen(child_ref, py)
    up_y[...] = lane_matrix(own_y, on_j)
    for c in range(2):
        up_z[c] = lane_matrix(child_ref[:, c, :], to_natural)
    wide = dot(flipped(own_x), onehot((iota((1, 48), 1) >> 1) == iota((K2, 48), 0)))
    mixed = dot(onehot((iota((80, 1), 0) >> 2) == iota((80, K2), 1)), wide.astype(BF))
    keep = ((iota((80, 1), 0) & 3) >> 1) == (iota((1, 48), 1) & 1)
    up_rows[...] = (mixed * onehot(keep, F32)).astype(BF)


def bf16(*shape):
    return jax.ShapeDtypeStruct(shape, BF)


def early(fine_blocks, coarse_blocks, child):
    operands = [
        pltpu.with_memory_space_constraint(x, pltpu.HBM)
        for x in (fine_blocks, coarse_blocks, jnp.transpose(child, (1, 0, 2)))
    ]
    out_shape = tuple(bf16(*x.shape) for x in operands[1:]) + (
        bf16(TERMS, 2, FINE_ROWS, 128), bf16(TERMS, 3, 128, 128), bf16(3, TERMS, 128, 128),
        bf16(96, 160), bf16(256, 128), bf16(256, 128),
    )
    return pl.pallas_call(
        early_kernel, out_shape=out_shape, name="early",
        in_specs=[pl.BlockSpec(memory_space=pltpu.HBM)] * 3,
        scratch_shapes=[pltpu.VMEM(operands[0].shape, BF)] + lane_scratch() + [pltpu.SemaphoreType.DMA((3,))],
        compiler_params=pltpu.CompilerParams(vmem_limit_bytes=16 << 20),
        cost_estimate=pl.CostEstimate(flops=2 * 10**9, bytes_accessed=4 * 10**6, transcendentals=0),
    )(*operands)


def lane_scratch():
    return [pltpu.VMEM((3, TERMS, 32, K2), F32)] * 2 + [pltpu.VMEM((3, TERMS, 32, 128), BF)] * 2


def late(blocks):
    out_shape = (bf16(TERMS, 2, COARSE_ROWS, 128), bf16(TERMS, 3, 128, 128), bf16(3, TERMS, 128, 128))
    out_shape += (bf16(80, 48), bf16(128, 128), bf16(2, 128, 128))
    return small_call(late_kernel, "late", out_shape, 2 * 10**9, *blocks, scratch=lane_scratch())


def source_kernel(own, xnear, ynear, corner, down_rows, down_y, down_z,
                  packet, nears, natural, mixed, turned):
    select = onehot(iota((400, 512), 0) == natural_place(iota((1, 512), 1)))

    def converted(ref, slot):
        values = ref[0, 0].astype(F32)
        for i in range(K2):
            natural[slot, 4 * i:4 * i + 4, :] = values[:, 400 * i:400 * i + 400]
        return dot(natural[slot].astype(BF), select).astype(BF)

    centre, diagonal = converted(own, 0), converted(corner, 1)
    x_near, y_near = converted(xnear, 2), converted(ynear, 3)
    for b in range(4):
        here = slice(128 * b, 128 * b + 128)
        packet[b, 0:80, :] = centre[:, here]
        nears[0, b] = x_near[:, here]
        nears[1, b] = y_near[:, here]
    for c, (one, two) in enumerate(((centre, x_near), (y_near, diagonal))):
        rows = dot(down_rows[...], jnp.concatenate([one, two], axis=0)).astype(BF)
        for b in range(4):
            mixed[c, 96 * b:96 * b + 96, :] = rows[:, 128 * b:128 * b + 128]
    summed = dot(jnp.concatenate([mixed[0], mixed[1]], axis=1), down_y[...])
    blocks = exchange([summed[96 * b:96 * b + 96, :] for b in range(4)])
    for b in range(4):
        for c in range(2):
            turned[c, 48 * b:48 * b + 48, :] = blocks[b][48 * c:48 * c + 48, :].astype(BF)
    total = dot(jnp.concatenate([turned[0], turned[1]], axis=1), down_z[...])
    blocks = exchange([total[48 * b:48 * b + 48, :] for b in range(4)])
    for b in range(4):
        packet[b, 80:120, :] = blocks[b][0:PARENT_ROWS, :].astype(BF)


def source(columns, down_rows, down_y, down_z):
    out_shape = (
        jax.ShapeDtypeStruct((4, FINE_ROWS + PARENT_ROWS, 128), BF),
        jax.ShapeDtypeStruct((2, 4, FINE_ROWS, 128), BF),
    )
    scratch = [
        pltpu.VMEM((4, FINE_ROWS, 400), F32),
        pltpu.VMEM((2, 8 * COARSE_ROWS, 128), BF),
        pltpu.VMEM((2, 4 * COARSE_ROWS, 128), BF),
    ]
    return pl.pallas_call(
        source_kernel, out_shape=out_shape, scratch_shapes=scratch, name="source",
        compiler_params=pltpu.CompilerParams(vmem_limit_bytes=16 << 20),
        cost_estimate=pl.CostEstimate(flops=10**9, bytes_accessed=10**6, transcendentals=0),
    )(*columns, down_rows, down_y, down_z)


def joined(blocks):
    return jnp.concatenate(blocks, axis=1)


def row_pass(rows, row_mats, stacks, targets):
    stacks = [[joined(column) for column in stack] for stack in stacks]
    stacks = [(stack[0] if len(stack) == 1 else jnp.concatenate(stack, axis=0)).astype(BF) for stack in stacks]
    chunk = 3
    for stack, target in zip(stacks, targets):
        for start in range(0, TERMS, chunk):
            mats = [row_mats[start:start + chunk, c].reshape(chunk * rows, 128) for c in range(2)]
            result = dot(jnp.concatenate(mats, axis=1)[:, 0:stack.shape[0]], stack)
            for c in range(chunk):
                for b in range(4):
                    target[start + c, b * rows:b * rows + rows, :] = (
                        result[c * rows:(c + 1) * rows, 128 * b:128 * b + 128].astype(BF)
                    )


def level_rest(rows, nz, parts, y_mats, z_mats, sums, centres):
    zero = jnp.zeros((128, 128), BF)
    for m in range(TERMS):
        mats = jnp.concatenate([
            jnp.concatenate([y_mats[m, 0], y_mats[m, 1], y_mats[m, 2], zero], axis=0),
            jnp.concatenate([zero, zero, zero, y_mats[m, 0]], axis=0),
        ], axis=1)
        result = dot(jnp.concatenate([part[m] for part in parts], axis=1), mats)
        for n, target in enumerate((sums, centres)):
            blocks = exchange([result[b * rows:(b + 1) * rows, 128 * n:128 * n + 128] for b in range(4)])
            for b in range(4):
                target[m, b * rows:(b + 1) * rows, :] = blocks[b].astype(BF)
    total = dot(jnp.concatenate([sums[m] for m in range(TERMS)], axis=1), z_mats[0].reshape(TERMS * 128, 128))
    sides = dot(
        jnp.concatenate([centres[m] for m in range(TERMS)], axis=1),
        jnp.concatenate([z_mats[n].reshape(TERMS * 128, 128) for n in (1, 2)], axis=1),
    )
    z = iota((4 * rows, 128), 0) & (nz - 1)
    total = total + jnp.where(z == nz - 1, 0.0, pltpu.roll(sides[:, 0:128], 4 * rows - 1, 0))
    return total + jnp.where(z == 0, 0.0, pltpu.roll(sides[:, 128:256], 1, 0))


def level_scratch(rows):
    return [
        pltpu.VMEM((TERMS, 4 * rows, 128), BF),
        pltpu.VMEM((TERMS, 4 * rows, 128), BF),
    ]


def fine_near_kernel(packet, nears, row_mats, y_near, centre):
    own = [packet[b, 0:80, :] for b in range(4)]
    row_pass(FINE_ROWS, row_mats, ([[nears[1, b] for b in range(4)]], [own]), (y_near, centre))


def parents_kernel(x_packet, y_packet, y_parent, x_parent):
    for b in range(4):
        y_parent[b] = y_packet[b, 80:120, :]
        x_parent[b] = x_packet[b, 80:120, :]


def fine_far_kernel(packet, nears, y_packet, x_packet, row_mats, x_sum, y_far):
    own, x_far, y_column = ([ref[b, 0:80, :] for b in range(4)] for ref in (packet, x_packet, y_packet))
    stacks = ([own, [nears[0, b] for b in range(4)], x_far], [y_column])
    row_pass(FINE_ROWS, row_mats, stacks, (x_sum, y_far))


def fine_rest_kernel(x_sum, y_near, y_far, centre, y_mats, z_mats, out, sums, centres):
    out[...] = level_rest(FINE_ROWS, 4, (x_sum, y_near, y_far, centre), y_mats, z_mats, sums, centres)


def small_call(kernel, name, out_shape, flops, *operands, scratch=()):
    return pl.pallas_call(
        kernel, out_shape=out_shape, name=name, scratch_shapes=scratch,
        compiler_params=pltpu.CompilerParams(vmem_limit_bytes=16 << 20),
        cost_estimate=pl.CostEstimate(flops=flops, bytes_accessed=4 * 10**6, transcendentals=0),
    )(*operands)


def coarse_kernel(packet, xfar, xother, yfar, yother, row_mats, y_mats, z_mats,
                  up_rows, up_y, up_z, fine_term, out, wide, grown, turned,
                  x_sum, far_side, other_side, centre, *scratch):
    own = [packet[b, 80:120, :].astype(F32) for b in range(4)]
    others = [[ref[b].astype(F32) for b in range(4)] for ref in (xfar, xother, yfar, yother)]
    stacks = ([own, others[0], others[1]], [others[2]], [others[3]], [own])
    parts = (x_sum, far_side, other_side, centre)
    row_pass(COARSE_ROWS, row_mats, stacks, parts)
    result = level_rest(COARSE_ROWS, 2, parts, y_mats, z_mats, *scratch)
    blocks = exchange([result[48 * b:48 * b + 48, :] for b in range(4)])
    for b in range(4):
        wide[:, 128 * b:128 * b + 128] = blocks[b].astype(BF)
    part = dot(up_rows[...], wide[...]).astype(BF)
    for b in range(4):
        grown[80 * b:80 * b + 80, :] = part[:, 128 * b:128 * b + 128]
    part = dot(grown[...], up_y[...])
    blocks = exchange([part[80 * b:80 * b + 80, :] for b in range(4)])
    for b in range(4):
        turned[80 * b:80 * b + 80, :] = blocks[b].astype(BF)
    both = dot(turned[...], jnp.concatenate([up_z[0], up_z[1]], axis=1))
    expanded = jnp.where((iota((320, 128), 0) & 1) == 0, both[:, 0:128], both[:, 128:256])
    total = fine_term[...] + expanded
    for i in range(K2):
        for b in range(4):
            here = 400 * i + 100 * b
            out[0, 0, :, here:here + 100] = total[80 * b + 4 * i:80 * b + 4 * i + 4, 0:100]


def coarse(operands):
    part = pltpu.VMEM((TERMS, 4 * COARSE_ROWS, 128), BF)
    scratch = [
        pltpu.VMEM((COARSE_ROWS, 512), BF),
        pltpu.VMEM((320, 128), BF),
        pltpu.VMEM((320, 128), BF),
    ] + [part] * 4 + level_scratch(COARSE_ROWS)
    return small_call(
        coarse_kernel, "coarse", jax.ShapeDtypeStruct((1, 1, 4, 8000), F32), 4 * 10**9, *operands, scratch=scratch
    )


def near(block, axis):
    return lax.ppermute(block, axis, [(i, i ^ 1) for i in range(lax.axis_size(axis))])


def far(block, axis):
    count = lax.axis_size(axis)
    return lax.ppermute(block, axis, [(i, ((i + 1) ^ 1) - 1) for i in range(1, count - 1)])


def corner(block):
    nx, ny = lax.axis_size("gx"), lax.axis_size("gy")
    route = [(x * ny + y, (x ^ 1) * ny + (y ^ 1)) for x in range(nx) for y in range(ny)]
    return lax.ppermute(block, ("gx", "gy"), route)


def shards(fine_source, fine_blocks, coarse_blocks, child_filter_matrices):
    columns = [fine_source, near(fine_source, "gx"), near(fine_source, "gy"), corner(fine_source)]
    *blocks, fine_rows, fine_y, fine_z, down_rows, down_y, down_z = early(fine_blocks, coarse_blocks, child_filter_matrices)
    packet, nears = source(columns, down_rows, down_y, down_z)
    y_packet, x_packet = far(packet, "gy"), far(packet, "gx")
    mats = late(blocks)
    part = jax.ShapeDtypeStruct((TERMS, 4 * FINE_ROWS, 128), BF)
    parent = jax.ShapeDtypeStruct((4, PARENT_ROWS, 128), BF)
    y_near, centre = small_call(fine_near_kernel, "fine_near", (part, part), 10**9, packet, nears, fine_rows)
    y_parent, x_parent = small_call(parents_kernel, "parents", (parent, parent), 10**6, x_packet, y_packet)
    y_other, x_other = near(y_parent, "gy"), near(x_parent, "gx")
    x_sum, y_far = small_call(
        fine_far_kernel, "fine_far", (part, part), 10**9, packet, nears, y_packet, x_packet, fine_rows,
    )
    fine_term = small_call(
        fine_rest_kernel, "fine_rest", jax.ShapeDtypeStruct((4 * FINE_ROWS, 128), F32), 4 * 10**9,
        x_sum, y_near, y_far, centre, fine_y, fine_z, scratch=level_scratch(FINE_ROWS),
    )
    return coarse((packet, x_parent, x_other, y_parent, y_other, *mats, fine_term))


def solution(mesh):
    in_specs = (P("gx", "gy", None, None), P(), P(), P())
    out_specs = P("gx", "gy", None, None)
    return jax.shard_map(shards, mesh=mesh, in_specs=in_specs, out_specs=out_specs, check_vma=False)
```

```python
import jax
import jax.numpy as jnp
from jax import lax
from jax.experimental import pallas as pl
from jax.experimental.pallas import tpu as pltpu
from jax.sharding import PartitionSpec as P

K2 = 20
TERMS = 12
BF = jnp.bfloat16
F32 = jnp.float32
FINE_ROWS = 80
COARSE_ROWS = 48
PARENT_ROWS = 40


def iota(shape, dim):
    return lax.broadcasted_iota(jnp.int32, shape, dim)


def dot(a, b):
    return jnp.dot(a, b, preferred_element_type=F32)


def place(n):
    piece, t = n >> 5, n & 31
    jj = (t * 13) >> 6
    return piece, jj, t - 5 * jj, t < 25


def natural_place(n):
    piece, jj, kk, ok = place(n & 127)
    return jnp.where(ok, (5 * piece + jj) * 20 + 5 * (n >> 7) + kk, -1)


def onehot(condition, dtype=BF):
    return jnp.where(condition, 1.0, 0.0).astype(dtype)


def lane_constants(on_j, natural=False):
    def index(n):
        piece, jj, kk, ok = place(n)
        return jnp.where(ok, piece * 5 + (jj if on_j else kk), -1)

    def fixed(n, none):
        _, jj, kk, ok = place(n)
        return jnp.where(ok, kk if on_j else jj, none)

    spread_rows = onehot(index(iota((128, 1), 0)) == iota((128, 32), 1))
    lane = iota((1, 128), 1)
    lane_index, lane_fixed = index(lane), fixed(lane, -2)
    if natural:
        lane_fixed = (lane * 205) >> 12
        lane_index = jnp.where(lane < 100, lane - 20 * lane_fixed, -1)
        lane_fixed = jnp.where(lane < 100, lane_fixed, -2)
    spread_lanes = onehot(lane_index == iota((K2, 128), 0))
    mask = onehot(fixed(iota((128, 1), 0), -1) == lane_fixed, F32)
    return spread_rows, spread_lanes, mask


def row_constants(rows, nz):
    taken = K2 * nz
    shift = nz.bit_length() - 1
    spread_rows = onehot((iota((rows, 1), 0) >> shift) == iota((rows, 32), 1))
    wide = 256
    lane = iota((1, wide), 1)
    which = sum(jnp.where(lane >= c * taken, 1, 0) for c in range(1, 4))
    lane = lane - which * taken
    spreads = [
        onehot(jnp.where(which == c, lane >> shift, -1) == iota((K2, wide), 0)) for c in range(3)
    ]
    mask = onehot((iota((rows, 1), 0) & (nz - 1)) == (lane & (nz - 1)), F32)
    return spread_rows, spreads, mask


def flipped(matrix):
    return matrix.astype(F32).T.astype(BF)


def exchange(tiles):
    lane = iota((1, 128), 1)
    low = (lane & 64) == 0
    a, b, c, d = tiles
    a, c = jnp.where(low, a, pltpu.roll(c, 64, 1)), jnp.where(low, pltpu.roll(a, 64, 1), c)
    b, d = jnp.where(low, b, pltpu.roll(d, 64, 1)), jnp.where(low, pltpu.roll(b, 64, 1), d)
    low = (lane & 32) == 0
    a, b = jnp.where(low, a, pltpu.roll(b, 32, 1)), jnp.where(low, pltpu.roll(a, 96, 1), b)
    c, d = jnp.where(low, c, pltpu.roll(d, 32, 1)), jnp.where(low, pltpu.roll(c, 96, 1), d)
    return a, b, c, d


def spread_rows_of(out, plain, rows, nz, order):
    spread_rows, spreads, mask = row_constants(rows, nz)
    wide = sum(dot(plain[d].reshape(TERMS * 32, K2).astype(BF), spreads[c]) for c, d in enumerate(order))
    wide = wide.astype(BF).reshape(TERMS, 32, 256)
    for m in range(TERMS):
        mats = (dot(spread_rows, wide[m]) * mask).astype(BF)
        for c in range(2):
            out[m, c] = mats[:, 128 * c:128 * c + 128]


def lane_matrix(transposed, constants):
    spread_rows, spread_lanes, mask = constants
    return (dot(spread_rows[:, 0:K2], dot(transposed, spread_lanes).astype(BF)) * mask).astype(BF)


def parity():
    return lax.axis_index("gx") & 1, lax.axis_index("gy") & 1


def chosen(child_ref, which):
    first, second = child_ref[:, 0, :].astype(F32), child_ref[:, 1, :].astype(F32)
    return jnp.where(which == 0, first, second).astype(BF), jnp.where(which == 0, second, first).astype(BF)


def lane_level(turned, wide_y, wide_z, y_out, z_out, on_j, along_k, order_y):
    both = jnp.concatenate([on_j[1], along_k[1]], axis=1)
    wide = dot(turned[...].reshape(3 * TERMS * 32, K2).astype(BF), both).astype(BF)
    wide_y[...] = wide[:, 0:128].reshape(3, TERMS, 32, 128)
    wide_z[...] = wide[:, 128:256].reshape(3, TERMS, 32, 128)
    for (spread, _, mask), source_ref, order, out in (
        (on_j, wide_y, order_y, y_out), (along_k, wide_z, (1, 2, 0), z_out),
    ):
        for m in range(0, TERMS, 2):
            tiles = [source_ref[d, m + c] for c in range(2) for d in order]
            mats = dot(spread, jnp.concatenate(tiles, axis=1))
            for c in range(2):
                for e in range(3):
                    lane = 384 * c + 128 * e
                    tile = (mats[:, lane:lane + 128] * mask).astype(BF)
                    if out is y_out:
                        out[m + c, e] = tile
                    else:
                        out[e, m + c] = tile


def early_kernel(fine_hbm, coarse_hbm, child_hbm, coarse_ref, child_ref,
                 fine_rows, fine_y, fine_z, down_rows, down_y, down_z, fine_ref, plain, turned, wide_y, wide_z, sems):
    copies = [
        pltpu.make_async_copy(src, dst, sems.at[n])
        for n, (src, dst) in enumerate(((fine_hbm, fine_ref), (coarse_hbm, coarse_ref), (child_hbm, child_ref)))
    ]
    for copy in copies:
        copy.start()
    plain[...] = jnp.zeros(plain.shape, F32)
    turned[...] = jnp.zeros(turned.shape, F32)
    px, py = parity()
    on_j, on_k, to_natural = lane_constants(True), lane_constants(False), lane_constants(False, True)
    for copy in copies:
        copy.wait()
    for d in range(3):
        for m in range(TERMS):
            matrix = fine_ref[d, m].astype(F32)
            plain[d, m, 0:K2, :] = matrix
            turned[d, m, 0:K2, :] = matrix.T
    near_x, near_y = 2 - 2 * px, 2 - 2 * py
    lane_level(turned, wide_y, wide_z, fine_y, fine_z, on_j, to_natural, (1, near_y, 2 - near_y))
    spread_rows_of(fine_rows, plain, FINE_ROWS, 4, (1, near_x, 2 - near_x))
    own_x, other_x = chosen(child_ref, px)
    own_y, other_y = chosen(child_ref, py)
    down_y[0:128, :] = lane_matrix(flipped(own_y), on_j)
    down_y[128:256, :] = lane_matrix(flipped(other_y), on_j)
    for c in range(2):
        down_z[128 * c:128 * c + 128, :] = lane_matrix(flipped(child_ref[:, c, :]), on_k)
    lane = iota((1, 160), 1)
    far = lane >= 80
    lane = jnp.where(far, lane - 80, lane)
    wide = dot(own_x, onehot(jnp.where(far, -1, lane >> 2) == iota((K2, 160), 0)))
    wide = wide + dot(other_x, onehot(jnp.where(far, lane >> 2, -1) == iota((K2, 160), 0)))
    r = iota((96, 1), 0)
    cz = jnp.where(r >= 48, 1, 0)
    r = r - 48 * cz
    mixed = dot(onehot((r >> 1) == iota((96, K2), 1)), wide.astype(BF))
    down_rows[...] = (mixed * onehot((2 * (r & 1) + cz) == (lane & 3), F32)).astype(BF)


def late_kernel(coarse_ref, child_ref, coarse_rows, coarse_y, coarse_z,
                up_rows, up_y, up_z, plain, turned, wide_y, wide_z):
    plain[...] = jnp.zeros(plain.shape, F32)
    turned[...] = jnp.zeros(turned.shape, F32)
    px, py = parity()
    on_j, on_k, to_natural = lane_constants(True), lane_constants(False), lane_constants(False, True)
    near_x, near_y = 2 - 2 * px, 2 - 2 * py
    for d in range(3):
        for m in range(TERMS):
            matrix = coarse_ref[d, m].astype(F32)
            plain[d, m, 0:K2, :] = matrix
            turned[d, m, 0:K2, :] = matrix.T
    lane_level(turned, wide_y, wide_z, coarse_y, coarse_z, on_j, on_k, (1, 2 - near_y, near_y))
    spread_rows_of(coarse_rows, plain, COARSE_ROWS, 2, (1, 2 - near_x, near_x))
    own_x, _ = chosen(child_ref, px)
    own_y, _ = chosen(child_ref, py)
    up_y[...] = lane_matrix(own_y, on_j)
    for c in range(2):
        up_z[c] = lane_matrix(child_ref[:, c, :], to_natural)
    wide = dot(flipped(own_x), onehot((iota((1, 48), 1) >> 1) == iota((K2, 48), 0)))
    mixed = dot(onehot((iota((80, 1), 0) >> 2) == iota((80, K2), 1)), wide.astype(BF))
    keep = ((iota((80, 1), 0) & 3) >> 1) == (iota((1, 48), 1) & 1)
    up_rows[...] = (mixed * onehot(keep, F32)).astype(BF)


def bf16(*shape):
    return jax.ShapeDtypeStruct(shape, BF)


def early(fine_blocks, coarse_blocks, child):
    operands = [
        pltpu.with_memory_space_constraint(x, pltpu.HBM)
        for x in (fine_blocks, coarse_blocks, jnp.transpose(child, (1, 0, 2)))
    ]
    out_shape = tuple(bf16(*x.shape) for x in operands[1:]) + (
        bf16(TERMS, 2, FINE_ROWS, 128), bf16(TERMS, 3, 128, 128), bf16(3, TERMS, 128, 128),
        bf16(96, 160), bf16(256, 128), bf16(256, 128),
    )
    return pl.pallas_call(
        early_kernel, out_shape=out_shape, name="early",
        in_specs=[pl.BlockSpec(memory_space=pltpu.HBM)] * 3,
        scratch_shapes=[pltpu.VMEM(operands[0].shape, BF)] + lane_scratch() + [pltpu.SemaphoreType.DMA((3,))],
        compiler_params=pltpu.CompilerParams(vmem_limit_bytes=16 << 20),
        cost_estimate=pl.CostEstimate(flops=2 * 10**9, bytes_accessed=4 * 10**6, transcendentals=0),
    )(*operands)


def lane_scratch():
    return [pltpu.VMEM((3, TERMS, 32, K2), F32)] * 2 + [pltpu.VMEM((3, TERMS, 32, 128), BF)] * 2


def late(blocks):
    out_shape = (bf16(TERMS, 2, COARSE_ROWS, 128), bf16(TERMS, 3, 128, 128), bf16(3, TERMS, 128, 128))
    out_shape += (bf16(80, 48), bf16(128, 128), bf16(2, 128, 128))
    return small_call(late_kernel, "late", out_shape, 2 * 10**9, *blocks, scratch=lane_scratch())


def source_kernel(own, xnear, ynear, corner, down_rows, down_y, down_z,
                  packet, nears, natural, mixed, turned):
    select = onehot(iota((400, 512), 0) == natural_place(iota((1, 512), 1)))

    def converted(ref, slot):
        values = ref[0, 0].astype(F32)
        for i in range(K2):
            natural[slot, 4 * i:4 * i + 4, :] = values[:, 400 * i:400 * i + 400]
        return dot(natural[slot].astype(BF), select).astype(BF)

    centre, diagonal = converted(own, 0), converted(corner, 1)
    x_near, y_near = converted(xnear, 2), converted(ynear, 3)
    for b in range(4):
        here = slice(128 * b, 128 * b + 128)
        packet[b, 0:80, :] = centre[:, here]
        nears[0, b] = x_near[:, here]
        nears[1, b] = y_near[:, here]
    for c, (one, two) in enumerate(((centre, x_near), (y_near, diagonal))):
        rows = dot(down_rows[...], jnp.concatenate([one, two], axis=0)).astype(BF)
        for b in range(4):
            mixed[c, 96 * b:96 * b + 96, :] = rows[:, 128 * b:128 * b + 128]
    summed = dot(jnp.concatenate([mixed[0], mixed[1]], axis=1), down_y[...])
    blocks = exchange([summed[96 * b:96 * b + 96, :] for b in range(4)])
    for b in range(4):
        for c in range(2):
            turned[c, 48 * b:48 * b + 48, :] = blocks[b][48 * c:48 * c + 48, :].astype(BF)
    total = dot(jnp.concatenate([turned[0], turned[1]], axis=1), down_z[...])
    blocks = exchange([total[48 * b:48 * b + 48, :] for b in range(4)])
    for b in range(4):
        packet[b, 80:120, :] = blocks[b][0:PARENT_ROWS, :].astype(BF)


def source(columns, down_rows, down_y, down_z):
    out_shape = (
        jax.ShapeDtypeStruct((4, FINE_ROWS + PARENT_ROWS, 128), BF),
        jax.ShapeDtypeStruct((2, 4, FINE_ROWS, 128), BF),
    )
    scratch = [
        pltpu.VMEM((4, FINE_ROWS, 400), F32),
        pltpu.VMEM((2, 8 * COARSE_ROWS, 128), BF),
        pltpu.VMEM((2, 4 * COARSE_ROWS, 128), BF),
    ]
    return pl.pallas_call(
        source_kernel, out_shape=out_shape, scratch_shapes=scratch, name="source",
        compiler_params=pltpu.CompilerParams(vmem_limit_bytes=16 << 20),
        cost_estimate=pl.CostEstimate(flops=10**9, bytes_accessed=10**6, transcendentals=0),
    )(*columns, down_rows, down_y, down_z)


def joined(blocks):
    return jnp.concatenate(blocks, axis=1)


def row_pass(rows, row_mats, stacks, targets):
    stacks = [[joined(column) for column in stack] for stack in stacks]
    stacks = [(stack[0] if len(stack) == 1 else jnp.concatenate(stack, axis=0)).astype(BF) for stack in stacks]
    chunk = 3
    for stack, target in zip(stacks, targets):
        for start in range(0, TERMS, chunk):
            mats = [row_mats[start:start + chunk, c].reshape(chunk * rows, 128) for c in range(2)]
            result = dot(jnp.concatenate(mats, axis=1)[:, 0:stack.shape[0]], stack)
            for c in range(chunk):
                for b in range(4):
                    target[start + c, b * rows:b * rows + rows, :] = (
                        result[c * rows:(c + 1) * rows, 128 * b:128 * b + 128].astype(BF)
                    )


def y_pass(rows, parts, y_mats, target):
    zero = jnp.zeros((128 * len(parts), 128), BF)
    for m in range(0, TERMS, 2):
        one, two = (jnp.concatenate([y_mats[m + c, n] for n in range(len(parts))], axis=0) for c in range(2))
        mats = jnp.concatenate(
            [jnp.concatenate([one, zero], axis=0), jnp.concatenate([zero, two], axis=0)], axis=1
        )
        values = jnp.concatenate([part[m + c] for c in range(2) for part in parts], axis=1)
        result = dot(values, mats)
        for c in range(2):
            blocks = exchange([result[b * rows:(b + 1) * rows, 128 * c:128 * c + 128] for b in range(4)])
            for b in range(4):
                target[m + c, b * rows:(b + 1) * rows, :] = blocks[b].astype(BF)


def level_vertical(rows, nz, centre, y_mats, z_mats, scratch):
    y_pass(rows, (centre,), y_mats, scratch)
    sides = dot(
        joined([scratch[m] for m in range(TERMS)]),
        joined([z_mats[n].reshape(TERMS * 128, 128) for n in (1, 2)]),
    )
    z = iota((4 * rows, 128), 0) & (nz - 1)
    upper = jnp.where(z == nz - 1, 0.0, pltpu.roll(sides[:, 0:128], 4 * rows - 1, 0))
    return upper + jnp.where(z == 0, 0.0, pltpu.roll(sides[:, 128:256], 1, 0))


def level_rest(rows, parts, y_mats, z_mats, scratch):
    y_pass(rows, parts, y_mats, scratch)
    return dot(joined([scratch[m] for m in range(TERMS)]), z_mats[0].reshape(TERMS * 128, 128))


def fine_near_kernel(packet, nears, row_mats, y_mats, z_mats, y_near, vertical, centre, scratch):
    own = [packet[b, 0:80, :] for b in range(4)]
    row_pass(FINE_ROWS, row_mats, ([[nears[1, b] for b in range(4)]], [own]), (y_near, centre))
    vertical[...] = level_vertical(FINE_ROWS, 4, centre, y_mats, z_mats, scratch)


def coarse_near_kernel(packet, row_mats, y_mats, z_mats, vertical, centre, scratch):
    own = [packet[b, 80:120, :].astype(F32) for b in range(4)]
    row_pass(COARSE_ROWS, row_mats, ([own],), (centre,))
    vertical[...] = level_vertical(COARSE_ROWS, 2, centre, y_mats, z_mats, scratch)


def parents_kernel(y_packet, x_packet, y_parent, x_parent):
    for b in range(4):
        y_parent[b] = y_packet[b, 80:120, :]
        x_parent[b] = x_packet[b, 80:120, :]


def fine_far_kernel(packet, nears, y_packet, x_packet, row_mats, x_sum, y_far):
    own, x_far, y_column = ([ref[b, 0:80, :] for b in range(4)] for ref in (packet, x_packet, y_packet))
    stacks = ([own, [nears[0, b] for b in range(4)], x_far], [y_column])
    row_pass(FINE_ROWS, row_mats, stacks, (x_sum, y_far))


def fine_rest_kernel(x_sum, y_near, y_far, vertical, y_mats, z_mats, out, scratch):
    out[...] = vertical[...] + level_rest(FINE_ROWS, (x_sum, y_near, y_far), y_mats, z_mats, scratch)


def small_call(kernel, name, out_shape, flops, *operands, scratch=()):
    return pl.pallas_call(
        kernel, out_shape=out_shape, name=name, scratch_shapes=scratch,
        compiler_params=pltpu.CompilerParams(vmem_limit_bytes=16 << 20),
        cost_estimate=pl.CostEstimate(flops=flops, bytes_accessed=4 * 10**6, transcendentals=0),
    )(*operands)


def coarse_kernel(packet, xfar, xother, yfar, yother, vertical, row_mats, y_mats, z_mats,
                  up_rows, up_y, up_z, fine_term, out, wide, grown, turned, x_sum, far_side, other_side, scratch):
    own = [packet[b, 80:120, :].astype(F32) for b in range(4)]
    others = [[ref[b].astype(F32) for b in range(4)] for ref in (xfar, xother, yfar, yother)]
    parts = (x_sum, far_side, other_side)
    row_pass(COARSE_ROWS, row_mats, ([own, others[0], others[1]], [others[2]], [others[3]]), parts)
    result = vertical[...] + level_rest(COARSE_ROWS, parts, y_mats, z_mats, scratch)
    blocks = exchange([result[48 * b:48 * b + 48, :] for b in range(4)])
    for b in range(4):
        wide[:, 128 * b:128 * b + 128] = blocks[b].astype(BF)
    part = dot(up_rows[...], wide[...]).astype(BF)
    for b in range(4):
        grown[80 * b:80 * b + 80, :] = part[:, 128 * b:128 * b + 128]
    part = dot(grown[...], up_y[...])
    blocks = exchange([part[80 * b:80 * b + 80, :] for b in range(4)])
    for b in range(4):
        turned[80 * b:80 * b + 80, :] = blocks[b].astype(BF)
    both = dot(turned[...], jnp.concatenate([up_z[0], up_z[1]], axis=1))
    expanded = jnp.where((iota((320, 128), 0) & 1) == 0, both[:, 0:128], both[:, 128:256])
    total = fine_term[...] + expanded
    for i in range(K2):
        for b in range(4):
            here = 400 * i + 100 * b
            out[0, 0, :, here:here + 100] = total[80 * b + 4 * i:80 * b + 4 * i + 4, 0:100]


def coarse(operands):
    part = pltpu.VMEM((TERMS, 4 * COARSE_ROWS, 128), BF)
    scratch = [
        pltpu.VMEM((COARSE_ROWS, 512), BF),
        pltpu.VMEM((320, 128), BF),
        pltpu.VMEM((320, 128), BF),
    ] + [part] * 4
    return small_call(
        coarse_kernel, "coarse", jax.ShapeDtypeStruct((1, 1, 4, 8000), F32), 4 * 10**9, *operands, scratch=scratch
    )


def near(block, axis):
    return lax.ppermute(block, axis, [(i, i ^ 1) for i in range(lax.axis_size(axis))])


def far(block, axis):
    count = lax.axis_size(axis)
    return lax.ppermute(block, axis, [(i, ((i + 1) ^ 1) - 1) for i in range(1, count - 1)])


def corner(block):
    nx, ny = lax.axis_size("gx"), lax.axis_size("gy")
    route = [(x * ny + y, (x ^ 1) * ny + (y ^ 1)) for x in range(nx) for y in range(ny)]
    return lax.ppermute(block, ("gx", "gy"), route)


def shards(fine_source, fine_blocks, coarse_blocks, child_filter_matrices):
    columns = [fine_source, near(fine_source, "gx"), near(fine_source, "gy"), corner(fine_source)]
    *blocks, fine_rows, fine_y, fine_z, down_rows, down_y, down_z = early(fine_blocks, coarse_blocks, child_filter_matrices)
    packet, nears = source(columns, down_rows, down_y, down_z)
    y_packet, x_packet = far(packet, "gy"), far(packet, "gx")
    blocks, _ = lax.optimization_barrier((tuple(blocks), packet))
    mats = late(blocks)
    part = jax.ShapeDtypeStruct((TERMS, 4 * FINE_ROWS, 128), BF)
    parent = jax.ShapeDtypeStruct((4, PARENT_ROWS, 128), BF)
    fine_part = pltpu.VMEM((TERMS, 4 * FINE_ROWS, 128), BF)
    coarse_part = pltpu.VMEM((TERMS, 4 * COARSE_ROWS, 128), BF)
    fine_sum = jax.ShapeDtypeStruct((4 * FINE_ROWS, 128), F32)
    coarse_sum = jax.ShapeDtypeStruct((4 * COARSE_ROWS, 128), F32)
    y_near, fine_vertical = small_call(
        fine_near_kernel, "fine_near", (part, fine_sum), 2 * 10**9,
        packet, nears, fine_rows, fine_y, fine_z, scratch=[fine_part] * 2,
    )
    coarse_vertical = small_call(
        coarse_near_kernel, "coarse_near", coarse_sum, 10**9, packet, *mats[0:3], scratch=[coarse_part] * 2,
    )
    y_parent, x_parent = small_call(parents_kernel, "parents", (parent, parent), 10**6, y_packet, x_packet)
    y_other, x_other = near(y_parent, "gy"), near(x_parent, "gx")
    x_sum, y_far = small_call(
        fine_far_kernel, "fine_far", (part, part), 10**9, packet, nears, y_packet, x_packet, fine_rows,
    )
    fine_term = small_call(
        fine_rest_kernel, "fine_rest", fine_sum, 4 * 10**9,
        x_sum, y_near, y_far, fine_vertical, fine_y, fine_z, scratch=[fine_part],
    )
    return coarse((packet, x_parent, x_other, y_parent, y_other, coarse_vertical, *mats, fine_term))


def solution(mesh):
    in_specs = (P("gx", "gy", None, None), P(), P(), P())
    out_specs = P("gx", "gy", None, None)
    return jax.shard_map(shards, mesh=mesh, in_specs=in_specs, out_specs=out_specs, check_vma=False)
```

```python
import jax
import jax.numpy as jnp
from jax import lax
from jax.experimental import pallas as pl
from jax.experimental.pallas import tpu as pltpu
from jax.sharding import PartitionSpec as P

K2 = 20
TERMS = 12
BF = jnp.bfloat16
F32 = jnp.float32
FINE_ROWS = 80
COARSE_ROWS = 48
PARENT_ROWS = 40


def iota(shape, dim):
    return lax.broadcasted_iota(jnp.int32, shape, dim)


def dot(a, b):
    return jnp.dot(a, b, preferred_element_type=F32)


def place(n):
    piece, t = n >> 5, n & 31
    jj = (t * 13) >> 6
    return piece, jj, t - 5 * jj, t < 25


def natural_place(n):
    piece, jj, kk, ok = place(n & 127)
    return jnp.where(ok, (5 * piece + jj) * 20 + 5 * (n >> 7) + kk, -1)


def onehot(condition, dtype=BF):
    return jnp.where(condition, 1.0, 0.0).astype(dtype)


def lane_constants(on_j, natural=False):
    def index(n):
        piece, jj, kk, ok = place(n)
        return jnp.where(ok, piece * 5 + (jj if on_j else kk), -1)

    def fixed(n, none):
        _, jj, kk, ok = place(n)
        return jnp.where(ok, kk if on_j else jj, none)

    spread_rows = onehot(index(iota((128, 1), 0)) == iota((128, 32), 1))
    lane = iota((1, 128), 1)
    lane_index, lane_fixed = index(lane), fixed(lane, -2)
    if natural:
        lane_fixed = (lane * 205) >> 12
        lane_index = jnp.where(lane < 100, lane - 20 * lane_fixed, -1)
        lane_fixed = jnp.where(lane < 100, lane_fixed, -2)
    spread_lanes = onehot(lane_index == iota((K2, 128), 0))
    mask = onehot(fixed(iota((128, 1), 0), -1) == lane_fixed, F32)
    return spread_rows, spread_lanes, mask


def row_constants(rows, nz):
    taken = K2 * nz
    shift = nz.bit_length() - 1
    spread_rows = onehot((iota((rows, 1), 0) >> shift) == iota((rows, 32), 1))
    wide = 256
    lane = iota((1, wide), 1)
    which = sum(jnp.where(lane >= c * taken, 1, 0) for c in range(1, 4))
    lane = lane - which * taken
    spreads = [
        onehot(jnp.where(which == c, lane >> shift, -1) == iota((K2, wide), 0)) for c in range(3)
    ]
    mask = onehot((iota((rows, 1), 0) & (nz - 1)) == (lane & (nz - 1)), F32)
    return spread_rows, spreads, mask


def flipped(matrix):
    return matrix.astype(F32).T.astype(BF)


def exchange(tiles):
    lane = iota((1, 128), 1)
    low = (lane & 64) == 0
    a, b, c, d = tiles
    a, c = jnp.where(low, a, pltpu.roll(c, 64, 1)), jnp.where(low, pltpu.roll(a, 64, 1), c)
    b, d = jnp.where(low, b, pltpu.roll(d, 64, 1)), jnp.where(low, pltpu.roll(b, 64, 1), d)
    low = (lane & 32) == 0
    a, b = jnp.where(low, a, pltpu.roll(b, 32, 1)), jnp.where(low, pltpu.roll(a, 96, 1), b)
    c, d = jnp.where(low, c, pltpu.roll(d, 32, 1)), jnp.where(low, pltpu.roll(c, 96, 1), d)
    return a, b, c, d


def spread_rows_of(out, plain, rows, nz, order):
    spread_rows, spreads, mask = row_constants(rows, nz)
    wide = sum(dot(plain[d].reshape(TERMS * 32, K2).astype(BF), spreads[c]) for c, d in enumerate(order))
    wide = wide.astype(BF).reshape(TERMS, 32, 256)
    for m in range(TERMS):
        mats = (dot(spread_rows, wide[m]) * mask).astype(BF)
        for c in range(2):
            out[m, c] = mats[:, 128 * c:128 * c + 128]


def lane_matrix(transposed, constants):
    spread_rows, spread_lanes, mask = constants
    return (dot(spread_rows[:, 0:K2], dot(transposed, spread_lanes).astype(BF)) * mask).astype(BF)


def parity():
    return lax.axis_index("gx") & 1, lax.axis_index("gy") & 1


def chosen(child_ref, which):
    first, second = child_ref[:, 0, :].astype(F32), child_ref[:, 1, :].astype(F32)
    return jnp.where(which == 0, first, second).astype(BF), jnp.where(which == 0, second, first).astype(BF)


def lane_level(turned, wide_y, wide_z, y_out, z_out, on_j, along_k, order_y):
    both = jnp.concatenate([on_j[1], along_k[1]], axis=1)
    wide = dot(turned[...].reshape(3 * TERMS * 32, K2).astype(BF), both).astype(BF)
    wide_y[...] = wide[:, 0:128].reshape(3, TERMS, 32, 128)
    wide_z[...] = wide[:, 128:256].reshape(3, TERMS, 32, 128)
    for (spread, _, mask), source_ref, order, out in (
        (on_j, wide_y, order_y, y_out), (along_k, wide_z, (1, 2, 0), z_out),
    ):
        for m in range(0, TERMS, 2):
            tiles = [source_ref[d, m + c] for c in range(2) for d in order]
            mats = dot(spread, jnp.concatenate(tiles, axis=1))
            for c in range(2):
                for e in range(3):
                    lane = 384 * c + 128 * e
                    tile = (mats[:, lane:lane + 128] * mask).astype(BF)
                    if out is y_out:
                        out[m + c, e] = tile
                    else:
                        out[e, m + c] = tile


def converted(ref, natural, select):
    values = ref[0, 0].astype(F32)
    for i in range(K2):
        natural[4 * i:4 * i + 4, :] = values[:, 400 * i:400 * i + 400]
    return dot(natural[...].astype(BF), select[...]).astype(BF)


def early_kernel(fine_hbm, coarse_hbm, child_hbm, own_hbm, coarse_ref, child_ref, own_blocks, select_out,
                 fine_rows, fine_y, fine_z, down_rows, down_y, down_z, fine_ref, own_ref, natural, plain, turned, wide_y, wide_z, sems):
    copies = [
        pltpu.make_async_copy(src, dst, sems.at[n])
        for n, (src, dst) in enumerate((
            (fine_hbm, fine_ref), (coarse_hbm, coarse_ref), (child_hbm, child_ref), (own_hbm, own_ref),
        ))
    ]
    for copy in copies:
        copy.start()
    plain[...] = jnp.zeros(plain.shape, F32)
    turned[...] = jnp.zeros(turned.shape, F32)
    px, py = parity()
    on_j, on_k, to_natural = lane_constants(True), lane_constants(False), lane_constants(False, True)
    for copy in copies:
        copy.wait()
    for d in range(3):
        for m in range(TERMS):
            matrix = fine_ref[d, m].astype(F32)
            plain[d, m, 0:K2, :] = matrix
            turned[d, m, 0:K2, :] = matrix.T
    near_x, near_y = 2 - 2 * px, 2 - 2 * py
    lane_level(turned, wide_y, wide_z, fine_y, fine_z, on_j, to_natural, (1, near_y, 2 - near_y))
    spread_rows_of(fine_rows, plain, FINE_ROWS, 4, (1, near_x, 2 - near_x))
    own_x, other_x = chosen(child_ref, px)
    own_y, other_y = chosen(child_ref, py)
    down_y[0:128, :] = lane_matrix(flipped(own_y), on_j)
    down_y[128:256, :] = lane_matrix(flipped(other_y), on_j)
    for c in range(2):
        down_z[128 * c:128 * c + 128, :] = lane_matrix(flipped(child_ref[:, c, :]), on_k)
    select_out[...] = onehot(iota((400, 512), 0) == natural_place(iota((1, 512), 1)))
    centre = converted(own_ref, natural, select_out)
    for b in range(4):
        own_blocks[b] = centre[:, 128 * b:128 * b + 128]
    lane = iota((1, 160), 1)
    far = lane >= 80
    lane = jnp.where(far, lane - 80, lane)
    wide = dot(own_x, onehot(jnp.where(far, -1, lane >> 2) == iota((K2, 160), 0)))
    wide = wide + dot(other_x, onehot(jnp.where(far, lane >> 2, -1) == iota((K2, 160), 0)))
    r = iota((96, 1), 0)
    cz = jnp.where(r >= 48, 1, 0)
    r = r - 48 * cz
    mixed = dot(onehot((r >> 1) == iota((96, K2), 1)), wide.astype(BF))
    down_rows[...] = (mixed * onehot((2 * (r & 1) + cz) == (lane & 3), F32)).astype(BF)


def late_kernel(coarse_ref, child_ref, coarse_rows, coarse_y, coarse_z,
                up_rows, up_y, up_z, plain, turned, wide_y, wide_z):
    plain[...] = jnp.zeros(plain.shape, F32)
    turned[...] = jnp.zeros(turned.shape, F32)
    px, py = parity()
    on_j, on_k, to_natural = lane_constants(True), lane_constants(False), lane_constants(False, True)
    near_x, near_y = 2 - 2 * px, 2 - 2 * py
    for d in range(3):
        for m in range(TERMS):
            matrix = coarse_ref[d, m].astype(F32)
            plain[d, m, 0:K2, :] = matrix
            turned[d, m, 0:K2, :] = matrix.T
    lane_level(turned, wide_y, wide_z, coarse_y, coarse_z, on_j, on_k, (1, 2 - near_y, near_y))
    spread_rows_of(coarse_rows, plain, COARSE_ROWS, 2, (1, 2 - near_x, near_x))
    own_x, _ = chosen(child_ref, px)
    own_y, _ = chosen(child_ref, py)
    up_y[...] = lane_matrix(own_y, on_j)
    for c in range(2):
        up_z[c] = lane_matrix(child_ref[:, c, :], to_natural)
    wide = dot(flipped(own_x), onehot((iota((1, 48), 1) >> 1) == iota((K2, 48), 0)))
    mixed = dot(onehot((iota((80, 1), 0) >> 2) == iota((80, K2), 1)), wide.astype(BF))
    keep = ((iota((80, 1), 0) & 3) >> 1) == (iota((1, 48), 1) & 1)
    up_rows[...] = (mixed * onehot(keep, F32)).astype(BF)


def bf16(*shape):
    return jax.ShapeDtypeStruct(shape, BF)


def early(fine_blocks, coarse_blocks, child, own):
    operands = [
        pltpu.with_memory_space_constraint(x, pltpu.HBM)
        for x in (fine_blocks, coarse_blocks, jnp.transpose(child, (1, 0, 2)), own)
    ]
    out_shape = tuple(bf16(*x.shape) for x in operands[1:3]) + (
        bf16(4, FINE_ROWS, 128), bf16(400, 512),
        bf16(TERMS, 2, FINE_ROWS, 128), bf16(TERMS, 3, 128, 128), bf16(3, TERMS, 128, 128),
        bf16(96, 160), bf16(256, 128), bf16(256, 128),
    )
    return pl.pallas_call(
        early_kernel, out_shape=out_shape, name="early",
        in_specs=[pl.BlockSpec(memory_space=pltpu.HBM)] * 4,
        scratch_shapes=[
            pltpu.VMEM(operands[0].shape, BF), pltpu.VMEM(operands[3].shape, BF), pltpu.VMEM((FINE_ROWS, 400), F32),
        ] + lane_scratch() + [pltpu.SemaphoreType.DMA((4,))],
        compiler_params=pltpu.CompilerParams(vmem_limit_bytes=16 << 20),
        cost_estimate=pl.CostEstimate(flops=2 * 10**9, bytes_accessed=4 * 10**6, transcendentals=0),
    )(*operands)


def lane_scratch():
    return [pltpu.VMEM((3, TERMS, 32, K2), F32)] * 2 + [pltpu.VMEM((3, TERMS, 32, 128), BF)] * 2


def late(blocks):
    out_shape = (bf16(TERMS, 2, COARSE_ROWS, 128), bf16(TERMS, 3, 128, 128), bf16(3, TERMS, 128, 128))
    out_shape += (bf16(80, 48), bf16(128, 128), bf16(2, 128, 128))
    return small_call(late_kernel, "late", out_shape, 2 * 10**9, *blocks, scratch=lane_scratch())


def source_kernel(own, select, xnear, ynear, corner, down_rows, down_y, down_z,
                  packet, nears, natural, mixed, turned):
    centre, diagonal = joined([own[b] for b in range(4)]), converted(corner, natural.at[0], select)
    x_near, y_near = converted(xnear, natural.at[1], select), converted(ynear, natural.at[2], select)
    for b in range(4):
        here = slice(128 * b, 128 * b + 128)
        packet[b, 0:80, :] = centre[:, here]
        nears[0, b] = x_near[:, here]
        nears[1, b] = y_near[:, here]
    for c, (one, two) in enumerate(((centre, x_near), (y_near, diagonal))):
        rows = dot(down_rows[...], jnp.concatenate([one, two], axis=0)).astype(BF)
        for b in range(4):
            mixed[c, 96 * b:96 * b + 96, :] = rows[:, 128 * b:128 * b + 128]
    summed = dot(jnp.concatenate([mixed[0], mixed[1]], axis=1), down_y[...])
    blocks = exchange([summed[96 * b:96 * b + 96, :] for b in range(4)])
    for b in range(4):
        for c in range(2):
            turned[c, 48 * b:48 * b + 48, :] = blocks[b][48 * c:48 * c + 48, :].astype(BF)
    total = dot(jnp.concatenate([turned[0], turned[1]], axis=1), down_z[...])
    blocks = exchange([total[48 * b:48 * b + 48, :] for b in range(4)])
    for b in range(4):
        packet[b, 80:120, :] = blocks[b][0:PARENT_ROWS, :].astype(BF)


def source(columns, down_rows, down_y, down_z):
    out_shape = (
        jax.ShapeDtypeStruct((4, FINE_ROWS + PARENT_ROWS, 128), BF),
        jax.ShapeDtypeStruct((2, 4, FINE_ROWS, 128), BF),
    )
    scratch = [
        pltpu.VMEM((3, FINE_ROWS, 400), F32),
        pltpu.VMEM((2, 8 * COARSE_ROWS, 128), BF),
        pltpu.VMEM((2, 4 * COARSE_ROWS, 128), BF),
    ]
    return pl.pallas_call(
        source_kernel, out_shape=out_shape, scratch_shapes=scratch, name="source",
        compiler_params=pltpu.CompilerParams(vmem_limit_bytes=16 << 20),
        cost_estimate=pl.CostEstimate(flops=10**9, bytes_accessed=10**6, transcendentals=0),
    )(*columns, down_rows, down_y, down_z)


def joined(blocks):
    return jnp.concatenate(blocks, axis=1)


def row_pass(rows, row_mats, stacks, targets):
    stacks = [[joined(column) for column in stack] for stack in stacks]
    stacks = [(stack[0] if len(stack) == 1 else jnp.concatenate(stack, axis=0)).astype(BF) for stack in stacks]
    chunk = 3
    for stack, target in zip(stacks, targets):
        for start in range(0, TERMS, chunk):
            mats = [row_mats[start:start + chunk, c].reshape(chunk * rows, 128) for c in range(2)]
            result = dot(jnp.concatenate(mats, axis=1)[:, 0:stack.shape[0]], stack)
            for c in range(chunk):
                for b in range(4):
                    target[start + c, b * rows:b * rows + rows, :] = (
                        result[c * rows:(c + 1) * rows, 128 * b:128 * b + 128].astype(BF)
                    )


def y_pass(rows, parts, y_mats, target):
    zero = jnp.zeros((128 * len(parts), 128), BF)
    for m in range(0, TERMS, 2):
        one, two = (jnp.concatenate([y_mats[m + c, n] for n in range(len(parts))], axis=0) for c in range(2))
        mats = jnp.concatenate(
            [jnp.concatenate([one, zero], axis=0), jnp.concatenate([zero, two], axis=0)], axis=1
        )
        values = jnp.concatenate([part[m + c] for c in range(2) for part in parts], axis=1)
        result = dot(values, mats)
        for c in range(2):
            blocks = exchange([result[b * rows:(b + 1) * rows, 128 * c:128 * c + 128] for b in range(4)])
            for b in range(4):
                target[m + c, b * rows:(b + 1) * rows, :] = blocks[b].astype(BF)


def level_vertical(rows, nz, centre, y_mats, z_mats, scratch):
    y_pass(rows, (centre,), y_mats, scratch)
    sides = dot(
        joined([scratch[m] for m in range(TERMS)]),
        joined([z_mats[n].reshape(TERMS * 128, 128) for n in (1, 2)]),
    )
    z = iota((4 * rows, 128), 0) & (nz - 1)
    upper = jnp.where(z == nz - 1, 0.0, pltpu.roll(sides[:, 0:128], 4 * rows - 1, 0))
    return upper + jnp.where(z == 0, 0.0, pltpu.roll(sides[:, 128:256], 1, 0))


def level_rest(rows, parts, y_mats, z_mats, scratch):
    y_pass(rows, parts, y_mats, scratch)
    return dot(joined([scratch[m] for m in range(TERMS)]), z_mats[0].reshape(TERMS * 128, 128))


def fine_near_kernel(packet, nears, row_mats, y_mats, z_mats, y_near, vertical, centre, scratch):
    own = [packet[b, 0:80, :] for b in range(4)]
    row_pass(FINE_ROWS, row_mats, ([[nears[1, b] for b in range(4)]], [own]), (y_near, centre))
    vertical[...] = level_vertical(FINE_ROWS, 4, centre, y_mats, z_mats, scratch)


def coarse_near_kernel(packet, row_mats, y_mats, z_mats, vertical, centre, scratch):
    own = [packet[b, 80:120, :].astype(F32) for b in range(4)]
    row_pass(COARSE_ROWS, row_mats, ([own],), (centre,))
    vertical[...] = level_vertical(COARSE_ROWS, 2, centre, y_mats, z_mats, scratch)


def parents_kernel(y_packet, x_packet, y_parent, x_parent):
    for b in range(4):
        y_parent[b] = y_packet[b, 80:120, :]
        x_parent[b] = x_packet[b, 80:120, :]


def fine_far_kernel(packet, nears, y_packet, x_packet, row_mats, x_sum, y_far):
    own, x_far, y_column = ([ref[b, 0:80, :] for b in range(4)] for ref in (packet, x_packet, y_packet))
    stacks = ([own, [nears[0, b] for b in range(4)], x_far], [y_column])
    row_pass(FINE_ROWS, row_mats, stacks, (x_sum, y_far))


def fine_rest_kernel(x_sum, y_near, y_far, vertical, y_mats, z_mats, out, scratch):
    out[...] = vertical[...] + level_rest(FINE_ROWS, (x_sum, y_near, y_far), y_mats, z_mats, scratch)


def small_call(kernel, name, out_shape, flops, *operands, scratch=()):
    return pl.pallas_call(
        kernel, out_shape=out_shape, name=name, scratch_shapes=scratch,
        compiler_params=pltpu.CompilerParams(vmem_limit_bytes=16 << 20),
        cost_estimate=pl.CostEstimate(flops=flops, bytes_accessed=4 * 10**6, transcendentals=0),
    )(*operands)


def coarse_kernel(packet, yfar, yother, xfar, xother, vertical, row_mats, y_mats, z_mats,
                  up_rows, up_y, up_z, fine_term, out, wide, grown, turned, x_sum, far_side, other_side, scratch):
    own = [packet[b, 80:120, :].astype(F32) for b in range(4)]
    others = [[ref[b].astype(F32) for b in range(4)] for ref in (xfar, xother, yfar, yother)]
    parts = (x_sum, far_side, other_side)
    row_pass(COARSE_ROWS, row_mats, ([own, others[0], others[1]], [others[2]], [others[3]]), parts)
    result = vertical[...] + level_rest(COARSE_ROWS, parts, y_mats, z_mats, scratch)
    blocks = exchange([result[48 * b:48 * b + 48, :] for b in range(4)])
    for b in range(4):
        wide[:, 128 * b:128 * b + 128] = blocks[b].astype(BF)
    part = dot(up_rows[...], wide[...]).astype(BF)
    for b in range(4):
        grown[80 * b:80 * b + 80, :] = part[:, 128 * b:128 * b + 128]
    part = dot(grown[...], up_y[...])
    blocks = exchange([part[80 * b:80 * b + 80, :] for b in range(4)])
    for b in range(4):
        turned[80 * b:80 * b + 80, :] = blocks[b].astype(BF)
    both = dot(turned[...], jnp.concatenate([up_z[0], up_z[1]], axis=1))
    expanded = jnp.where((iota((320, 128), 0) & 1) == 0, both[:, 0:128], both[:, 128:256])
    total = fine_term[...] + expanded
    for i in range(K2):
        for b in range(4):
            here = 400 * i + 100 * b
            out[0, 0, :, here:here + 100] = total[80 * b + 4 * i:80 * b + 4 * i + 4, 0:100]


def coarse(operands):
    part = pltpu.VMEM((TERMS, 4 * COARSE_ROWS, 128), BF)
    scratch = [
        pltpu.VMEM((COARSE_ROWS, 512), BF),
        pltpu.VMEM((320, 128), BF),
        pltpu.VMEM((320, 128), BF),
    ] + [part] * 4
    return small_call(
        coarse_kernel, "coarse", jax.ShapeDtypeStruct((1, 1, 4, 8000), F32), 4 * 10**9, *operands, scratch=scratch
    )


def near(block, axis):
    return lax.ppermute(block, axis, [(i, i ^ 1) for i in range(lax.axis_size(axis))])


def far(block, axis):
    count = lax.axis_size(axis)
    return lax.ppermute(block, axis, [(i, ((i + 1) ^ 1) - 1) for i in range(1, count - 1)])


def corner(block):
    nx, ny = lax.axis_size("gx"), lax.axis_size("gy")
    route = [(x * ny + y, (x ^ 1) * ny + (y ^ 1)) for x in range(nx) for y in range(ny)]
    return lax.ppermute(block, ("gx", "gy"), route)


def shards(fine_source, fine_blocks, coarse_blocks, child_filter_matrices):
    columns = [near(fine_source, "gx"), near(fine_source, "gy"), corner(fine_source)]
    coarse_ref, child_ref, own, select, fine_rows, fine_y, fine_z, *down = early(
        fine_blocks, coarse_blocks, child_filter_matrices, fine_source
    )
    packet, nears = source([own, select] + columns, *down)
    y_packet, x_packet = far(packet, "gy"), far(packet, "gx")
    blocks, _ = lax.optimization_barrier(((coarse_ref, child_ref), packet))
    mats = late(blocks)
    part = jax.ShapeDtypeStruct((TERMS, 4 * FINE_ROWS, 128), BF)
    parent = jax.ShapeDtypeStruct((4, PARENT_ROWS, 128), BF)
    fine_part = pltpu.VMEM((TERMS, 4 * FINE_ROWS, 128), BF)
    coarse_part = pltpu.VMEM((TERMS, 4 * COARSE_ROWS, 128), BF)
    fine_sum = jax.ShapeDtypeStruct((4 * FINE_ROWS, 128), F32)
    coarse_sum = jax.ShapeDtypeStruct((4 * COARSE_ROWS, 128), F32)
    y_near, fine_vertical = small_call(
        fine_near_kernel, "fine_near", (part, fine_sum), 2 * 10**9,
        packet, nears, fine_rows, fine_y, fine_z, scratch=[fine_part] * 2,
    )
    coarse_vertical = small_call(
        coarse_near_kernel, "coarse_near", coarse_sum, 10**9, packet, *mats[0:3], scratch=[coarse_part] * 2,
    )
    y_parent, x_parent = small_call(parents_kernel, "parents", (parent, parent), 10**6, y_packet, x_packet)
    y_other, x_other = near(y_parent, "gy"), near(x_parent, "gx")
    x_sum, y_far = small_call(
        fine_far_kernel, "fine_far", (part, part), 10**9, packet, nears, y_packet, x_packet, fine_rows,
    )
    fine_term = small_call(
        fine_rest_kernel, "fine_rest", fine_sum, 4 * 10**9,
        x_sum, y_near, y_far, fine_vertical, fine_y, fine_z, scratch=[fine_part],
    )
    return coarse((packet, y_parent, y_other, x_parent, x_other, coarse_vertical, *mats, fine_term))


def solution(mesh):
    in_specs = (P("gx", "gy", None, None), P(), P(), P())
    out_specs = P("gx", "gy", None, None)
    return jax.shard_map(shards, mesh=mesh, in_specs=in_specs, out_specs=out_specs, check_vma=False)
```

```python
import jax
import jax.numpy as jnp
from jax import lax
from jax.experimental import pallas as pl
from jax.experimental.pallas import tpu as pltpu
from jax.sharding import PartitionSpec as P

K2 = 20
TERMS = 12
BF = jnp.bfloat16
F32 = jnp.float32
FINE_ROWS = 80
COARSE_ROWS = 48
PARENT_ROWS = 40


def iota(shape, dim):
    return lax.broadcasted_iota(jnp.int32, shape, dim)


def dot(a, b):
    return jnp.dot(a, b, preferred_element_type=F32)


def place(n):
    piece, t = n >> 5, n & 31
    jj = (t * 13) >> 6
    return piece, jj, t - 5 * jj, t < 25


def natural_place(n):
    piece, jj, kk, ok = place(n & 127)
    return jnp.where(ok, (5 * piece + jj) * 20 + 5 * (n >> 7) + kk, -1)


def onehot(condition, dtype=BF):
    return jnp.where(condition, 1.0, 0.0).astype(dtype)


def lane_constants(on_j, natural=False):
    def index(n):
        piece, jj, kk, ok = place(n)
        return jnp.where(ok, piece * 5 + (jj if on_j else kk), -1)

    def fixed(n, none):
        _, jj, kk, ok = place(n)
        return jnp.where(ok, kk if on_j else jj, none)

    spread_rows = onehot(index(iota((128, 1), 0)) == iota((128, 32), 1))
    lane = iota((1, 128), 1)
    lane_index, lane_fixed = index(lane), fixed(lane, -2)
    if natural:
        lane_fixed = (lane * 205) >> 12
        lane_index = jnp.where(lane < 100, lane - 20 * lane_fixed, -1)
        lane_fixed = jnp.where(lane < 100, lane_fixed, -2)
    spread_lanes = onehot(lane_index == iota((K2, 128), 0))
    mask = onehot(fixed(iota((128, 1), 0), -1) == lane_fixed, F32)
    return spread_rows, spread_lanes, mask


def row_constants(rows, nz):
    taken = K2 * nz
    shift = nz.bit_length() - 1
    spread_rows = onehot((iota((rows, 1), 0) >> shift) == iota((rows, 32), 1))
    wide = 256
    lane = iota((1, wide), 1)
    which = sum(jnp.where(lane >= c * taken, 1, 0) for c in range(1, 4))
    lane = lane - which * taken
    spreads = [
        onehot(jnp.where(which == c, lane >> shift, -1) == iota((K2, wide), 0)) for c in range(3)
    ]
    mask = onehot((iota((rows, 1), 0) & (nz - 1)) == (lane & (nz - 1)), F32)
    return spread_rows, spreads, mask


def flipped(matrix):
    return matrix.astype(F32).T.astype(BF)


def exchange(tiles):
    lane = iota((1, 128), 1)
    low = (lane & 64) == 0
    a, b, c, d = tiles
    a, c = jnp.where(low, a, pltpu.roll(c, 64, 1)), jnp.where(low, pltpu.roll(a, 64, 1), c)
    b, d = jnp.where(low, b, pltpu.roll(d, 64, 1)), jnp.where(low, pltpu.roll(b, 64, 1), d)
    low = (lane & 32) == 0
    a, b = jnp.where(low, a, pltpu.roll(b, 32, 1)), jnp.where(low, pltpu.roll(a, 96, 1), b)
    c, d = jnp.where(low, c, pltpu.roll(d, 32, 1)), jnp.where(low, pltpu.roll(c, 96, 1), d)
    return a, b, c, d


def spread_rows_of(out, plain, rows, nz, order):
    spread_rows, spreads, mask = row_constants(rows, nz)
    wide = sum(dot(plain[d].reshape(TERMS * 32, K2).astype(BF), spreads[c]) for c, d in enumerate(order))
    wide = wide.astype(BF).reshape(TERMS, 32, 256)
    for m in range(TERMS):
        mats = (dot(spread_rows, wide[m]) * mask).astype(BF)
        for c in range(2):
            out[m, c] = mats[:, 128 * c:128 * c + 128]


def lane_matrix(transposed, constants):
    spread_rows, spread_lanes, mask = constants
    return (dot(spread_rows[:, 0:K2], dot(transposed, spread_lanes).astype(BF)) * mask).astype(BF)


def parity():
    return lax.axis_index("gx") & 1, lax.axis_index("gy") & 1


def chosen(child_ref, which):
    first, second = child_ref[:, 0, :].astype(F32), child_ref[:, 1, :].astype(F32)
    return jnp.where(which == 0, first, second).astype(BF), jnp.where(which == 0, second, first).astype(BF)


def lane_level(turned, wide_y, wide_z, y_out, z_out, on_j, along_k, order_y):
    both = jnp.concatenate([on_j[1], along_k[1]], axis=1)
    wide = dot(turned[...].reshape(3 * TERMS * 32, K2).astype(BF), both).astype(BF)
    wide_y[...] = wide[:, 0:128].reshape(3, TERMS, 32, 128)
    wide_z[...] = wide[:, 128:256].reshape(3, TERMS, 32, 128)
    for (spread, _, mask), source_ref, order, out in (
        (on_j, wide_y, order_y, y_out), (along_k, wide_z, (1, 2, 0), z_out),
    ):
        for m in range(0, TERMS, 2):
            tiles = [source_ref[d, m + c] for c in range(2) for d in order]
            mats = dot(spread, jnp.concatenate(tiles, axis=1))
            for c in range(2):
                for e in range(3):
                    lane = 384 * c + 128 * e
                    tile = (mats[:, lane:lane + 128] * mask).astype(BF)
                    if out is y_out:
                        out[m + c, e] = tile
                    else:
                        out[e, m + c] = tile


def converted(ref, natural, select):
    values = ref[0, 0].astype(F32)
    for i in range(K2):
        natural[4 * i:4 * i + 4, :] = values[:, 400 * i:400 * i + 400]
    return dot(natural[...].astype(BF), select[...]).astype(BF)


def early_kernel(fine_hbm, coarse_hbm, child_hbm, own_hbm, coarse_ref, child_ref, own_blocks, select_out,
                 fine_rows, fine_y, fine_z, down_rows, down_y, down_z, fine_ref, own_ref, natural, plain, turned, wide_y, wide_z, sems):
    copies = [
        pltpu.make_async_copy(src, dst, sems.at[n])
        for n, (src, dst) in enumerate((
            (fine_hbm, fine_ref), (coarse_hbm, coarse_ref), (child_hbm, child_ref), (own_hbm, own_ref),
        ))
    ]
    for copy in copies:
        copy.start()
    plain[...] = jnp.zeros(plain.shape, F32)
    turned[...] = jnp.zeros(turned.shape, F32)
    px, py = parity()
    on_j, on_k, to_natural = lane_constants(True), lane_constants(False), lane_constants(False, True)
    for copy in copies:
        copy.wait()
    for d in range(3):
        for m in range(TERMS):
            matrix = fine_ref[d, m].astype(F32)
            plain[d, m, 0:K2, :] = matrix
            turned[d, m, 0:K2, :] = matrix.T
    near_x, near_y = 2 - 2 * px, 2 - 2 * py
    lane_level(turned, wide_y, wide_z, fine_y, fine_z, on_j, to_natural, (1, near_y, 2 - near_y))
    spread_rows_of(fine_rows, plain, FINE_ROWS, 4, (1, near_x, 2 - near_x))
    own_x, other_x = chosen(child_ref, px)
    own_y, other_y = chosen(child_ref, py)
    down_y[0:128, :] = lane_matrix(flipped(own_y), on_j)
    down_y[128:256, :] = lane_matrix(flipped(other_y), on_j)
    for c in range(2):
        down_z[128 * c:128 * c + 128, :] = lane_matrix(flipped(child_ref[:, c, :]), on_k)
    select_out[...] = onehot(iota((400, 512), 0) == natural_place(iota((1, 512), 1)))
    centre = converted(own_ref, natural, select_out)
    for b in range(4):
        own_blocks[b] = centre[:, 128 * b:128 * b + 128]
    lane = iota((1, 160), 1)
    far = lane >= 80
    lane = jnp.where(far, lane - 80, lane)
    wide = dot(own_x, onehot(jnp.where(far, -1, lane >> 2) == iota((K2, 160), 0)))
    wide = wide + dot(other_x, onehot(jnp.where(far, lane >> 2, -1) == iota((K2, 160), 0)))
    r = iota((96, 1), 0)
    cz = jnp.where(r >= 48, 1, 0)
    r = r - 48 * cz
    mixed = dot(onehot((r >> 1) == iota((96, K2), 1)), wide.astype(BF))
    down_rows[...] = (mixed * onehot((2 * (r & 1) + cz) == (lane & 3), F32)).astype(BF)


def late_kernel(coarse_ref, child_ref, coarse_rows, coarse_y, coarse_z,
                up_rows, up_y, up_z, plain, turned, wide_y, wide_z):
    plain[...] = jnp.zeros(plain.shape, F32)
    turned[...] = jnp.zeros(turned.shape, F32)
    px, py = parity()
    on_j, on_k, to_natural = lane_constants(True), lane_constants(False), lane_constants(False, True)
    near_x, near_y = 2 - 2 * px, 2 - 2 * py
    for d in range(3):
        for m in range(TERMS):
            matrix = coarse_ref[d, m].astype(F32)
            plain[d, m, 0:K2, :] = matrix
            turned[d, m, 0:K2, :] = matrix.T
    lane_level(turned, wide_y, wide_z, coarse_y, coarse_z, on_j, on_k, (1, 2 - near_y, near_y))
    spread_rows_of(coarse_rows, plain, COARSE_ROWS, 2, (1, 2 - near_x, near_x))
    own_x, _ = chosen(child_ref, px)
    own_y, _ = chosen(child_ref, py)
    up_y[...] = lane_matrix(own_y, on_j)
    for c in range(2):
        up_z[c] = lane_matrix(child_ref[:, c, :], to_natural)
    wide = dot(flipped(own_x), onehot((iota((1, 48), 1) >> 1) == iota((K2, 48), 0)))
    mixed = dot(onehot((iota((80, 1), 0) >> 2) == iota((80, K2), 1)), wide.astype(BF))
    keep = ((iota((80, 1), 0) & 3) >> 1) == (iota((1, 48), 1) & 1)
    up_rows[...] = (mixed * onehot(keep, F32)).astype(BF)


def bf16(*shape):
    return jax.ShapeDtypeStruct(shape, BF)


def early(fine_blocks, coarse_blocks, child, own):
    operands = [
        pltpu.with_memory_space_constraint(x, pltpu.HBM)
        for x in (fine_blocks, coarse_blocks, jnp.transpose(child, (1, 0, 2)), own)
    ]
    out_shape = tuple(bf16(*x.shape) for x in operands[1:3]) + (
        bf16(4, FINE_ROWS, 128), bf16(400, 512),
        bf16(TERMS, 2, FINE_ROWS, 128), bf16(TERMS, 3, 128, 128), bf16(3, TERMS, 128, 128),
        bf16(96, 160), bf16(256, 128), bf16(256, 128),
    )
    return pl.pallas_call(
        early_kernel, out_shape=out_shape, name="early",
        in_specs=[pl.BlockSpec(memory_space=pltpu.HBM)] * 4,
        scratch_shapes=[
            pltpu.VMEM(operands[0].shape, BF), pltpu.VMEM(operands[3].shape, BF), pltpu.VMEM((FINE_ROWS, 400), F32),
        ] + lane_scratch() + [pltpu.SemaphoreType.DMA((4,))],
        compiler_params=pltpu.CompilerParams(vmem_limit_bytes=16 << 20),
        cost_estimate=pl.CostEstimate(flops=2 * 10**9, bytes_accessed=4 * 10**6, transcendentals=0),
    )(*operands)


def lane_scratch():
    return [pltpu.VMEM((3, TERMS, 32, K2), F32)] * 2 + [pltpu.VMEM((3, TERMS, 32, 128), BF)] * 2


def late(blocks):
    out_shape = (bf16(TERMS, 2, COARSE_ROWS, 128), bf16(TERMS, 3, 128, 128), bf16(3, TERMS, 128, 128))
    out_shape += (bf16(80, 48), bf16(128, 128), bf16(2, 128, 128))
    return small_call(late_kernel, "late", out_shape, 2 * 10**9, *blocks, scratch=lane_scratch())


def source_kernel(own, select, ynear, corner, xnear, down_rows, down_y, down_z,
                  packet, nears, natural, mixed, turned):
    centre, diagonal = joined([own[b] for b in range(4)]), converted(corner, natural.at[0], select)
    x_near, y_near = converted(xnear, natural.at[1], select), converted(ynear, natural.at[2], select)
    for b in range(4):
        here = slice(128 * b, 128 * b + 128)
        packet[b, 0:80, :] = centre[:, here]
        nears[0, b] = x_near[:, here]
        nears[1, b] = y_near[:, here]
    for c, (one, two) in enumerate(((centre, x_near), (y_near, diagonal))):
        rows = dot(down_rows[...], jnp.concatenate([one, two], axis=0)).astype(BF)
        for b in range(4):
            mixed[c, 96 * b:96 * b + 96, :] = rows[:, 128 * b:128 * b + 128]
    summed = dot(jnp.concatenate([mixed[0], mixed[1]], axis=1), down_y[...])
    blocks = exchange([summed[96 * b:96 * b + 96, :] for b in range(4)])
    for b in range(4):
        for c in range(2):
            turned[c, 48 * b:48 * b + 48, :] = blocks[b][48 * c:48 * c + 48, :].astype(BF)
    total = dot(jnp.concatenate([turned[0], turned[1]], axis=1), down_z[...])
    blocks = exchange([total[48 * b:48 * b + 48, :] for b in range(4)])
    for b in range(4):
        packet[b, 80:120, :] = blocks[b][0:PARENT_ROWS, :].astype(BF)


def source(columns, down_rows, down_y, down_z):
    out_shape = (
        jax.ShapeDtypeStruct((4, FINE_ROWS + PARENT_ROWS, 128), BF),
        jax.ShapeDtypeStruct((2, 4, FINE_ROWS, 128), BF),
    )
    scratch = [
        pltpu.VMEM((3, FINE_ROWS, 400), F32),
        pltpu.VMEM((2, 8 * COARSE_ROWS, 128), BF),
        pltpu.VMEM((2, 4 * COARSE_ROWS, 128), BF),
    ]
    return pl.pallas_call(
        source_kernel, out_shape=out_shape, scratch_shapes=scratch, name="source",
        compiler_params=pltpu.CompilerParams(vmem_limit_bytes=16 << 20),
        cost_estimate=pl.CostEstimate(flops=10**9, bytes_accessed=10**6, transcendentals=0),
    )(*columns, down_rows, down_y, down_z)


def joined(blocks):
    return jnp.concatenate(blocks, axis=1)


def row_pass(rows, row_mats, stacks, targets):
    stacks = [[joined(column) for column in stack] for stack in stacks]
    stacks = [(stack[0] if len(stack) == 1 else jnp.concatenate(stack, axis=0)).astype(BF) for stack in stacks]
    chunk = 3
    for stack, target in zip(stacks, targets):
        for start in range(0, TERMS, chunk):
            mats = [row_mats[start:start + chunk, c].reshape(chunk * rows, 128) for c in range(2)]
            result = dot(jnp.concatenate(mats, axis=1)[:, 0:stack.shape[0]], stack)
            for c in range(chunk):
                for b in range(4):
                    target[start + c, b * rows:b * rows + rows, :] = (
                        result[c * rows:(c + 1) * rows, 128 * b:128 * b + 128].astype(BF)
                    )


def y_pass(rows, parts, y_mats, target):
    zero = jnp.zeros((128 * len(parts), 128), BF)
    for m in range(0, TERMS, 2):
        one, two = (jnp.concatenate([y_mats[m + c, n] for n in range(len(parts))], axis=0) for c in range(2))
        mats = jnp.concatenate(
            [jnp.concatenate([one, zero], axis=0), jnp.concatenate([zero, two], axis=0)], axis=1
        )
        values = jnp.concatenate([part[m + c] for c in range(2) for part in parts], axis=1)
        result = dot(values, mats)
        for c in range(2):
            blocks = exchange([result[b * rows:(b + 1) * rows, 128 * c:128 * c + 128] for b in range(4)])
            for b in range(4):
                target[m + c, b * rows:(b + 1) * rows, :] = blocks[b].astype(BF)


def level_vertical(rows, nz, centre, y_mats, z_mats, scratch):
    y_pass(rows, (centre,), y_mats, scratch)
    sides = dot(
        joined([scratch[m] for m in range(TERMS)]),
        joined([z_mats[n].reshape(TERMS * 128, 128) for n in (1, 2)]),
    )
    z = iota((4 * rows, 128), 0) & (nz - 1)
    upper = jnp.where(z == nz - 1, 0.0, pltpu.roll(sides[:, 0:128], 4 * rows - 1, 0))
    return upper + jnp.where(z == 0, 0.0, pltpu.roll(sides[:, 128:256], 1, 0))


def level_rest(rows, parts, y_mats, z_mats, scratch):
    y_pass(rows, parts, y_mats, scratch)
    return dot(joined([scratch[m] for m in range(TERMS)]), z_mats[0].reshape(TERMS * 128, 128))


def fine_near_kernel(packet, nears, row_mats, y_mats, z_mats, y_near, vertical, centre, scratch):
    own = [packet[b, 0:80, :] for b in range(4)]
    row_pass(FINE_ROWS, row_mats, ([[nears[1, b] for b in range(4)]], [own]), (y_near, centre))
    vertical[...] = level_vertical(FINE_ROWS, 4, centre, y_mats, z_mats, scratch)


def coarse_near_kernel(packet, row_mats, y_mats, z_mats, vertical, centre, scratch):
    own = [packet[b, 80:120, :].astype(F32) for b in range(4)]
    row_pass(COARSE_ROWS, row_mats, ([own],), (centre,))
    vertical[...] = level_vertical(COARSE_ROWS, 2, centre, y_mats, z_mats, scratch)


def parents_kernel(y_packet, x_packet, y_parent, x_parent):
    for b in range(4):
        y_parent[b] = y_packet[b, 80:120, :]
        x_parent[b] = x_packet[b, 80:120, :]


def fine_far_kernel(packet, nears, y_packet, x_packet, row_mats, x_sum, y_far):
    own, x_far, y_column = ([ref[b, 0:80, :] for b in range(4)] for ref in (packet, x_packet, y_packet))
    stacks = ([own, [nears[0, b] for b in range(4)], x_far], [y_column])
    row_pass(FINE_ROWS, row_mats, stacks, (x_sum, y_far))


def fine_rest_kernel(x_sum, y_near, y_far, vertical, y_mats, z_mats, out, scratch):
    out[...] = vertical[...] + level_rest(FINE_ROWS, (x_sum, y_near, y_far), y_mats, z_mats, scratch)


def small_call(kernel, name, out_shape, flops, *operands, scratch=()):
    return pl.pallas_call(
        kernel, out_shape=out_shape, name=name, scratch_shapes=scratch,
        compiler_params=pltpu.CompilerParams(vmem_limit_bytes=16 << 20),
        cost_estimate=pl.CostEstimate(flops=flops, bytes_accessed=4 * 10**6, transcendentals=0),
    )(*operands)


def coarse_kernel(packet, yfar, yother, xfar, xother, vertical, row_mats, y_mats, z_mats,
                  up_rows, up_y, up_z, fine_term, out, wide, grown, turned, x_sum, far_side, other_side, scratch):
    own = [packet[b, 80:120, :].astype(F32) for b in range(4)]
    others = [[ref[b].astype(F32) for b in range(4)] for ref in (xfar, xother, yfar, yother)]
    parts = (x_sum, far_side, other_side)
    row_pass(COARSE_ROWS, row_mats, ([own, others[0], others[1]], [others[2]], [others[3]]), parts)
    result = vertical[...] + level_rest(COARSE_ROWS, parts, y_mats, z_mats, scratch)
    blocks = exchange([result[48 * b:48 * b + 48, :] for b in range(4)])
    for b in range(4):
        wide[:, 128 * b:128 * b + 128] = blocks[b].astype(BF)
    part = dot(up_rows[...], wide[...]).astype(BF)
    for b in range(4):
        grown[80 * b:80 * b + 80, :] = part[:, 128 * b:128 * b + 128]
    part = dot(grown[...], up_y[...])
    blocks = exchange([part[80 * b:80 * b + 80, :] for b in range(4)])
    for b in range(4):
        turned[80 * b:80 * b + 80, :] = blocks[b].astype(BF)
    both = dot(turned[...], jnp.concatenate([up_z[0], up_z[1]], axis=1))
    expanded = jnp.where((iota((320, 128), 0) & 1) == 0, both[:, 0:128], both[:, 128:256])
    total = fine_term[...] + expanded
    for i in range(K2):
        for b in range(4):
            here = 400 * i + 100 * b
            out[0, 0, :, here:here + 100] = total[80 * b + 4 * i:80 * b + 4 * i + 4, 0:100]


def coarse(operands):
    part = pltpu.VMEM((TERMS, 4 * COARSE_ROWS, 128), BF)
    scratch = [
        pltpu.VMEM((COARSE_ROWS, 512), BF),
        pltpu.VMEM((320, 128), BF),
        pltpu.VMEM((320, 128), BF),
    ] + [part] * 4
    return small_call(
        coarse_kernel, "coarse", jax.ShapeDtypeStruct((1, 1, 4, 8000), F32), 4 * 10**9, *operands, scratch=scratch
    )


def near(block, axis):
    return lax.ppermute(block, axis, [(i, i ^ 1) for i in range(lax.axis_size(axis))])


def far(block, axis):
    count = lax.axis_size(axis)
    return lax.ppermute(block, axis, [(i, ((i + 1) ^ 1) - 1) for i in range(1, count - 1)])


def corner(block):
    nx, ny = lax.axis_size("gx"), lax.axis_size("gy")
    route = [(x * ny + y, (x ^ 1) * ny + (y ^ 1)) for x in range(nx) for y in range(ny)]
    return lax.ppermute(block, ("gx", "gy"), route)


def shards(fine_source, fine_blocks, coarse_blocks, child_filter_matrices):
    columns = [near(fine_source, "gy"), corner(fine_source), near(fine_source, "gx")]
    coarse_ref, child_ref, own, select, fine_rows, fine_y, fine_z, *down = early(
        fine_blocks, coarse_blocks, child_filter_matrices, fine_source
    )
    packet, nears = source([own, select] + columns, *down)
    y_packet, x_packet = far(packet, "gy"), far(packet, "gx")
    blocks, _ = lax.optimization_barrier(((coarse_ref, child_ref), packet))
    mats = late(blocks)
    part = jax.ShapeDtypeStruct((TERMS, 4 * FINE_ROWS, 128), BF)
    parent = jax.ShapeDtypeStruct((4, PARENT_ROWS, 128), BF)
    fine_part = pltpu.VMEM((TERMS, 4 * FINE_ROWS, 128), BF)
    coarse_part = pltpu.VMEM((TERMS, 4 * COARSE_ROWS, 128), BF)
    fine_sum = jax.ShapeDtypeStruct((4 * FINE_ROWS, 128), F32)
    coarse_sum = jax.ShapeDtypeStruct((4 * COARSE_ROWS, 128), F32)
    y_near, fine_vertical = small_call(
        fine_near_kernel, "fine_near", (part, fine_sum), 2 * 10**9,
        packet, nears, fine_rows, fine_y, fine_z, scratch=[fine_part] * 2,
    )
    coarse_vertical = small_call(
        coarse_near_kernel, "coarse_near", coarse_sum, 10**9, packet, *mats[0:3], scratch=[coarse_part] * 2,
    )
    y_parent, x_parent = small_call(parents_kernel, "parents", (parent, parent), 10**6, y_packet, x_packet)
    y_other, x_other = near(y_parent, "gy"), near(x_parent, "gx")
    x_sum, y_far = small_call(
        fine_far_kernel, "fine_far", (part, part), 10**9, packet, nears, y_packet, x_packet, fine_rows,
    )
    fine_term = small_call(
        fine_rest_kernel, "fine_rest", fine_sum, 4 * 10**9,
        x_sum, y_near, y_far, fine_vertical, fine_y, fine_z, scratch=[fine_part],
    )
    return coarse((packet, y_parent, y_other, x_parent, x_other, coarse_vertical, *mats, fine_term))


def solution(mesh):
    in_specs = (P("gx", "gy", None, None), P(), P(), P())
    out_specs = P("gx", "gy", None, None)
    return jax.shard_map(shards, mesh=mesh, in_specs=in_specs, out_specs=out_specs, check_vma=False)
```
